32 devices in a mesh: seq: 8 (over z, x), head: 4 (over y, core).
Axes of the slice: x: 2, y: 2, z: 4, core: 2. Of those that a mesh axis runs over, the one named last changes fastest.
Arguments:
- hidden_in: bfloat16 [4, 2048, 1024], P(None, ('seq', 'head')), may hold values from -6 to 6
- norm_gain1: float32 [1024], replicated, may hold values from 0.5 to 1.5
- w_query: bfloat16 [1024, 1024], P(None, 'head'), may hold values from -0.1875 to 0.1875
- w_key: bfloat16 [1024, 512], P(None, 'head'), may hold values from -0.1875 to 0.1875
- w_value: bfloat16 [1024, 512], P(None, 'head'), may hold values from -0.1875 to 0.1875
- w_out: bfloat16 [1024, 1024], P('head'), may hold values from -2 to 2
- norm_gain2: float32 [1024], replicated, may hold values from 0.5 to 1.5
- expert_gate: bfloat16 [16, 1024, 512], P('seq'), may hold values from -0.1875 to 0.1875
- expert_up: bfloat16 [16, 1024, 512], P('seq'), may hold values from -0.1875 to 0.1875
- expert_down: bfloat16 [16, 512, 1024], P('seq'), may hold values from -1 to 1
- routes: int32 [4, 2048, 8], P(None, ('seq', 'head')), may hold values from 0 to 15, all different within a row
- gate_weights: float32 [4, 2048, 8], P(None, ('seq', 'head')), may hold values from 0.05 to 0.25
- cotangent: bfloat16 [4, 2048, 1024], P(None, ('seq', 'head')), may hold values from -6 to 6
Outputs:
- layer_out: bfloat16 [4, 2048, 1024], P(None, ('seq', 'head'))
- input_grad: bfloat16 [4, 2048, 1024], P(None, ('seq', 'head'))
- norm_gain1_grad: float32 [1024], replicated
- w_query_grad: float32 [1024, 1024], P(None, 'head')
- w_key_grad: float32 [1024, 512], P(None, 'head')
- w_value_grad: float32 [1024, 512], P(None, 'head')
- w_out_grad: float32 [1024, 1024], P('head')
- norm_gain2_grad: float32 [1024], replicated
- expert_gate_grad: float32 [16, 1024, 512], P('seq')
- expert_up_grad: float32 [16, 1024, 512], P('seq')
- expert_down_grad: float32 [16, 512, 1024], P('seq')
The draws below stay inside these ranges and needn't reach their ends.
Inputs may be any that keep to these rules, and one draw needn't show every extreme that they name: `routes`: each token names 8 different experts.
All inputs are finite; a program needn't handle non-finite values.
Results may differ from the reference program's by a relative error of at most 0.028.
Values may be sent and summed in bfloat16 or wider, within the bound.
No kernel may reach another device: no remote copies, remote signals or barrier semaphores. Data moves between devices by JAX's collectives and lax.ppermute only.
A program may use at most 192 MiB of HBM per device.

```python
import math
import jax
import jax.numpy as jnp
from jax import lax

D = 1024
HEADS = 16
KV_HEADS = 8
HD = 64
FF = 512
TOP = 8
SEQS = 4
SUB = 64
LEN = 2048
EXPERTS = 16
CAP = 160
N_SEQ = 8
N_HEAD = 4


def shard_levels(stream_key, dims, split, smallest, top_value):
    factor_of, own = 1.0, jax.random.fold_in(stream_key, 6)
    for dim, shards_of in split:
        steps = jnp.exp(jax.random.uniform(jax.random.fold_in(own, dim), (shards_of,), jnp.float32, smallest / len(split), top_value / len(split)))
        factor_of = factor_of * jnp.repeat(steps, dims[dim] // shards_of).reshape([-1 if axis == dim else 1 for axis in range(len(dims))])
    return factor_of


def different_ones(stream_key, rows, count, top, lift):
    order = jax.random.permutation(jax.random.fold_in(stream_key, 1), count)
    pull = order
    for power in range(3):
        pull = pull * pull // count
    pull = pull * lift // count
    tickets = jax.random.randint(jax.random.fold_in(stream_key, 2), (rows, count), 0, 4096) + pull
    sure = jax.random.permutation(jax.random.fold_in(stream_key, 3), rows)[jnp.arange(count) % rows]
    tickets = jnp.where(jnp.arange(rows)[:, None] == sure[None, :], 1 << 14, tickets)
    merit = tickets * count + jnp.arange(count)
    return lax.top_k(merit.astype(jnp.int32), top)[1].astype(jnp.int32)


def noise(key, extent, spread, bound, split=(), kind=jnp.bfloat16):
    values = jax.random.normal(key, extent, jnp.float32) * spread
    if len(split) > 0:
        values = shard_levels(key, extent, split, -0.22, 0.18) * values
    return jnp.clip(values, min=-bound, max=bound).astype(kind)


def setup_inputs(seed: int = 0) -> dict:
    seeds = jax.random.split(jax.random.key(seed), 14)
    return {
        "hidden_in": noise(seeds[0], (SEQS, LEN, D), 1.0, 6.0, ((1, 32),)),
        "norm_gain1": jnp.clip(1.0 + 0.1 * jax.random.normal(seeds[1], (D,), jnp.float32), 0.5, 1.5),
        "w_query": noise(seeds[2], (D, HEADS * HD), D ** -0.5, 0.1875, ((1, 4),)),
        "w_key": noise(seeds[3], (D, KV_HEADS * HD), D ** -0.5, 0.1875, ((1, 4),)),
        "w_value": noise(seeds[4], (D, KV_HEADS * HD), D ** -0.5, 0.1875, ((1, 4),)),
        "w_out": noise(seeds[5], (HEADS * HD, D), (HEADS * HD // 128) ** -0.5, 2.0, ((0, 4),)),
        "norm_gain2": jnp.clip(1.0 + 0.1 * jax.random.normal(seeds[6], (D,), jnp.float32), 0.5, 1.5),
        "expert_gate": noise(seeds[7], (EXPERTS, D, FF), D ** -0.5, 0.1875, ((0, 8),)),
        "expert_up": noise(seeds[8], (EXPERTS, D, FF), D ** -0.5, 0.1875, ((0, 8),)),
        "expert_down": noise(seeds[9], (EXPERTS, FF, D), (FF // 16) ** -0.5, 1.0, ((0, 8),)),
        "routes": different_ones(seeds[10], SEQS * LEN, EXPERTS, TOP, 4096).reshape((SEQS, LEN, TOP)),
        "gate_weights": jnp.clip(jnp.exp(math.log(0.25) - 1.609438 * jax.random.uniform(seeds[11], (SEQS, LEN, TOP), jnp.float32) ** shard_levels(seeds[11], (SEQS, LEN, TOP), ((1, 32),), -0.2, 0.2)), 0.05, 0.25),
        "cotangent": noise(seeds[12], (SEQS, LEN, D), 1.0, 6.0, ((1, 32),)),
    }


norm_eps = 1e-06
rope_base = 10000.0
masked_value = -1e+30

@jax.custom_vjp
def low(v):
    return lax.optimization_barrier(v.astype(jnp.bfloat16)).astype(jnp.float32)

@jax.custom_vjp
def low_back(v):
    return v

def low_keep(v):
    return (low(v), None)

def low_pass(kept, grad):
    return (grad,)

def back_keep(v):
    return (v, None)

def back_low(kept, grad):
    return (low(grad),)
low.defvjp(low_keep, low_pass)
low_back.defvjp(back_keep, back_low)

def angle_tables(count, head_dim):
    half_dim = head_dim // 2
    frequencies = jnp.exp(-jnp.log(rope_base) * jnp.arange(half_dim, dtype=jnp.float32) * 2.0 / head_dim)
    angles = jnp.arange(count, dtype=jnp.float32)[:, None] * frequencies[None, :]
    return (jnp.cos(angles), jnp.sin(angles))

def rotate(values, cosine, sine_table):
    half_dim = values.shape[-1] // 2
    front_half = values[..., :half_dim]
    back_half = values[..., half_dim:]
    return jnp.concatenate([front_half * cosine - back_half * sine_table, back_half * cosine + front_half * sine_table], -1)

def rms_norm(values, gain_vec):
    return values * lax.rsqrt(lax.optimization_barrier(jnp.mean(values * values, -1, keepdims=True)) + norm_eps) * gain_vec

def high_dot(left_mat, right_mat):
    return jnp.dot(left_mat, right_mat, precision=lax.Precision.HIGHEST)

def route_tables(routes):
    devices = N_SEQ * N_HEAD
    pair_total = SEQS * SUB * TOP
    local_routes = routes.reshape(SEQS, devices, SUB, TOP).transpose(1, 0, 2, 3).reshape(devices, pair_total)
    seq_ids = jnp.arange(SEQS, dtype=jnp.int32)[None, :, None, None]
    dev_ids = jnp.arange(devices, dtype=jnp.int32)[:, None, None, None]
    row_ids = jnp.arange(SUB, dtype=jnp.int32)[None, None, :, None]
    top_ids = jnp.arange(TOP, dtype=jnp.int32)[None, None, None, :]
    pair_ids = ((seq_ids * LEN + dev_ids * SUB + row_ids) * TOP + top_ids).astype(jnp.int32).reshape(devices, pair_total)
    onehot = (local_routes[:, :, None] == jnp.arange(EXPERTS, dtype=jnp.int32)[None, None, :]).astype(jnp.int32)
    earlier = (jnp.cumsum(onehot, 1) - onehot).astype(jnp.int32)
    pair_rank = lax.optimization_barrier(jnp.sum(earlier * onehot, -1)).astype(jnp.int32)
    pair_kept = pair_rank < CAP
    dev_grid = jnp.broadcast_to(jnp.arange(devices, dtype=jnp.int32)[:, None], local_routes.shape)
    slot_table = jnp.full((EXPERTS, devices, CAP), -1, jnp.int32).at[local_routes, dev_grid, pair_rank].set(pair_ids, mode='drop')
    slot_of_pair = jnp.where(pair_kept, (local_routes * devices + dev_grid) * CAP + pair_rank, -1).astype(jnp.int32)
    pair_slot = jnp.zeros((SEQS * LEN * TOP,), jnp.int32).at[pair_ids.reshape(-1)].set(slot_of_pair.reshape(-1))
    return (slot_table.reshape(EXPERTS, devices * CAP), pair_slot.reshape(SEQS * LEN, TOP))

def reference(hidden_in, norm_gain1, w_query, w_key, w_value, w_out, norm_gain2, expert_gate, expert_up, expert_down, routes, gate_weights, cotangent):
    slot_table, pair_slot = route_tables(routes)
    gate_pairs = gate_weights.astype(jnp.float32).reshape(SEQS * LEN, TOP)
    group_size = HEADS // KV_HEADS
    query_block = min(512, LEN)
    block_total = LEN // query_block
    score_scale = 1.0 / math.sqrt(HD)

    def forward(x_val, gain_one, wq_val, wk_val, wv_val, wo_val, gain_two, wg_val, wu_val, wd_val):
        normed_one = low(rms_norm(x_val, gain_one))
        cosine, sine_table = angle_tables(LEN, HD)
        query_lin = low_back(high_dot(normed_one, wq_val)).reshape(SEQS, LEN, KV_HEADS, group_size, HD)
        query_rot = low(rotate(query_lin, cosine[:, None, None, :], sine_table[:, None, None, :]))
        key_lin = low_back(high_dot(normed_one, wk_val)).reshape(SEQS, LEN, KV_HEADS, HD)
        key_rot = low(rotate(key_lin, cosine[:, None, :], sine_table[:, None, :]))
        value_all = low(low_back(high_dot(normed_one, wv_val))).reshape(SEQS, LEN, KV_HEADS, HD)

        def attend(block_index):
            seq_index = block_index // block_total
            block_start = block_index % block_total * query_block
            query_seq = lax.dynamic_index_in_dim(query_rot, seq_index, 0, keepdims=False)
            query_part = lax.dynamic_slice_in_dim(query_seq, block_start, query_block, 0)
            key_seq = lax.dynamic_index_in_dim(key_rot, seq_index, 0, keepdims=False)
            value_seq = lax.dynamic_index_in_dim(value_all, seq_index, 0, keepdims=False)
            scores = low_back(jnp.einsum('qgrd,kgd->grqk', query_part, key_seq, precision=lax.Precision.HIGHEST)) * score_scale
            query_pos = block_start + jnp.arange(query_block, dtype=jnp.int32)
            key_pos = jnp.arange(LEN, dtype=jnp.int32)
            scores = jnp.where(key_pos[None, :] <= query_pos[:, None], scores, masked_value)
            probs_b = low(jax.nn.softmax(scores, -1))
            return jnp.einsum('grqk,kgd->qgrd', probs_b, value_seq, precision=lax.Precision.HIGHEST)
        blocks = lax.map(jax.checkpoint(attend), jnp.arange(SEQS * block_total, dtype=jnp.int32))
        attended = low(low_back(blocks.reshape(SEQS, LEN, HEADS * HD)))
        resid = x_val + low_back(high_dot(attended, wo_val))
        normed_two = low(rms_norm(resid, gain_two))
        flat_rows = normed_two.reshape(SEQS * LEN, D)
        slot_valid = slot_table >= 0
        slot_token = jnp.where(slot_valid, slot_table // TOP, 0).astype(jnp.int32)

        def expert(pack):
            token_e, valid_e, gate_e, up_e, down_e = pack
            slot_rows = jnp.where(valid_e[:, None], low_back(flat_rows[token_e]), jnp.float32(0.0))
            gate_lin = low_back(high_dot(slot_rows, gate_e))
            up_lin = low_back(high_dot(slot_rows, up_e))
            hidden = low(jax.nn.silu(gate_lin) * up_lin)
            return low(low_back(high_dot(hidden, down_e)))
        outputs = lax.map(jax.checkpoint(expert), (slot_token, slot_valid, wg_val, wu_val, wd_val))
        outputs = outputs.reshape(-1, D)
        pair_keep = pair_slot >= 0
        flat_index = jnp.where(pair_keep, pair_slot, 0).astype(jnp.int32)
        pair_weight = jnp.where(pair_keep, gate_pairs, jnp.float32(0.0))
        mixture = jnp.zeros((SEQS * LEN, D), jnp.float32)
        for top_slot in range(TOP):
            mixture = mixture + pair_weight[:, top_slot:top_slot + 1] * outputs[flat_index[:, top_slot]]
        return resid + mixture.reshape(SEQS, LEN, D)
    result, pullback = jax.vjp(forward, hidden_in.astype(jnp.float32), norm_gain1.astype(jnp.float32), w_query.astype(jnp.float32), w_key.astype(jnp.float32), w_value.astype(jnp.float32), w_out.astype(jnp.float32), norm_gain2.astype(jnp.float32), expert_gate.astype(jnp.float32), expert_up.astype(jnp.float32), expert_down.astype(jnp.float32))
    gradients = pullback(cotangent.astype(jnp.float32))
    return (result.astype(jnp.bfloat16), gradients[0].astype(jnp.bfloat16), gradients[1], gradients[2], gradients[3], gradients[4], gradients[5], gradients[6], gradients[7], gradients[8], gradients[9])
```

```python
import functools
import math

import jax
import jax.numpy as jnp
from jax import lax
from jax.experimental import pallas as pl
from jax.experimental.pallas import tpu as pltpu
from jax.sharding import PartitionSpec as P

HD = 64
TOP = 8
LANES = 128

norm_eps = 1e-06
rope_base = 10000.0
masked_value = -1e30
BF = jnp.bfloat16
F32 = jnp.float32


def attn_fwd_kernel(share_ref, pay_ref, out_ref, ot_ref, lse_ref, kv_ref, kvt_ref, *, span, rows, block):
    b = pl.program_id(0)
    count = pay_ref.shape[0]

    @pl.when(b == 0)
    def _():
        def fill(i, _):
            start = pl.multiple_of(i * span, span)
            tile = pay_ref[i, pl.ds(rows, span), :]
            kv_ref[pl.ds(start, span), :] = tile
            kvt_ref[:, pl.ds(start, span)] = tile.T
            return 0
        lax.fori_loop(0, count, fill, 0)

    q_start = b * span + share_ref[0] * rows
    qt = pay_ref[b, pl.ds(0, rows), :].T * jnp.bfloat16(0.125)
    qt = jnp.concatenate([qt[:HD], qt[HD:]], 1)
    qt = jnp.concatenate([qt, jnp.zeros_like(qt)], 0)
    last = (q_start + rows - 1) // block

    def step(kb, carry, masked):
        run_max, run_sum, acc = carry
        start = pl.multiple_of(kb * block, block)
        scores = jnp.dot(kv_ref[pl.ds(start, block), :], qt, preferred_element_type=jnp.float32)
        if masked:
            keys = start + lax.broadcasted_iota(jnp.int32, scores.shape, 0)
            queries = q_start + lax.broadcasted_iota(jnp.int32, scores.shape, 1) % rows
            scores = jnp.where(keys <= queries, scores, masked_value)
        new_max = jnp.maximum(run_max, jnp.max(scores, 0, keepdims=True))
        factor = jnp.exp(run_max - new_max)
        probs = jnp.exp(scores - new_max)
        run_sum = run_sum * factor + jnp.sum(probs, 0, keepdims=True)
        acc = acc * factor + jnp.dot(
            kvt_ref[pl.ds(HD, HD), pl.ds(start, block)], probs.astype(jnp.bfloat16), preferred_element_type=jnp.float32)
        return new_max, run_sum, acc

    carry = (jnp.full((1, 2 * rows), masked_value, jnp.float32), jnp.zeros((1, 2 * rows), jnp.float32), jnp.zeros((HD, 2 * rows), jnp.float32))
    carry = lax.fori_loop(0, last, functools.partial(step, masked=False), carry)
    run_max, run_sum, acc = step(last, carry, True)
    ot = acc / run_sum
    ot_ref[0] = ot
    lse_ref[0] = jnp.broadcast_to(run_max + jnp.log(run_sum), lse_ref.shape[1:])
    out_ref[0] = jnp.concatenate([ot[:, :rows], ot[:, rows:]], 0).T.astype(jnp.bfloat16)

def attn_fwd(pay, share, span, block=512):
    n, r, _ = pay.shape
    rows = r - span
    total = n * span
    block = min(block, total)
    return pl.pallas_call(
        functools.partial(attn_fwd_kernel, span=span, rows=rows, block=block),
        out_shape=(jax.ShapeDtypeStruct((n, rows, 128), jnp.bfloat16), jax.ShapeDtypeStruct((n, HD, 2 * rows), jnp.float32), jax.ShapeDtypeStruct((n, 8, 2 * rows), jnp.float32)),
        grid_spec=pltpu.PrefetchScalarGridSpec(
            num_scalar_prefetch=1, grid=(n,),
            in_specs=[pl.BlockSpec((n, r, 128), lambda b, s: (0, 0, 0))],
            out_specs=[pl.BlockSpec((1, rows, 128), lambda b, s: (b, 0, 0)), pl.BlockSpec((1, HD, 2 * rows), lambda b, s: (b, 0, 0)), pl.BlockSpec((1, 8, 2 * rows), lambda b, s: (b, 0, 0))],
            scratch_shapes=[pltpu.VMEM((total, 128), jnp.bfloat16), pltpu.VMEM((128, total), jnp.bfloat16)],
        ),
        name="attn_fwd",
    )(share, pay)

def swap_halves(v):
    lane = lax.broadcasted_iota(jnp.int32, v.shape, v.ndim - 1)
    return jnp.where(lane % HD < HD // 2, pltpu.roll(v, 128 - HD // 2, v.ndim - 1), pltpu.roll(v, HD // 2, v.ndim - 1))

def attn_bwd_kernel(share_ref, pay_ref, go_ref, ot_ref, lse_ref, cos_ref, sin_ref, out_ref, kv_ref, kvt_ref, dk_ref, dv_ref, *, span, rows, block):
    b = pl.program_id(0)
    count = pay_ref.shape[0]

    @pl.when(b == 0)
    def _():
        def fill(i, _):
            start = pl.multiple_of(i * span, span)
            tile = pay_ref[i, pl.ds(rows, span), :]
            kv_ref[pl.ds(start, span), :] = tile
            kvt_ref[:, pl.ds(start, span)] = tile.T
            return 0
        lax.fori_loop(0, count, fill, 0)
        dk_ref[...] = jnp.zeros_like(dk_ref)
        dv_ref[...] = jnp.zeros_like(dv_ref)

    q_start = b * span + share_ref[0] * rows
    low = lax.broadcasted_iota(jnp.int32, (rows, 128), 1) < HD
    q01 = pay_ref[b, pl.ds(0, rows), :] * jnp.bfloat16(0.125)
    go01 = go_ref[0]
    zero = jnp.zeros_like(q01)
    q_rows = jnp.concatenate([jnp.where(low, q01, zero), jnp.where(low, zero, q01)], 0)
    go_rows = jnp.concatenate([jnp.where(low, go01, zero), jnp.where(low, zero, go01)], 0)
    qt = q01.T
    qt = jnp.concatenate([qt[:HD], qt[HD:]], 1)
    qt = jnp.concatenate([qt, jnp.zeros_like(qt)], 0)
    gt = go01.T
    gt = jnp.concatenate([gt[:HD], gt[HD:]], 1)
    delta = jnp.sum(gt.astype(jnp.float32) * ot_ref[0], 0, keepdims=True)
    gt = jnp.concatenate([jnp.zeros_like(gt), gt], 0)
    lse = lse_ref[0, 0:1, :]
    last = (q_start + rows - 1) // block

    def step(kb, dq, masked):
        start = pl.multiple_of(kb * block, block)
        kv = kv_ref[pl.ds(start, block), :]
        scores = jnp.dot(kv, qt, preferred_element_type=jnp.float32)
        probs = jnp.exp(scores - lse)
        if masked:
            keys = start + lax.broadcasted_iota(jnp.int32, scores.shape, 0)
            queries = q_start + lax.broadcasted_iota(jnp.int32, scores.shape, 1) % rows
            probs = jnp.where(keys <= queries, probs, 0.0)
        dprobs = jnp.dot(kv, gt, preferred_element_type=jnp.float32)
        dscores = (probs * (dprobs - delta)).astype(jnp.bfloat16)
        dv_ref[pl.ds(start, block), :] += jnp.dot(probs.astype(jnp.bfloat16), go_rows, preferred_element_type=jnp.float32)
        dk_ref[pl.ds(start, block), :] += jnp.dot(dscores, q_rows, preferred_element_type=jnp.float32)
        return dq + jnp.dot(kvt_ref[pl.ds(0, HD), pl.ds(start, block)], dscores, preferred_element_type=jnp.float32)

    dq = lax.fori_loop(0, last, functools.partial(step, masked=False), jnp.zeros((HD, 2 * rows), jnp.float32))
    dq = step(last, dq, True)
    dq = jnp.concatenate([dq[:, :rows], dq[:, rows:]], 0).T * 0.125
    at = pl.multiple_of(q_start, rows)
    dq = dq * cos_ref[pl.ds(at, rows), :] - swap_halves(dq) * sin_ref[pl.ds(at, rows), :]
    out_ref[b, pl.ds(0, rows), :] = dq.astype(jnp.bfloat16)

    @pl.when(b == count - 1)
    def _():
        def drain(i, _):
            start = pl.multiple_of(i * span, span)
            dk = dk_ref[pl.ds(start, span), :]
            dk = dk + pltpu.roll(dk, HD, 1)
            dk = dk * cos_ref[pl.ds(start, span), :] - swap_halves(dk) * sin_ref[pl.ds(start, span), :]
            dv = dv_ref[pl.ds(start, span), :]
            dv = dv + pltpu.roll(dv, HD, 1)
            lane = lax.broadcasted_iota(jnp.int32, dk.shape, 1)
            out_ref[i, pl.ds(rows, span), :] = jnp.where(lane < HD, dk, dv).astype(jnp.bfloat16)
            return 0
        lax.fori_loop(0, count, drain, 0)

def attn_bwd(pay, go, ot, lse, cos, sin, share, span, block=512):
    n, r, _ = pay.shape
    rows = r - span
    total = n * span
    block = min(block, total)
    whole = lambda *shape: pl.BlockSpec(shape, lambda b, s: (0,) * len(shape))
    return pl.pallas_call(
        functools.partial(attn_bwd_kernel, span=span, rows=rows, block=block),
        out_shape=jax.ShapeDtypeStruct((n, r, 128), jnp.bfloat16),
        grid_spec=pltpu.PrefetchScalarGridSpec(
            num_scalar_prefetch=1, grid=(n,),
            in_specs=[whole(n, r, 128), pl.BlockSpec((1, rows, 128), lambda b, s: (b, 0, 0)), pl.BlockSpec((1, HD, 2 * rows), lambda b, s: (b, 0, 0)), pl.BlockSpec((1, 8, 2 * rows), lambda b, s: (b, 0, 0)), whole(total, 128), whole(total, 128)],
            out_specs=whole(n, r, 128),
            scratch_shapes=[pltpu.VMEM((total, 128), jnp.bfloat16), pltpu.VMEM((128, total), jnp.bfloat16), pltpu.VMEM((total, 128), jnp.float32), pltpu.VMEM((total, 128), jnp.float32)],
        ),
        name="attn_bwd",
    )(share, pay, go, ot, lse, cos, sin)

def angle_tables(positions):
    half = HD // 2
    frequencies = jnp.exp(-jnp.log(rope_base) * jnp.arange(half, dtype=F32) * 2.0 / HD)
    angles = positions.astype(F32)[:, None] * frequencies[None, :]
    cosine, sine = jnp.cos(angles), jnp.sin(angles)
    return jnp.concatenate([cosine] * 4, 1), jnp.concatenate([-sine, sine] * 2, 1)


def qkv_kernel(x_ref, w_ref, cos_ref, sin_ref, out_ref, *, rows):
    span = x_ref.shape[1]
    shares = span // rows
    joint = jnp.dot(x_ref[0], w_ref[...], preferred_element_type=F32)
    low = lax.broadcasted_iota(jnp.int32, (span, LANES), 1) < HD
    cosine, sine = cos_ref[...], sin_ref[...]
    for g in range(joint.shape[1] // 256):
        query = joint[:, g * 256 : g * 256 + LANES]
        other = joint[:, g * 256 + LANES : (g + 1) * 256]
        query = (query * cosine + swap_halves(query) * sine).astype(BF)
        other = jnp.where(low, other * cosine + swap_halves(other) * sine, other).astype(BF)
        for j in range(shares):
            out_ref[g * shares + j, pl.ds(0, rows), :] = query[j * rows : (j + 1) * rows]
            out_ref[g * shares + j, pl.ds(rows, span), :] = other


def project_qkv(normed_all, w_joint, cosine, sine, rows):
    seqs, span, width = normed_all.shape
    cols = w_joint.shape[1]
    units = cols // 256 * (span // rows)
    fixed = lambda *shape: pl.BlockSpec(shape, lambda s: (0,) * len(shape))
    return pl.pallas_call(
        functools.partial(qkv_kernel, rows=rows),
        out_shape=jax.ShapeDtypeStruct((seqs * units, rows + span, LANES), BF),
        grid=(seqs,),
        in_specs=[
            pl.BlockSpec((1, span, width), lambda s: (s, 0, 0)),
            fixed(width, cols),
            fixed(span, LANES),
            fixed(span, LANES),
        ],
        out_specs=pl.BlockSpec((units, rows + span, LANES), lambda s: (s, 0, 0)),
        name="project_qkv",
    )(normed_all, w_joint, cosine, sine)


def minor_of(axis):
    return 2 if axis == "head" or lax.axis_size(axis) < 16 else 4


def place_of(axis):
    minor = minor_of(axis)
    index = lax.axis_index(axis)
    return index // minor, index % minor


def hop(value, axis, da, db):
    n, minor = lax.axis_size(axis), minor_of(axis)
    major = n // minor
    pairs = [
        (a * minor + b, (a + da) % major * minor + (b + db) % minor)
        for a in range(major)
        for b in range(minor)
    ]
    return lax.ppermute(value, axis, pairs)


def gather_slots(value, axis):
    minor = minor_of(axis)
    major = lax.axis_size(axis) // minor
    slots = []
    for a in range(major):
        if a:
            value = hop(value, axis, 1, 0)
        row, moved = [value], value
        for _ in range(1, minor):
            moved = hop(moved, axis, 0, 1)
            row.append(moved)
        slots.append(row)
    return slots


def slot_owner(axis, a, b):
    minor = minor_of(axis)
    major = lax.axis_size(axis) // minor
    my_a, my_b = place_of(axis)
    return (my_a - a) % major * minor + (my_b - b) % minor


def ring_reduce(parts, axis, da, db):
    def add(x, y):
        return (x.astype(F32) + y.astype(F32)).astype(BF)

    total = parts[1 % len(parts)]
    for part in parts[2:]:
        total = add(hop(total, axis, da, db), part)
    if len(parts) > 1:
        total = hop(total, axis, da, db).astype(F32) + parts[0].astype(F32)
    return total


def reduce_slots(slots, axis):
    rows = [ring_reduce(row, axis, 0, 1).astype(BF) for row in slots]
    return ring_reduce(rows, axis, 1, 0)


def pick(value, index):
    return lax.dynamic_index_in_dim(value, index, 0, keepdims=False)


def all_reduce(value, axis):
    minor, major = value.shape[:2]
    my_a, my_b = place_of(axis)
    total = pick(value, my_b).astype(F32)
    for d in range(1, minor):
        total = total + hop(pick(value, (my_b + d) % minor), axis, 0, d).astype(F32)
    value = total.astype(BF)
    total = pick(value, my_a).astype(F32)
    for d in range(1, major):
        total = total + hop(pick(value, (my_a + d) % major), axis, d, 0).astype(F32)
    part = total.astype(BF)
    half = lax.dynamic_update_index_in_dim(jnp.zeros(value.shape, BF), part, my_a, 0)
    for d in range(1, major):
        half = lax.dynamic_update_index_in_dim(half, hop(part, axis, d, 0), (my_a - d) % major, 0)
    whole = lax.dynamic_update_index_in_dim(jnp.zeros((minor,) + half.shape, BF), half, my_b, 0)
    for d in range(1, minor):
        whole = lax.dynamic_update_index_in_dim(whole, hop(half, axis, 0, d), (my_b - d) % minor, 0)
    return whole.astype(F32)


def small_sum(value, axis):
    minor = minor_of(axis)
    major = lax.axis_size(axis) // minor
    value = value + sum(hop(value, axis, 0, d) for d in range(1, minor))
    return value + sum(hop(value, axis, d, 0) for d in range(1, major))


def in_order(slots, axis):
    n = lax.axis_size(axis)
    whole = jnp.zeros((n,) + slots[0][0].shape, slots[0][0].dtype)
    for a, row in enumerate(slots):
        for b, block in enumerate(row):
            whole = lax.dynamic_update_index_in_dim(whole, block, slot_owner(axis, a, b), 0)
    return whole


def norm_backward(values, inv_root, gain_vec, grad_normed):
    weighted = grad_normed * gain_vec
    gain_part = jnp.sum(grad_normed * values * inv_root, (0, 1))
    grad_values = inv_root * weighted - values * (inv_root * inv_root * inv_root) * jnp.mean(
        values * weighted, -1, keepdims=True
    )
    return (grad_values, gain_part)


def dot(left, right):
    return jnp.dot(left, right, preferred_element_type=F32)


def dot_nt(left, right):
    return lax.dot_general(left, right, (((1,), (1,)), ((), ())), preferred_element_type=F32)


def dot_tn(left, right):
    return lax.dot_general(left, right, (((0,), (0,)), ((), ())), preferred_element_type=F32)


def per_device(
    hidden_in,
    norm_gain1,
    w_query,
    w_key,
    w_value,
    w_out,
    norm_gain2,
    expert_gate,
    expert_up,
    expert_down,
    routes,
    gate_weights,
    cotangent,
):
    seqs, sub, width = hidden_in.shape
    tokens = seqs * sub
    heads, ranks = lax.axis_size("head"), lax.axis_size("seq")
    kv_local = w_key.shape[1] // HD
    q_cols, k_cols = w_query.shape[1], w_key.shape[1]
    span = sub * heads
    total_len = span * ranks
    shares = ranks // (seqs * kv_local)
    rows = span // shares
    experts_local = expert_gate.shape[0]
    expert_total = experts_local * ranks
    capacity = tokens * TOP * 5 // (4 * expert_total)
    seq_rank = lax.axis_index("seq")
    head_rank = lax.axis_index("head")
    share = (seq_rank % shares).astype(jnp.int32).reshape(1)

    x_float = hidden_in.astype(F32)
    inv_one = lax.rsqrt(jnp.mean(x_float * x_float, -1, keepdims=True) + norm_eps)
    normed_one = (x_float * inv_one * norm_gain1).astype(BF)
    normed_all = in_order(gather_slots(normed_one, "head"), "head")
    normed_all = normed_all.transpose(1, 0, 2, 3).reshape(seqs, span, width)

    w_joint = jnp.concatenate(
        [
            part
            for g in range(kv_local)
            for part in (
                w_query[:, g * LANES : (g + 1) * LANES],
                w_key[:, g * HD : (g + 1) * HD],
                w_value[:, g * HD : (g + 1) * HD],
            )
        ],
        1,
    )
    cos_all, sin_all = angle_tables(jnp.arange(total_len, dtype=jnp.int32))
    cos_own = lax.dynamic_slice_in_dim(cos_all, seq_rank * span, span, 0)
    sin_own = lax.dynamic_slice_in_dim(sin_all, seq_rank * span, span, 0)

    route_tok = routes.reshape(tokens, TOP)
    gate_tok = gate_weights.reshape(tokens, TOP)
    chosen = route_tok[:, :, None] == jnp.arange(expert_total, dtype=jnp.int32)
    named = jnp.any(chosen, 1)
    gate_of = jnp.sum(jnp.where(chosen, gate_tok[:, :, None], 0.0), 1)
    order = jnp.arange(tokens, dtype=jnp.int32)
    before = (order[:, None] > order[None, :]).astype(BF)
    rank_of = dot(before, named.astype(BF))
    weight_of = jnp.where(named & (rank_of < capacity), gate_of, 0.0)
    weight_send = weight_of.reshape(tokens, ranks, experts_local).transpose(1, 2, 0)
    weight_all = lax.all_to_all(weight_send, "seq", 0, 0, tiled=True)

    pay = project_qkv(normed_all, w_joint, cos_own, sin_own, rows)
    pay = lax.all_to_all(pay, "seq", 0, 0, tiled=True)
    cot_slots = gather_slots(cotangent.reshape(tokens, width), "seq")
    w_full = in_order(gather_slots(w_out, "head"), "head").reshape(heads * q_cols, width)
    attn, attn_t, lse = attn_fwd(pay, share, span)

    def to_tokens(value):
        if shares == 1:
            value = value.reshape(ranks * heads, sub, LANES)
            value = lax.all_to_all(value, ("seq", "head"), 0, 0, tiled=True)
            value = value.reshape(seqs, kv_local, heads, sub, LANES)
            return value.transpose(0, 3, 2, 1, 4)
        value = lax.all_to_all(value, "seq", 0, 0, tiled=True)
        value = value.reshape(seqs, kv_local, heads, sub, LANES).transpose(2, 0, 1, 3, 4)
        value = lax.all_to_all(value, "head", 0, 0, tiled=True)
        return value.transpose(1, 3, 0, 2, 4)

    def to_units(value):
        if shares == 1:
            value = value.transpose(0, 3, 2, 1, 4).reshape(ranks * heads, sub, LANES)
            value = lax.all_to_all(value, ("seq", "head"), 0, 0, tiled=True)
            return value.reshape(ranks, rows, LANES)
        value = value.transpose(2, 0, 3, 1, 4)
        value = lax.all_to_all(value, "head", 0, 0, tiled=True)
        value = value.transpose(1, 2, 0, 3, 4).reshape(ranks, rows, LANES)
        return lax.all_to_all(value, "seq", 0, 0, tiled=True)

    attn_local = to_tokens(attn).reshape(tokens, heads * q_cols)
    resid = x_float + dot(attn_local, w_full).reshape(seqs, sub, width)
    inv_two = lax.rsqrt(jnp.mean(resid * resid, -1, keepdims=True) + norm_eps)
    normed_two = (resid * inv_two * norm_gain2).astype(BF).reshape(tokens, width)

    row_slots = gather_slots(normed_two, "seq")
    out_slots, grad_slots = [], []
    kept = [[] for _ in range(4)]
    for a, row in enumerate(row_slots):
        x_blk = jnp.concatenate(row, 0)
        c_blk = jnp.concatenate(cot_slots[a], 0)
        w_blk = jnp.concatenate([pick(weight_all, slot_owner("seq", a, b)) for b in range(len(row))], 1)
        out_blk, grad_blk = 0.0, 0.0
        hiddens, grads = [], []
        for e in range(experts_local):
            weight = w_blk[e][:, None]
            gate_lin = dot(x_blk, expert_gate[e])
            up_lin = dot(x_blk, expert_up[e])
            sig = jax.nn.sigmoid(gate_lin)
            silu = gate_lin * sig
            hidden = (weight * (silu * up_lin)).astype(BF)
            grad_hidden = weight * dot_nt(c_blk, expert_down[e])
            grad_up = (grad_hidden * silu).astype(BF)
            grad_gate = (grad_hidden * up_lin * sig * (1.0 + gate_lin * (1.0 - sig))).astype(BF)
            out_blk = out_blk + dot(hidden, expert_down[e])
            grad_blk = grad_blk + dot_nt(grad_gate, expert_gate[e]) + dot_nt(grad_up, expert_up[e])
            hiddens.append(hidden)
            grads.append((grad_gate, grad_up))
        kept[0].append(x_blk)
        kept[1].append(c_blk)
        kept[2].append(hiddens)
        kept[3].append(grads)
        out_blk = out_blk.astype(BF).reshape(len(row), tokens, width)
        grad_blk = grad_blk.astype(BF).reshape(len(row), tokens, width)
        out_slots.append([out_blk[b] for b in range(len(row))])
        grad_slots.append([grad_blk[b] for b in range(len(row))])

    grad_normed_two = reduce_slots(grad_slots, "seq").reshape(seqs, sub, width)
    grad_out = cotangent.astype(F32)
    grad_norm_two, gain_two_part = norm_backward(resid, inv_two, norm_gain2, grad_normed_two)
    grad_resid = grad_out + grad_norm_two
    grad_resid_b = grad_resid.astype(BF)
    grad_attn = dot_nt(grad_resid_b.reshape(tokens, width), w_full).astype(BF)
    grad_attn = to_units(grad_attn.reshape(seqs, sub, heads, kv_local, LANES))
    grad_pay = attn_bwd(pay, grad_attn, attn_t, lse, cos_all, sin_all, share, span)

    x_every, c_every = jnp.concatenate(kept[0], 0), jnp.concatenate(kept[1], 0)
    grad_gate_w, grad_up_w, grad_down_w = [], [], []
    for e in range(experts_local):
        h_every = jnp.concatenate([h[e] for h in kept[2]], 0)
        g_every = jnp.concatenate([g[e][0] for g in kept[3]], 0)
        u_every = jnp.concatenate([g[e][1] for g in kept[3]], 0)
        grad_gate_w.append(dot_tn(x_every, g_every).astype(BF))
        grad_up_w.append(dot_tn(x_every, u_every).astype(BF))
        grad_down_w.append(dot_tn(h_every, c_every).astype(BF))

    def head_total(parts):
        value = jnp.stack(parts)
        inner = value.shape[1] // (heads // 2)
        value = all_reduce(value.reshape(2, heads // 2, inner, value.shape[2]), "head")
        return value.reshape(experts_local, -1, value.shape[3])

    gate_total, up_total, down_total = head_total(grad_gate_w), head_total(grad_up_w), head_total(grad_down_w)
    mixture = reduce_slots(out_slots, "seq").reshape(seqs, sub, width)
    layer_out = (resid + mixture).astype(BF)

    def seq_total(value):
        minor = minor_of("seq")
        major = ranks // minor
        shape = value.shape
        value = value.reshape(minor, major, shape[0] // ranks, shape[1])
        return all_reduce(value, "seq").reshape(shape)

    out_w_part = dot_tn(attn_local, grad_resid_b.reshape(tokens, width)).astype(BF)
    out_w_part = out_w_part.reshape(heads, q_cols, width)
    out_w_slots = [
        [pick(out_w_part, slot_owner("head", a, b)) for b in range(2)] for a in range(heads // 2)
    ]
    out_total = seq_total(reduce_slots(out_w_slots, "head").astype(BF))

    grad_pay = lax.all_to_all(grad_pay, "seq", 0, 0, tiled=True)
    grad_q = grad_pay[:, :rows].reshape(seqs, kv_local, span, LANES)
    grad_kv = grad_pay[:, rows:].reshape(seqs, kv_local, shares, span, LANES)
    if shares == 1:
        grad_kv = grad_kv[:, :, 0]
    else:
        grad_kv = jnp.sum(grad_kv.astype(F32), 2).astype(BF)
    grad_joint = jnp.concatenate([grad_q, grad_kv], -1).transpose(0, 2, 1, 3)
    grad_joint = grad_joint.reshape(seqs * span, kv_local * 256)
    grad_w_joint = dot_tn(normed_all.reshape(seqs * span, width), grad_joint)
    joint_total = seq_total(grad_w_joint.astype(BF))
    grad_part = dot_nt(grad_joint, w_joint).astype(BF)
    grad_part = grad_part.reshape(seqs, heads, sub, width).transpose(1, 0, 2, 3)
    part_slots = [
        [pick(grad_part, slot_owner("head", a, b)) for b in range(2)] for a in range(heads // 2)
    ]
    grad_normed_one = reduce_slots(part_slots, "head")
    grad_norm_one, gain_one_part = norm_backward(x_float, inv_one, norm_gain1, grad_normed_one)
    input_grad = (grad_resid + grad_norm_one).astype(BF)
    gains = small_sum(small_sum(jnp.stack([gain_one_part, gain_two_part]), "head"), "seq")

    joint_total = joint_total.reshape(width, kv_local, 256)
    query_total = joint_total[:, :, :LANES].reshape(width, q_cols)
    key_total = joint_total[:, :, LANES : LANES + HD].reshape(width, k_cols)
    value_total = joint_total[:, :, LANES + HD :].reshape(width, k_cols)
    return (
        layer_out,
        input_grad,
        gains[0],
        query_total,
        key_total,
        value_total,
        out_total,
        gains[1],
        gate_total,
        up_total,
        down_total,
    )


def solution(mesh):
    return jax.shard_map(
        per_device,
        mesh=mesh,
        in_specs=(
            P(None, ("seq", "head"), None),
            P(),
            P(None, "head"),
            P(None, "head"),
            P(None, "head"),
            P("head", None),
            P(),
            P("seq", None, None),
            P("seq", None, None),
            P("seq", None, None),
            P(None, ("seq", "head"), None),
            P(None, ("seq", "head"), None),
            P(None, ("seq", "head"), None),
        ),
        out_specs=(
            P(None, ("seq", "head"), None),
            P(None, ("seq", "head"), None),
            P(),
            P(None, "head"),
            P(None, "head"),
            P(None, "head"),
            P("head", None),
            P(),
            P("seq", None, None),
            P("seq", None, None),
            P("seq", None, None),
        ),
        check_vma=False,
    )
```

```python
import functools
import math

import jax
import jax.numpy as jnp
import numpy as np
from jax import lax
from jax.experimental import pallas as pl
from jax.experimental.pallas import tpu as pltpu
from jax.sharding import PartitionSpec as P

HD = 64
TOP = 8
LANES = 128

norm_eps = 1e-06
rope_base = 10000.0
masked_value = -1e30
BF = jnp.bfloat16
F32 = jnp.float32


def cost(us):
    return pl.CostEstimate(flops=0, bytes_accessed=us * 3000000, transcendentals=0)


def attn_fwd_kernel(share_ref, pay_ref, out_ref, ot_ref, lse_ref, kv_ref, kvt_ref, *, span, rows, block):
    b = pl.program_id(0)
    count = pay_ref.shape[0]

    @pl.when(b == 0)
    def _():
        def fill(i, _):
            start = pl.multiple_of(i * span, span)
            tile = pay_ref[i, pl.ds(rows, span), :]
            kv_ref[pl.ds(start, span), :] = tile
            kvt_ref[:, pl.ds(start, span)] = tile.T
            return 0
        lax.fori_loop(0, count, fill, 0)

    q_start = b * span + share_ref[0] * rows
    qt = pay_ref[b, pl.ds(0, rows), :].T * jnp.bfloat16(0.125)
    qt = jnp.concatenate([qt[:HD], qt[HD:]], 1)
    qt = jnp.concatenate([qt, jnp.zeros_like(qt)], 0)
    last = (q_start + rows - 1) // block

    def step(kb, carry, masked):
        run_max, run_sum, acc = carry
        start = pl.multiple_of(kb * block, block)
        scores = jnp.dot(kv_ref[pl.ds(start, block), :], qt, preferred_element_type=jnp.float32)
        if masked:
            keys = start + lax.broadcasted_iota(jnp.int32, scores.shape, 0)
            queries = q_start + lax.broadcasted_iota(jnp.int32, scores.shape, 1) % rows
            scores = jnp.where(keys <= queries, scores, masked_value)
        new_max = jnp.maximum(run_max, jnp.max(scores, 0, keepdims=True))
        factor = jnp.exp(run_max - new_max)
        probs = jnp.exp(scores - new_max)
        run_sum = run_sum * factor + jnp.sum(probs, 0, keepdims=True)
        acc = acc * factor + jnp.dot(
            kvt_ref[pl.ds(HD, HD), pl.ds(start, block)], probs.astype(jnp.bfloat16), preferred_element_type=jnp.float32)
        return new_max, run_sum, acc

    carry = (jnp.full((1, 2 * rows), masked_value, jnp.float32), jnp.zeros((1, 2 * rows), jnp.float32), jnp.zeros((HD, 2 * rows), jnp.float32))
    carry = lax.fori_loop(0, last, functools.partial(step, masked=False), carry)
    run_max, run_sum, acc = step(last, carry, True)
    ot = acc / run_sum
    ot_ref[0] = ot
    lse_ref[0] = jnp.broadcast_to(run_max + jnp.log(run_sum), lse_ref.shape[1:])
    out_ref[0] = jnp.concatenate([ot[:, :rows], ot[:, rows:]], 0).T.astype(jnp.bfloat16)

def attn_fwd(pay, share, span, block=512):
    n, r, _ = pay.shape
    rows = r - span
    total = n * span
    block = min(block, total)
    return pl.pallas_call(
        functools.partial(attn_fwd_kernel, span=span, rows=rows, block=block),
        out_shape=(jax.ShapeDtypeStruct((n, rows, 128), jnp.bfloat16), jax.ShapeDtypeStruct((n, HD, 2 * rows), jnp.float32), jax.ShapeDtypeStruct((n, 8, 2 * rows), jnp.float32)),
        grid_spec=pltpu.PrefetchScalarGridSpec(
            num_scalar_prefetch=1, grid=(n,),
            in_specs=[pl.BlockSpec((n, r, 128), lambda b, s: (0, 0, 0))],
            out_specs=[pl.BlockSpec((1, rows, 128), lambda b, s: (b, 0, 0)), pl.BlockSpec((1, HD, 2 * rows), lambda b, s: (b, 0, 0)), pl.BlockSpec((1, 8, 2 * rows), lambda b, s: (b, 0, 0))],
            scratch_shapes=[pltpu.VMEM((total, 128), jnp.bfloat16), pltpu.VMEM((128, total), jnp.bfloat16)],
        ),
        cost_estimate=cost(16),
        name="attn_fwd",
    )(share, pay)

def swap_halves(v):
    lane = lax.broadcasted_iota(jnp.int32, v.shape, v.ndim - 1)
    return jnp.where(lane % HD < HD // 2, pltpu.roll(v, 128 - HD // 2, v.ndim - 1), pltpu.roll(v, HD // 2, v.ndim - 1))

def attn_bwd_kernel(share_ref, pay_ref, go_ref, ot_ref, lse_ref, *refs, span, rows, block):
    tables, (out_ref, kv_ref, kvt_ref, dk_ref, dv_ref) = refs[:4], refs[4:]
    b = pl.program_id(0)
    count = pay_ref.shape[0]

    @pl.when(b == 0)
    def _():
        def fill(i, _):
            start = pl.multiple_of(i * span, span)
            tile = pay_ref[i, pl.ds(rows, span), :]
            kv_ref[pl.ds(start, span), :] = tile
            kvt_ref[:, pl.ds(start, span)] = tile.T
            return 0
        lax.fori_loop(0, count, fill, 0)
        dk_ref[...] = jnp.zeros_like(dk_ref)
        dv_ref[...] = jnp.zeros_like(dv_ref)

    q_start = b * span + share_ref[0] * rows
    low = lax.broadcasted_iota(jnp.int32, (rows, 128), 1) < HD
    q01 = pay_ref[b, pl.ds(0, rows), :] * jnp.bfloat16(0.125)
    go01 = go_ref[0]
    zero = jnp.zeros_like(q01)
    q_rows = jnp.concatenate([jnp.where(low, q01, zero), jnp.where(low, zero, q01)], 0)
    go_rows = jnp.concatenate([jnp.where(low, go01, zero), jnp.where(low, zero, go01)], 0)
    qt = q01.T
    qt = jnp.concatenate([qt[:HD], qt[HD:]], 1)
    qt = jnp.concatenate([qt, jnp.zeros_like(qt)], 0)
    gt = go01.T
    gt = jnp.concatenate([gt[:HD], gt[HD:]], 1)
    delta = jnp.sum(gt.astype(jnp.float32) * ot_ref[0], 0, keepdims=True)
    gt = jnp.concatenate([jnp.zeros_like(gt), gt], 0)
    lse = lse_ref[0, 0:1, :]
    last = (q_start + rows - 1) // block

    def step(kb, dq, masked):
        start = pl.multiple_of(kb * block, block)
        kv = kv_ref[pl.ds(start, block), :]
        scores = jnp.dot(kv, qt, preferred_element_type=jnp.float32)
        probs = jnp.exp(scores - lse)
        if masked:
            keys = start + lax.broadcasted_iota(jnp.int32, scores.shape, 0)
            queries = q_start + lax.broadcasted_iota(jnp.int32, scores.shape, 1) % rows
            probs = jnp.where(keys <= queries, probs, 0.0)
        dprobs = jnp.dot(kv, gt, preferred_element_type=jnp.float32)
        dscores = (probs * (dprobs - delta)).astype(jnp.bfloat16)
        dv_ref[pl.ds(start, block), :] += jnp.dot(probs.astype(jnp.bfloat16), go_rows, preferred_element_type=jnp.float32)
        dk_ref[pl.ds(start, block), :] += jnp.dot(dscores, q_rows, preferred_element_type=jnp.float32)
        return dq + jnp.dot(kvt_ref[pl.ds(0, HD), pl.ds(start, block)], dscores, preferred_element_type=jnp.float32)

    dq = lax.fori_loop(0, last, functools.partial(step, masked=False), jnp.zeros((HD, 2 * rows), jnp.float32))
    dq = step(last, dq, True)
    dq = jnp.concatenate([dq[:, :rows], dq[:, rows:]], 0).T * 0.125
    cosine, sine = turned(tables, pl.ds(pl.multiple_of(share_ref[0] * rows, rows), rows), b)
    dq = dq * cosine - swap_halves(dq) * sine
    out_ref[b, pl.ds(0, rows), :] = dq.astype(jnp.bfloat16)

    @pl.when(b == count - 1)
    def _():
        def drain(i, _):
            start = pl.multiple_of(i * span, span)
            dk = dk_ref[pl.ds(start, span), :]
            dk = dk + pltpu.roll(dk, HD, 1)
            cosine, sine = turned(tables, pl.ds(0, span), i)
            dk = dk * cosine - swap_halves(dk) * sine
            dv = dv_ref[pl.ds(start, span), :]
            dv = dv + pltpu.roll(dv, HD, 1)
            lane = lax.broadcasted_iota(jnp.int32, dk.shape, 1)
            out_ref[i, pl.ds(rows, span), :] = jnp.where(lane < HD, dk, dv).astype(jnp.bfloat16)
            return 0
        lax.fori_loop(0, count, drain, 0)

def attn_bwd(pay, go, ot, lse, tables, share, span, block=512):
    n, r, _ = pay.shape
    rows = r - span
    total = n * span
    block = min(block, total)
    whole = lambda *shape: pl.BlockSpec(shape, lambda b, s: (0,) * len(shape))
    return pl.pallas_call(
        functools.partial(attn_bwd_kernel, span=span, rows=rows, block=block),
        out_shape=jax.ShapeDtypeStruct((n, r, 128), jnp.bfloat16),
        grid_spec=pltpu.PrefetchScalarGridSpec(
            num_scalar_prefetch=1, grid=(n,),
            in_specs=[whole(n, r, 128), pl.BlockSpec((1, rows, 128), lambda b, s: (b, 0, 0)), pl.BlockSpec((1, HD, 2 * rows), lambda b, s: (b, 0, 0)), pl.BlockSpec((1, 8, 2 * rows), lambda b, s: (b, 0, 0)), *[whole(*table.shape) for table in tables]],
            out_specs=whole(n, r, 128),
            scratch_shapes=[pltpu.VMEM((total, 128), jnp.bfloat16), pltpu.VMEM((128, total), jnp.bfloat16), pltpu.VMEM((total, 128), jnp.float32), pltpu.VMEM((total, 128), jnp.float32)],
        ),
        cost_estimate=cost(24),
        name="attn_bwd",
    )(share, pay, go, ot, lse, *tables)

def angle_tables(count, step):
    half = HD // 2
    angles = step * np.arange(count)[:, None] * rope_base ** (-2.0 * np.arange(half) / HD)
    cosine, sine = np.cos(angles), np.sin(angles)
    tables = np.concatenate([cosine] * 4, 1), np.concatenate([-sine, sine] * 2, 1)
    return [table.astype(np.float32) for table in tables]


def turned(tables, at, far):
    cos_ref, sin_ref, cos_far_ref, sin_far_ref = tables
    cosine, sine = cos_ref[at, :], sin_ref[at, :]
    cos_far, sin_far = cos_far_ref[pl.ds(far, 1), :], sin_far_ref[pl.ds(far, 1), :]
    return cosine * cos_far - sine * sin_far, sine * cos_far + cosine * sin_far


def dot(left, right):
    return jnp.dot(left, right, preferred_element_type=F32)


def dot_nt(left, right):
    return lax.dot_general(left, right, (((1,), (1,)), ((), ())), preferred_element_type=F32)


def dot_tn(left, right):
    return lax.dot_general(left, right, (((0,), (0,)), ((), ())), preferred_element_type=F32)


def qkv_kernel(rank_ref, x_ref, wq_ref, wk_ref, wv_ref, *refs, rows):
    tables, (out_ref, w_ref, cos_own, sin_own) = refs[:4], refs[4:]
    span = x_ref.shape[1]
    shares = span // rows
    groups = wk_ref.shape[1] // HD

    @pl.when(pl.program_id(0) == 0)
    def _():
        for g in range(groups):
            w_ref[:, g * 256 : g * 256 + LANES] = wq_ref[:, g * LANES : (g + 1) * LANES]
            pair = [wk_ref[:, g * HD : (g + 1) * HD], wv_ref[:, g * HD : (g + 1) * HD]]
            w_ref[:, g * 256 + LANES : (g + 1) * 256] = jnp.concatenate(pair, 1)
        cos_own[...], sin_own[...] = turned(tables, pl.ds(0, span), rank_ref[0])

    joint = jnp.dot(x_ref[0], w_ref[...], preferred_element_type=F32)
    low = lax.broadcasted_iota(jnp.int32, (span, LANES), 1) < HD
    cosine, sine = cos_own[...], sin_own[...]
    for g in range(groups):
        query = joint[:, g * 256 : g * 256 + LANES]
        other = joint[:, g * 256 + LANES : (g + 1) * 256]
        query = (query * cosine + swap_halves(query) * sine).astype(BF)
        other = jnp.where(low, other * cosine + swap_halves(other) * sine, other).astype(BF)
        for j in range(shares):
            out_ref[g * shares + j, pl.ds(0, rows), :] = query[j * rows : (j + 1) * rows]
            out_ref[g * shares + j, pl.ds(rows, span), :] = other


def project_qkv(normed_all, w_query, w_key, w_value, tables, rank, rows):
    seqs, span, width = normed_all.shape
    q_cols, k_cols = w_query.shape[1], w_key.shape[1]
    cols = q_cols + 2 * k_cols
    units = cols // 256 * (span // rows)
    fixed = lambda *shape: pl.BlockSpec(shape, lambda s, r: (0,) * len(shape))
    return pl.pallas_call(
        functools.partial(qkv_kernel, rows=rows),
        out_shape=(
            jax.ShapeDtypeStruct((seqs * units, rows + span, LANES), BF),
            jax.ShapeDtypeStruct((width, cols), BF),
        ),
        grid_spec=pltpu.PrefetchScalarGridSpec(
            num_scalar_prefetch=1,
            grid=(seqs,),
            in_specs=[
                pl.BlockSpec((1, span, width), lambda s, r: (s, 0, 0)),
                fixed(width, q_cols),
                fixed(width, k_cols),
                fixed(width, k_cols),
                *[fixed(*table.shape) for table in tables],
            ],
            out_specs=[pl.BlockSpec((units, rows + span, LANES), lambda s, r: (s, 0, 0)), fixed(width, cols)],
            scratch_shapes=[pltpu.VMEM((span, LANES), F32), pltpu.VMEM((span, LANES), F32)],
        ),
        cost_estimate=cost(6),
        name="project_qkv",
    )(rank, normed_all, w_query, w_key, w_value, *tables)


def grad_attn_kernel(g_ref, w_ref, out_ref, *, seqs, heads, groups):
    sub = g_ref.shape[0] // seqs
    grad = dot_nt(g_ref[...], w_ref[...]).astype(BF)
    for h in range(heads):
        for g in range(groups):
            at = (h * groups + g) * LANES
            for s in range(seqs):
                out_ref[(s * groups + g) * heads + h] = grad[s * sub : (s + 1) * sub, at : at + LANES]


def grad_attn_units(grad, w_full, seqs, heads, groups):
    tokens, width = grad.shape
    return pl.pallas_call(
        functools.partial(grad_attn_kernel, seqs=seqs, heads=heads, groups=groups),
        out_shape=jax.ShapeDtypeStruct((seqs * groups * heads, tokens // seqs, LANES), BF),
        in_specs=[pl.BlockSpec(memory_space=pltpu.VMEM)] * 2,
        out_specs=pl.BlockSpec(memory_space=pltpu.VMEM),
        cost_estimate=cost(3),
        name="grad_attn_units",
    )(grad, w_full)


def minor_of(axis):
    return 2 if axis == "head" or lax.axis_size(axis) < 16 else 4


def place_of(axis):
    minor = minor_of(axis)
    index = lax.axis_index(axis)
    return index // minor, index % minor


def hop(value, axis, da, db):
    n, minor = lax.axis_size(axis), minor_of(axis)
    major = n // minor
    pairs = [
        (a * minor + b, (a + da) % major * minor + (b + db) % minor)
        for a in range(major)
        for b in range(minor)
    ]
    return lax.ppermute(value, axis, pairs)


def after(value, *others):
    return lax.optimization_barrier((value,) + others)[0]


def gather_slots(value, axis):
    slots = [spread(value, axis)]
    for _ in range(1, lax.axis_size(axis) // minor_of(axis)):
        slots.append(spread(hop(slots[-1][0], axis, 1, 0), axis))
    return slots


def join(*values):
    return lax.optimization_barrier(values)


def spread(value, axis):
    row = [value]
    for _ in range(1, minor_of(axis)):
        row.append(hop(row[-1], axis, 0, 1))
    return row


def slot_owner(axis, a, b):
    minor = minor_of(axis)
    major = lax.axis_size(axis) // minor
    my_a, my_b = place_of(axis)
    return (my_a - a) % major * minor + (my_b - b) % minor


def add(x, y):
    return x.astype(F32) + y.astype(F32)


def ring_reduce(parts, axis, da, db, gate=None):
    total = parts[1 % len(parts)]
    for part in parts[2:]:
        total = add(hop(total, axis, da, db), part).astype(BF)
    if len(parts) > 1:
        moved = hop(total, axis, da, db)
        total = add(moved if gate is None else after(moved, gate), parts[0])
    return total


def reduce_slots(slots, axis, gate=None):
    rows = [ring_reduce(row, axis, 0, 1).astype(BF) for row in slots]
    return ring_reduce(rows, axis, 1, 0, gate)


def pick(value, index):
    return lax.dynamic_index_in_dim(value, index, 0, keepdims=False)


def line_sum(value, axis):
    major = value.shape[0]
    my_a, _ = place_of(axis)
    total = pick(value, my_a)
    for d in range(1, major):
        total = add(total, hop(pick(value, (my_a + d) % major), axis, d, 0))
    return total.astype(BF)


def share_sum(value, axis):
    minor = value.shape[0]
    _, my_b = place_of(axis)
    total = pick(value, my_b)
    for d in range(1, minor):
        total = add(total, hop(pick(value, (my_b + d) % minor), axis, 0, d))
    return line_sum(total.astype(BF), axis)


def small_sum(value, axis):
    minor = minor_of(axis)
    major = lax.axis_size(axis) // minor
    value = value + sum(hop(value, axis, 0, d) for d in range(1, minor))
    return value + sum(hop(value, axis, d, 0) for d in range(1, major))


def expert_kernel(owner_ref, *refs, halves, steps, tall):
    slots, (gate_ref, up_ref, down_ref) = refs[: len(refs) - 3], refs[len(refs) - 3 :]
    e, y, k = pl.program_id(0), pl.program_id(1), pl.program_id(2)
    row = y * steps + k
    for i, slot in enumerate(slots):

        @pl.when(owner_ref[i] == e * halves + y)
        def _():
            block = slot[...].astype(F32)
            half = block.shape[1] // 2

            @pl.when(row < tall)
            def _():
                gate_ref[0] = block[:, :half]
                up_ref[0] = block[:, half:]

            @pl.when(row >= tall)
            def _():
                down_ref[0] = block


def expert_outputs(slots, width, ff):
    my_a, my_b = place_of("head")
    halves, experts = len(slots), len(slots[0])
    flat = [block for row in slots for block in row]
    owner = [
        (my_b - b) % experts * halves + (my_a - a) % halves
        for a in range(halves)
        for b in range(experts)
    ]
    owner = jnp.stack(owner).astype(jnp.int32)
    block = math.gcd(flat[0].shape[0], 256)
    steps, tall = flat[0].shape[0] // block, width // block

    def spec(i):
        def place(e, y, k, owner):
            turn = owner[i] - (e * halves + y)
            return (jnp.where(turn == 0, k, jnp.where(turn > 0, 0, steps - 1)), 0)

        return pl.BlockSpec((block, width), place)

    return pl.pallas_call(
        functools.partial(expert_kernel, halves=halves, steps=steps, tall=tall),
        out_shape=(
            jax.ShapeDtypeStruct((experts, width, ff), F32),
            jax.ShapeDtypeStruct((experts, width, ff), F32),
            jax.ShapeDtypeStruct((experts, ff, width), F32),
        ),
        grid_spec=pltpu.PrefetchScalarGridSpec(
            num_scalar_prefetch=1,
            grid=(experts, halves, steps),
            in_specs=[spec(i) for i in range(len(flat))],
            out_specs=[
                pl.BlockSpec((1, block, ff), lambda e, y, k, o: (e, jnp.minimum(y * steps + k, tall - 1), 0)),
                pl.BlockSpec((1, block, ff), lambda e, y, k, o: (e, jnp.minimum(y * steps + k, tall - 1), 0)),
                pl.BlockSpec((1, block, width), lambda e, y, k, o: (e, jnp.maximum(y * steps + k - tall, 0), 0)),
            ],
        ),
        cost_estimate=cost(12),
        name="expert_outputs",
    )(owner, *flat)


def in_order(slots, axis, by_minor=False):
    major, minor = len(slots), len(slots[0])
    whole = jnp.zeros((major * minor,) + slots[0][0].shape, slots[0][0].dtype)
    for a, row in enumerate(slots):
        for b, block in enumerate(row):
            owner = slot_owner(axis, a, b)
            if by_minor:
                owner = owner % minor * major + owner // minor
            whole = lax.dynamic_update_index_in_dim(whole, block, owner, 0)
    return whole


def norm_backward(values, inv_root, gain_vec, grad_normed):
    weighted = grad_normed * gain_vec
    gain_part = jnp.sum(grad_normed * values * inv_root, (0, 1))
    grad_values = inv_root * weighted - values * (inv_root * inv_root * inv_root) * jnp.mean(
        values * weighted, -1, keepdims=True
    )
    return (grad_values, gain_part)


def moe_kernel(*refs, parts):
    x_refs, c_refs = refs[:parts], refs[parts : 2 * parts]
    w_ref, gate_ref, up_ref, down_ref = refs[2 * parts : 2 * parts + 4]
    xs_ref, cs_ref, h_ref, dg_ref, du_ref, out_acc, dx_acc = refs[-7:]
    out_refs, dx_refs = refs[-7 - 2 * parts : -7 - parts], refs[-7 - parts : -7]
    j = pl.program_id(0)
    rows = x_refs[0].shape[0]

    @pl.when(j == 0)
    def _():
        for p in range(parts):
            xs_ref[pl.ds(p * rows, rows), :] = x_refs[p][...]
            cs_ref[pl.ds(p * rows, rows), :] = c_refs[p][...]

    gate, up, down = gate_ref[0], up_ref[0], down_ref[0]
    x, c = xs_ref[...], cs_ref[...]
    weight = jnp.broadcast_to(w_ref[0], (LANES, x.shape[0])).T
    weight = jnp.concatenate([weight] * (gate.shape[1] // LANES), 1)
    gate_lin, up_lin = dot(x, gate), dot(x, up)
    sig = 1.0 / (1.0 + jnp.exp(-gate_lin))
    silu = gate_lin * sig
    h_ref[...] = (weight * silu * up_lin).astype(BF)
    grad_hidden = weight * dot_nt(c, down)
    du_ref[...] = (grad_hidden * silu).astype(BF)
    dg_ref[...] = (grad_hidden * up_lin * (sig + silu * (1.0 - sig))).astype(BF)
    out = dot(h_ref[...], down)
    dx = dot_nt(dg_ref[...], gate) + dot_nt(du_ref[...], up)

    @pl.when(j == 0)
    def _():
        out_acc[...] = out
        dx_acc[...] = dx

    @pl.when(j > 0)
    def _():
        for p in range(parts):
            at = pl.ds(p * rows, rows)
            out_refs[p][...] = (out_acc[at, :] + out[p * rows : (p + 1) * rows]).astype(BF)
            dx_refs[p][...] = (dx_acc[at, :] + dx[p * rows : (p + 1) * rows]).astype(BF)


def moe_block(k, count, xs_in, cs_in, weight, gate, up, down, kept):
    parts = len(xs_in)
    rows, width = xs_in[0].shape
    m = parts * rows
    experts, _, ff = gate.shape
    alone = pl.BlockSpec((rows, width), lambda j: (0, 0))
    wide = pl.BlockSpec((m, width), lambda j: (k, 0))
    narrow = pl.BlockSpec((m, ff), lambda j: (k, j))
    tall = pl.BlockSpec((1, width, ff), lambda j: (j, 0, 0))
    row = jax.ShapeDtypeStruct((rows, width), BF)
    xs = jax.ShapeDtypeStruct((count * m, width), BF)
    hs = jax.ShapeDtypeStruct((count * m, experts * ff), BF)
    outs = pl.pallas_call(
        functools.partial(moe_kernel, parts=parts),
        out_shape=(row,) * (2 * parts) + (xs, xs, hs, hs, hs),
        grid=(experts,),
        in_specs=[alone] * (2 * parts)
        + [
            pl.BlockSpec((1, 1, m), lambda j: (j, 0, 0)),
            tall,
            tall,
            pl.BlockSpec((1, ff, width), lambda j: (j, 0, 0)),
        ]
        + [pl.BlockSpec(memory_space=pl.ANY)] * len(kept),
        out_specs=[alone] * (2 * parts) + [wide, wide, narrow, narrow, narrow],
        scratch_shapes=[pltpu.VMEM((m, width), F32), pltpu.VMEM((m, width), F32)],
        input_output_aliases={2 * parts + 4 + i: 2 * parts + i for i in range(len(kept))},
        cost_estimate=cost(13),
        name="moe_block",
    )(*xs_in, *cs_in, weight, gate, up, down, *kept)
    return outs[:parts], outs[parts : 2 * parts], outs[2 * parts :]


def expert_grad_kernel(expert_ref, x_ref, dg_ref, du_ref, h_ref, c_ref, out_ref, *, tall, ff):
    i = pl.program_id(0)

    @pl.when(i < tall)
    def _():
        out_ref[:, :ff] = dot_tn(x_ref[...], dg_ref[...]).astype(BF)
        out_ref[:, ff:] = dot_tn(x_ref[...], du_ref[...]).astype(BF)

    @pl.when(i >= tall)
    def _():
        out_ref[...] = dot_tn(h_ref[...], c_ref[...]).astype(BF)


def expert_grad(e, xs, cs, hs, dgs, dus, ff):
    m, width = xs.shape
    block = 256
    tall, steps = width // block, (width + ff) // block
    return pl.pallas_call(
        functools.partial(expert_grad_kernel, tall=tall, ff=ff),
        out_shape=jax.ShapeDtypeStruct((width + ff, width), BF),
        grid_spec=pltpu.PrefetchScalarGridSpec(
            num_scalar_prefetch=1,
            grid=(steps,),
            in_specs=[
                pl.BlockSpec((m, block), lambda i, s: (0, jnp.minimum(i, tall - 1))),
                pl.BlockSpec((m, ff), lambda i, s: (0, s[0])),
                pl.BlockSpec((m, ff), lambda i, s: (0, s[0])),
                pl.BlockSpec((m, block), lambda i, s: (0, s[0] * (ff // block) + jnp.maximum(i - tall, 0))),
                pl.BlockSpec((m, width), lambda i, s: (0, 0)),
            ],
            out_specs=pl.BlockSpec((block, width), lambda i, s: (i, 0)),
        ),
        cost_estimate=cost(13),
        name="expert_grad",
    )(e.astype(jnp.int32).reshape(1), xs, dgs, dus, hs, cs)


def qkv_grad_kernel(owner_ref, x_ref, g_ref, w_ref, part_ref, grad_ref, acc_ref, *, rows, sub):
    s = pl.program_id(0)
    span = x_ref.shape[1]
    shares = span // rows
    joint = []
    for g in range(g_ref.shape[0] // shares):
        units = [g_ref[g * shares + j] for j in range(shares)]
        joint.append(jnp.concatenate([unit[:rows] for unit in units], 0))
        if shares == 1:
            joint.append(units[0][rows:])
        else:
            joint.append(sum(unit[rows:].astype(F32) for unit in units).astype(BF))
    joint = jnp.concatenate(joint, 1)
    acc_ref[...] = jnp.where(s == 0, 0.0, acc_ref[...]) + dot_tn(x_ref[0], joint)
    back_ref = part_ref
    back = dot_nt(joint, w_ref[...]).astype(BF)
    for place in range(span // sub):
        slot = owner_ref[place]
        back_ref[slot, 0] = back[place * sub : (place + 1) * sub]

    @pl.when(s == pl.num_programs(0) - 1)
    def _():
        grad_ref[...] = acc_ref[...].astype(BF)


def qkv_grad(slot_at, normed_all, grad_pay, w_joint, rows, sub):
    seqs, span, width = normed_all.shape
    n, r, _ = grad_pay.shape
    cols = w_joint.shape[1]
    heads = span // sub
    return pl.pallas_call(
        functools.partial(qkv_grad_kernel, rows=rows, sub=sub),
        out_shape=(
            jax.ShapeDtypeStruct((heads, seqs, sub, width), BF),
            jax.ShapeDtypeStruct((width, cols), BF),
        ),
        grid_spec=pltpu.PrefetchScalarGridSpec(
            num_scalar_prefetch=1,
            grid=(seqs,),
            in_specs=[
                pl.BlockSpec((1, span, width), lambda s, o: (s, 0, 0)),
                pl.BlockSpec((n // seqs, r, LANES), lambda s, o: (s, 0, 0)),
                pl.BlockSpec((width, cols), lambda s, o: (0, 0)),
            ],
            out_specs=[
                pl.BlockSpec((heads, 1, sub, width), lambda s, o: (0, s, 0, 0)),
                pl.BlockSpec((width, cols), lambda s, o: (0, 0)),
            ],
            scratch_shapes=[pltpu.VMEM((width, cols), F32)],
        ),
        cost_estimate=cost(7),
        name="qkv_grad",
    )(slot_at, normed_all, grad_pay, w_joint)


def weight_kernel(owner_ref, *refs, tall, low):
    slots, (q_ref, k_ref, v_ref, o_ref) = refs[:-4], refs[-4:]
    cols = slots[0].shape[1]
    pieces = o_ref.shape[1] // cols
    short = low // pieces
    for i, slot in enumerate(slots):
        block = slot[...].astype(F32)
        at = pl.ds(pl.multiple_of(owner_ref[i] * tall, tall), tall)
        keys, values = [], []
        for g in range(cols // 256):
            q_ref[at, g * LANES : (g + 1) * LANES] = block[:tall, g * 256 : g * 256 + LANES]
            keys.append(block[:tall, g * 256 + LANES : g * 256 + LANES + HD])
            values.append(block[:tall, g * 256 + LANES + HD : (g + 1) * 256])
        k_ref[at, :] = jnp.concatenate(keys, 1)
        v_ref[at, :] = jnp.concatenate(values, 1)
        at = pl.ds(pl.multiple_of(owner_ref[i] * short, short), short)
        for p in range(pieces):
            o_ref[at, p * cols : (p + 1) * cols] = block[tall + p * short : tall + (p + 1) * short]


def weight_outputs(slots, owner, width, q_cols, k_cols, low):
    tall = width // len(slots)
    return pl.pallas_call(
        functools.partial(weight_kernel, tall=tall, low=low),
        out_shape=(
            jax.ShapeDtypeStruct((width, q_cols), F32),
            jax.ShapeDtypeStruct((width, k_cols), F32),
            jax.ShapeDtypeStruct((width, k_cols), F32),
            jax.ShapeDtypeStruct((q_cols, width), F32),
        ),
        in_specs=[pl.BlockSpec(memory_space=pltpu.SMEM)] + [pl.BlockSpec(memory_space=pltpu.VMEM)] * len(slots),
        out_specs=[pl.BlockSpec(memory_space=pltpu.VMEM)] * 4,
        cost_estimate=cost(3),
        name="weight_outputs",
    )(owner, *slots)


def per_device(
    hidden_in,
    norm_gain1,
    w_query,
    w_key,
    w_value,
    w_out,
    norm_gain2,
    expert_gate,
    expert_up,
    expert_down,
    routes,
    gate_weights,
    cotangent,
):
    seqs, sub, width = hidden_in.shape
    tokens = seqs * sub
    heads, ranks = lax.axis_size("head"), lax.axis_size("seq")
    kv_local = w_key.shape[1] // HD
    q_cols, k_cols = w_query.shape[1], w_key.shape[1]
    span = sub * heads
    total_len = span * ranks
    shares = ranks // (seqs * kv_local)
    rows = span // shares
    experts_local = expert_gate.shape[0]
    expert_total = experts_local * ranks
    capacity = tokens * TOP * 5 // (4 * expert_total)
    seq_rank = lax.axis_index("seq")
    head_rank = lax.axis_index("head")
    share = (seq_rank % shares).astype(jnp.int32).reshape(1)

    x_float = hidden_in.astype(F32)
    inv_one = lax.rsqrt(jnp.mean(x_float * x_float, -1, keepdims=True) + norm_eps)
    normed_one = (x_float * inv_one * norm_gain1).astype(BF)
    normed_all = in_order(gather_slots(normed_one, "head"), "head")
    normed_all = normed_all.transpose(1, 0, 2, 3).reshape(seqs, span, width)

    route_tok = routes.reshape(tokens, TOP)
    gate_tok = gate_weights.reshape(tokens, TOP)
    chosen = route_tok[:, :, None] == jnp.arange(expert_total, dtype=jnp.int32)
    named = jnp.any(chosen, 1)
    gate_of = jnp.sum(jnp.where(chosen, gate_tok[:, :, None], 0.0), 1)
    order = jnp.arange(tokens, dtype=jnp.int32)
    before = (order[:, None] > order[None, :]).astype(BF)
    rank_of = dot(before, named.astype(BF))
    weight_of = jnp.where(named & (rank_of < capacity), gate_of, 0.0)
    minor = minor_of("seq")
    major = ranks // minor
    weight_send = weight_of.reshape(tokens, ranks, experts_local).transpose(1, 2, 0)
    weight_all = lax.all_to_all(weight_send, "seq", 0, 0, tiled=True)
    weights = [
        jnp.concatenate([pick(weight_all, slot_owner("seq", a, b)) for b in range(minor)], 1)[:, None, :]
        for a in range(major)
    ]

    tables = [jnp.asarray(table) for table in angle_tables(span, 1) + angle_tables(ranks, span)]
    cot_value = cotangent.reshape(tokens, width)
    cot_line = [cot_value]
    for a in range(1, major - 1):
        cot_line.append(hop(cot_line[-1], "seq", 1, 0))
    cot_rows = [spread(cot_line[a], "seq") for a in range(major - 2)]
    normed_all = after(normed_all, cot_line[1], weight_all)
    pay, w_joint = project_qkv(normed_all, w_query, w_key, w_value, tables, seq_rank.astype(jnp.int32).reshape(1), rows)

    pay = after(pay, cot_line[-1], *[block for row in cot_rows for block in row])
    pay = lax.all_to_all(pay, "seq", 0, 0, tiled=True)
    w_full = in_order(gather_slots(after(w_out, normed_all), "head"), "head").reshape(heads * q_cols, width)
    cot_line.append(hop(after(cot_line[-1], pay), "seq", 1, 0))
    cot_rows.append(spread(after(cot_line[-2], pay), "seq"))
    attn, attn_t, lse = attn_fwd(after(pay, *weights), share, span)
    attn = after(attn, cot_line[-1], *cot_rows[-1])
    cot_rows.append(spread(cot_line[-1], "seq"))

    def to_tokens(value):
        if shares == 1:
            value = value.reshape(ranks * heads, sub, LANES)
            value = lax.all_to_all(value, ("seq", "head"), 0, 0, tiled=True)
            value = value.reshape(seqs, kv_local, heads, sub, LANES)
            return value.transpose(0, 3, 2, 1, 4)
        value = lax.all_to_all(value, "seq", 0, 0, tiled=True)
        value = value.reshape(seqs, kv_local, heads, sub, LANES).transpose(2, 0, 1, 3, 4)
        value = lax.all_to_all(value, "head", 0, 0, tiled=True)
        return value.transpose(1, 3, 0, 2, 4)

    def to_units(value):
        value = value.transpose(2, 0, 3, 1, 4)
        value = lax.all_to_all(value, "head", 0, 0, tiled=True)
        value = value.transpose(1, 2, 0, 3, 4).reshape(ranks, rows, LANES)
        return lax.all_to_all(value, "seq", 0, 0, tiled=True)

    attn_local = after(to_tokens(attn), w_full, *cot_rows[-1]).reshape(tokens, heads * q_cols)
    resid = x_float + dot(attn_local, w_full).reshape(seqs, sub, width)
    inv_two = lax.rsqrt(jnp.mean(resid * resid, -1, keepdims=True) + norm_eps)
    normed_two = (resid * inv_two * norm_gain2).astype(BF).reshape(tokens, width)

    def block(a, row, kept):
        return moe_block(
            a, major, row, cot_rows[a], weights[a], expert_gate, expert_up, expert_down, kept
        )

    row, value = join(spread(normed_two, "seq"), hop(normed_two, "seq", 1, 0))
    outs, kept, out_slots, grads = (), (), [], []
    for a in range(major - 1):
        if a + 2 < major:
            moved = hop(value, "seq", 1, 0)
        else:
            moved = ring_reduce(grads[1], "seq", 0, 1).astype(BF)
        coming = spread(value, "seq")
        outs, grad, kept = block(a, row, kept)
        row, value, outs, grad = join(coming, moved, outs, grad)
        out_slots.append(outs)
        grads.append(grad)
    total, grad_rows = value, {}
    ff = expert_gate.shape[2]
    my_y, my_core = place_of("head")
    experts = [1 - my_core, my_core]
    expert_sum = []
    for a in range(2, major + 1):
        moved = hop(total, "seq", 1, 0)
        slot = a % major
        came = ring_reduce(grads[slot], "seq", 0, 1).astype(BF)
        if a == 2:
            outs, grad, kept = block(major - 1, row, kept)
            moved, came, outs, grad = join(moved, came, outs, grad)
            out_slots.append(outs)
            grads.append(grad)
            total = add(moved, came).astype(BF)
            continue
        if len(expert_sum) < 2:
            xs, cs, hs, dgs, dus = kept
            part = expert_grad(experts[len(expert_sum)], after(xs, total), cs, hs, dgs, dus, ff)
            moved, came, part = join(moved, came, part)
            expert_sum.append(part)
        total = add(moved, came)
        if a < major:
            total = total.astype(BF)
    grad_normed_two = total.reshape(seqs, sub, width)
    grad_out = cotangent.astype(F32)
    grad_norm_two, gain_two_part = norm_backward(resid, inv_two, norm_gain2, grad_normed_two)
    grad_resid = grad_out + grad_norm_two
    grad_resid_b = grad_resid.astype(BF)
    if shares == 1:
        grad_attn_sent = grad_attn_units(grad_resid_b.reshape(tokens, width), w_full, seqs, heads, kv_local)
        grad_attn = lax.all_to_all(grad_attn_sent, ("seq", "head"), 0, 0, tiled=True).reshape(ranks, rows, LANES)
    else:
        grad_attn = dot_nt(grad_resid_b.reshape(tokens, width), w_full).astype(BF)
        grad_attn_sent = grad_attn.reshape(seqs, sub, heads, kv_local, LANES)
        grad_attn = to_units(grad_attn_sent)
    expert_sum = [value.reshape(heads // 2, -1, width) for value in expert_sum]

    halves = heads // 2
    other = hop(expert_sum[0], "head", 0, 1)
    mine = add(after(expert_sum[1], grad_attn_sent), other).astype(BF)
    got = [pick(mine, (my_y + d) % halves) for d in range(1, halves)]

    out_row = ring_reduce([after(block, grad_normed_two) for block in out_slots[1]], "seq", 0, 1).astype(BF)
    grad_attn, mine, out_row, got, out_slots = join(grad_attn, mine, out_row, got, out_slots)
    out_moved = hop(out_row, "seq", 1, 0)
    out_rows = [ring_reduce(out_slots[a], "seq", 0, 1).astype(BF) for a in range(2, major)]
    half = mine.shape[1] // 2
    early = [hop(value[:half], "head", d, 0) for d, value in enumerate(got, 1)]
    grad_pay = attn_bwd(pay, grad_attn, attn_t, lse, tables, share, span)
    grad_pay, out_moved, out_rows, early, got, out_slots = join(
        grad_pay, out_moved, out_rows, early, got, out_slots
    )
    out_rows.append(ring_reduce(out_slots[0], "seq", 0, 1).astype(BF))

    got_pay = lax.all_to_all(grad_pay, "seq", 0, 0, tiled=True)
    late = [hop(value[half:], "head", d, 0) for d, value in enumerate(got, 1)]
    part = pick(mine, my_y)
    parts = []
    for piece, moved in ((part[:half], early), (part[half:], late)):
        for value in moved:
            piece = add(piece, value)
        parts.append(piece.astype(BF))
    part = jnp.concatenate(parts, 0)
    expert_rows = [part] + [hop(part, "head", d, 0) for d in range(1, halves)]
    expert_slots = [[row, hop(row, "head", 0, 1)] for row in expert_rows]

    out_w_part = dot_tn(attn_local, after(grad_resid_b, grad_pay).reshape(tokens, width)).astype(BF)
    out_w_part = out_w_part.reshape(heads, q_cols, width)
    out_w_slots = [
        [pick(out_w_part, slot_owner("head", a, b)) for b in range(2)] for a in range(heads // 2)
    ]
    out_w = reduce_slots(out_w_slots, "head").astype(BF)

    my_a, my_b = place_of("seq")
    cols = w_joint.shape[1]
    out_w = out_w.reshape(minor, major, q_cols // ranks, width // cols, cols)
    out_w = out_w.transpose(0, 1, 3, 2, 4).reshape(minor, major, -1, cols)
    out_w = share_sum(out_w, "seq")

    out_total = add(out_moved, out_rows[0]).astype(BF)
    got_pay, part, out_total = join(got_pay, part, out_total)
    slot_at = [
        (my_y - place // 2) % halves * 2 + (my_core - place % 2) % 2 for place in range(heads)
    ]
    slot_at = jnp.stack(slot_at).astype(jnp.int32)
    grad_part, grad_w_joint = qkv_grad(slot_at, normed_all, got_pay, w_joint, rows, sub)

    value = grad_w_joint.reshape(minor, major, width // ranks, cols)
    out_total, value = join(out_total, value)
    out_moved = hop(out_total, "seq", 1, 0)
    total = pick(value, my_b)
    value = [hop(pick(value, (my_b + d) % minor), "seq", 0, d) for d in range(1, minor)]
    value, out_moved = join(value, out_moved)
    for moved in value:
        total = add(total, moved)
    total = line_sum(total.astype(BF), "seq")
    out_total = add(out_moved, out_rows[1]).astype(BF)
    part_slots = [[grad_part[a * 2 + b] for b in range(2)] for a in range(halves)]
    grad_normed_one = reduce_slots(part_slots, "head")
    grad_norm_one, gain_one_part = norm_backward(x_float, inv_one, norm_gain1, grad_normed_one)
    input_grad = (grad_resid + grad_norm_one).astype(BF)

    gains = small_sum(jnp.stack([gain_one_part, gain_two_part]), "head")
    gains = gains + sum(hop(gains, "seq", 0, d) for d in range(1, minor))
    gains = gains.astype(BF).reshape(-1, cols)
    low = out_w.shape[0]
    pad = jnp.zeros((16 - gains.shape[0] % 16, cols), BF)
    total = jnp.concatenate([total, out_w, gains, pad], 0)
    first = [total] + [hop(total, "seq", 0, d) for d in range(1, minor)]
    sums = [hop(total, "seq", d, 0) for d in range(1, major)]
    at = width // ranks + low
    gains = sum(row[at : at + gains.shape[0]].astype(F32) for row in [total] + sums).reshape(2, width)

    expert_slots = [[after(block, total) for block in row] for row in expert_slots]
    gate_total, up_total, down_total = expert_outputs(expert_slots, width, ff)
    rest = [hop(after(jnp.stack(sums), gate_total), "seq", 0, d) for d in range(1, minor)]
    weight_slots, weight_owner = list(first), [(my_b - d) % minor * major + my_a for d in range(minor)]
    for d in range(1, major):
        weight_slots += [sums[d - 1]] + [row[d - 1] for row in rest]
        weight_owner += [(my_b - b) % minor * major + (my_a - d) % major for b in range(minor)]
    weight_owner = jnp.stack(weight_owner).astype(jnp.int32)

    out_total = add(hop(after(out_total, gate_total), "seq", 1, 0), out_rows[-1])
    layer_out = (resid + out_total.reshape(seqs, sub, width)).astype(BF)
    query_total, key_total, value_total, w_out_total = weight_outputs(
        weight_slots, weight_owner, width, q_cols, k_cols, low
    )

    return (
        layer_out,
        input_grad,
        gains[0],
        query_total,
        key_total,
        value_total,
        w_out_total,
        gains[1],
        gate_total,
        up_total,
        down_total,
    )


def solution(mesh):
    return jax.shard_map(
        per_device,
        mesh=mesh,
        in_specs=(
            P(None, ("seq", "head"), None),
            P(),
            P(None, "head"),
            P(None, "head"),
            P(None, "head"),
            P("head", None),
            P(),
            P("seq", None, None),
            P("seq", None, None),
            P("seq", None, None),
            P(None, ("seq", "head"), None),
            P(None, ("seq", "head"), None),
            P(None, ("seq", "head"), None),
        ),
        out_specs=(
            P(None, ("seq", "head"), None),
            P(None, ("seq", "head"), None),
            P(),
            P(None, "head"),
            P(None, "head"),
            P(None, "head"),
            P("head", None),
            P(),
            P("seq", None, None),
            P("seq", None, None),
            P("seq", None, None),
        ),
        check_vma=False,
    )
```

```python
import functools
import math

import jax
import jax.numpy as jnp
import numpy as np
from jax import lax
from jax.experimental import pallas as pl
from jax.experimental.pallas import tpu as pltpu
from jax.sharding import PartitionSpec as P

HD = 64
TOP = 8
LANES = 128

norm_eps = 1e-06
rope_base = 10000.0
masked_value = -1e30
BF = jnp.bfloat16
F32 = jnp.float32


def cost(us):
    return pl.CostEstimate(flops=0, bytes_accessed=us * 3000000, transcendentals=0)


def attn_fwd_kernel(share_ref, pay_ref, out_ref, ot_ref, lse_ref, kv_ref, kvt_ref, *, span, rows, block):
    b = pl.program_id(0)
    count = pay_ref.shape[0]

    @pl.when(b == 0)
    def _():
        def fill(i, _):
            start = pl.multiple_of(i * span, span)
            tile = pay_ref[i, pl.ds(rows, span), :]
            kv_ref[pl.ds(start, span), :] = tile
            kvt_ref[:, pl.ds(start, span)] = tile.T
            return 0
        lax.fori_loop(0, count, fill, 0)

    q_start = b * span + share_ref[0] * rows
    qt = pay_ref[b, pl.ds(0, rows), :].T * jnp.bfloat16(0.125)
    qt = jnp.concatenate([qt[:HD], qt[HD:]], 1)
    qt = jnp.concatenate([qt, jnp.zeros_like(qt)], 0)
    last = (q_start + rows - 1) // block

    def step(kb, carry, masked):
        run_max, run_sum, acc = carry
        start = pl.multiple_of(kb * block, block)
        scores = jnp.dot(kv_ref[pl.ds(start, block), :], qt, preferred_element_type=jnp.float32)
        if masked:
            keys = start + lax.broadcasted_iota(jnp.int32, scores.shape, 0)
            queries = q_start + lax.broadcasted_iota(jnp.int32, scores.shape, 1) % rows
            scores = jnp.where(keys <= queries, scores, masked_value)
        new_max = jnp.maximum(run_max, jnp.max(scores, 0, keepdims=True))
        factor = jnp.exp(run_max - new_max)
        probs = jnp.exp(scores - new_max)
        run_sum = run_sum * factor + jnp.sum(probs, 0, keepdims=True)
        acc = acc * factor + jnp.dot(
            kvt_ref[pl.ds(HD, HD), pl.ds(start, block)], probs.astype(jnp.bfloat16), preferred_element_type=jnp.float32)
        return new_max, run_sum, acc

    carry = (jnp.full((1, 2 * rows), masked_value, jnp.float32), jnp.zeros((1, 2 * rows), jnp.float32), jnp.zeros((HD, 2 * rows), jnp.float32))
    carry = lax.fori_loop(0, last, functools.partial(step, masked=False), carry)
    run_max, run_sum, acc = step(last, carry, True)
    ot = acc / run_sum
    ot_ref[0] = ot
    lse_ref[0] = jnp.broadcast_to(run_max + jnp.log(run_sum), lse_ref.shape[1:])
    out_ref[0] = jnp.concatenate([ot[:, :rows], ot[:, rows:]], 0).T.astype(jnp.bfloat16)

def attn_fwd(pay, share, span, block=512):
    n, r, _ = pay.shape
    rows = r - span
    total = n * span
    block = min(block, total)
    return pl.pallas_call(
        functools.partial(attn_fwd_kernel, span=span, rows=rows, block=block),
        out_shape=(jax.ShapeDtypeStruct((n, rows, 128), jnp.bfloat16), jax.ShapeDtypeStruct((n, HD, 2 * rows), jnp.float32), jax.ShapeDtypeStruct((n, 8, 2 * rows), jnp.float32)),
        grid_spec=pltpu.PrefetchScalarGridSpec(
            num_scalar_prefetch=1, grid=(n,),
            in_specs=[pl.BlockSpec((n, r, 128), lambda b, s: (0, 0, 0))],
            out_specs=[pl.BlockSpec((1, rows, 128), lambda b, s: (b, 0, 0)), pl.BlockSpec((1, HD, 2 * rows), lambda b, s: (b, 0, 0)), pl.BlockSpec((1, 8, 2 * rows), lambda b, s: (b, 0, 0))],
            scratch_shapes=[pltpu.VMEM((total, 128), jnp.bfloat16), pltpu.VMEM((128, total), jnp.bfloat16)],
        ),
        cost_estimate=cost(16),
        name="attn_fwd",
    )(share, pay)

def swap_halves(v):
    lane = lax.broadcasted_iota(jnp.int32, v.shape, v.ndim - 1)
    return jnp.where(lane % HD < HD // 2, pltpu.roll(v, 128 - HD // 2, v.ndim - 1), pltpu.roll(v, HD // 2, v.ndim - 1))

def attn_bwd_kernel(share_ref, pay_ref, go_ref, ot_ref, lse_ref, *refs, span, rows, block):
    tables, (out_ref, kv_ref, kvt_ref, dk_ref, dv_ref) = refs[:4], refs[4:]
    b = pl.program_id(0)
    count = pay_ref.shape[0]

    @pl.when(b == 0)
    def _():
        def fill(i, _):
            start = pl.multiple_of(i * span, span)
            tile = pay_ref[i, pl.ds(rows, span), :]
            kv_ref[pl.ds(start, span), :] = tile
            kvt_ref[:, pl.ds(start, span)] = tile.T
            return 0
        lax.fori_loop(0, count, fill, 0)
        dk_ref[...] = jnp.zeros_like(dk_ref)
        dv_ref[...] = jnp.zeros_like(dv_ref)

    q_start = b * span + share_ref[0] * rows
    low = lax.broadcasted_iota(jnp.int32, (rows, 128), 1) < HD
    q01 = pay_ref[b, pl.ds(0, rows), :] * jnp.bfloat16(0.125)
    go01 = go_ref[0]
    zero = jnp.zeros_like(q01)
    q_rows = jnp.concatenate([jnp.where(low, q01, zero), jnp.where(low, zero, q01)], 0)
    go_rows = jnp.concatenate([jnp.where(low, go01, zero), jnp.where(low, zero, go01)], 0)
    qt = q01.T
    qt = jnp.concatenate([qt[:HD], qt[HD:]], 1)
    qt = jnp.concatenate([qt, jnp.zeros_like(qt)], 0)
    gt = go01.T
    gt = jnp.concatenate([gt[:HD], gt[HD:]], 1)
    delta = jnp.sum(gt.astype(jnp.float32) * ot_ref[0], 0, keepdims=True)
    gt = jnp.concatenate([jnp.zeros_like(gt), gt], 0)
    lse = lse_ref[0, 0:1, :]
    last = (q_start + rows - 1) // block

    def step(kb, dq, masked):
        start = pl.multiple_of(kb * block, block)
        kv = kv_ref[pl.ds(start, block), :]
        scores = jnp.dot(kv, qt, preferred_element_type=jnp.float32)
        probs = jnp.exp(scores - lse)
        if masked:
            keys = start + lax.broadcasted_iota(jnp.int32, scores.shape, 0)
            queries = q_start + lax.broadcasted_iota(jnp.int32, scores.shape, 1) % rows
            probs = jnp.where(keys <= queries, probs, 0.0)
        dprobs = jnp.dot(kv, gt, preferred_element_type=jnp.float32)
        dscores = (probs * (dprobs - delta)).astype(jnp.bfloat16)
        dv_ref[pl.ds(start, block), :] += jnp.dot(probs.astype(jnp.bfloat16), go_rows, preferred_element_type=jnp.float32)
        dk_ref[pl.ds(start, block), :] += jnp.dot(dscores, q_rows, preferred_element_type=jnp.float32)
        return dq + jnp.dot(kvt_ref[pl.ds(0, HD), pl.ds(start, block)], dscores, preferred_element_type=jnp.float32)

    dq = lax.fori_loop(0, last, functools.partial(step, masked=False), jnp.zeros((HD, 2 * rows), jnp.float32))
    dq = step(last, dq, True)
    dq = jnp.concatenate([dq[:, :rows], dq[:, rows:]], 0).T * 0.125
    cosine, sine = turned(tables, pl.ds(pl.multiple_of(share_ref[0] * rows, rows), rows), b)
    dq = dq * cosine - swap_halves(dq) * sine
    out_ref[b, pl.ds(0, rows), :] = dq.astype(jnp.bfloat16)

    @pl.when(b == count - 1)
    def _():
        def drain(i, _):
            start = pl.multiple_of(i * span, span)
            dk = dk_ref[pl.ds(start, span), :]
            dk = dk + pltpu.roll(dk, HD, 1)
            cosine, sine = turned(tables, pl.ds(0, span), i)
            dk = dk * cosine - swap_halves(dk) * sine
            dv = dv_ref[pl.ds(start, span), :]
            dv = dv + pltpu.roll(dv, HD, 1)
            lane = lax.broadcasted_iota(jnp.int32, dk.shape, 1)
            out_ref[i, pl.ds(rows, span), :] = jnp.where(lane < HD, dk, dv).astype(jnp.bfloat16)
            return 0
        lax.fori_loop(0, count, drain, 0)

def attn_bwd(pay, go, ot, lse, tables, share, span, block=512):
    n, r, _ = pay.shape
    rows = r - span
    total = n * span
    block = min(block, total)
    whole = lambda *shape: pl.BlockSpec(shape, lambda b, s: (0,) * len(shape))
    return pl.pallas_call(
        functools.partial(attn_bwd_kernel, span=span, rows=rows, block=block),
        out_shape=jax.ShapeDtypeStruct((n, r, 128), jnp.bfloat16),
        grid_spec=pltpu.PrefetchScalarGridSpec(
            num_scalar_prefetch=1, grid=(n,),
            in_specs=[whole(n, r, 128), pl.BlockSpec((1, rows, 128), lambda b, s: (b, 0, 0)), pl.BlockSpec((1, HD, 2 * rows), lambda b, s: (b, 0, 0)), pl.BlockSpec((1, 8, 2 * rows), lambda b, s: (b, 0, 0)), *[whole(*table.shape) for table in tables]],
            out_specs=whole(n, r, 128),
            scratch_shapes=[pltpu.VMEM((total, 128), jnp.bfloat16), pltpu.VMEM((128, total), jnp.bfloat16), pltpu.VMEM((total, 128), jnp.float32), pltpu.VMEM((total, 128), jnp.float32)],
        ),
        cost_estimate=cost(24),
        name="attn_bwd",
    )(share, pay, go, ot, lse, *tables)

def angle_tables(count, step):
    half = HD // 2
    angles = step * np.arange(count)[:, None] * rope_base ** (-2.0 * np.arange(half) / HD)
    cosine, sine = np.cos(angles), np.sin(angles)
    tables = np.concatenate([cosine] * 4, 1), np.concatenate([-sine, sine] * 2, 1)
    return [table.astype(np.float32) for table in tables]


def turned(tables, at, far):
    cos_ref, sin_ref, cos_far_ref, sin_far_ref = tables
    cosine, sine = cos_ref[at, :], sin_ref[at, :]
    cos_far, sin_far = cos_far_ref[pl.ds(far, 1), :], sin_far_ref[pl.ds(far, 1), :]
    return cosine * cos_far - sine * sin_far, sine * cos_far + cosine * sin_far


def dot(left, right):
    return jnp.dot(left, right, preferred_element_type=F32)


def dot_nt(left, right):
    return lax.dot_general(left, right, (((1,), (1,)), ((), ())), preferred_element_type=F32)


def dot_tn(left, right):
    return lax.dot_general(left, right, (((0,), (0,)), ((), ())), preferred_element_type=F32)


def qkv_kernel(rank_ref, x_ref, wq_ref, wk_ref, wv_ref, *refs, rows):
    tables, (out_ref, w_ref, cos_own, sin_own) = refs[:4], refs[4:]
    span = x_ref.shape[1]
    shares = span // rows
    groups = wk_ref.shape[1] // HD

    @pl.when(pl.program_id(0) == 0)
    def _():
        for g in range(groups):
            w_ref[:, g * 256 : g * 256 + LANES] = wq_ref[:, g * LANES : (g + 1) * LANES]
            pair = [wk_ref[:, g * HD : (g + 1) * HD], wv_ref[:, g * HD : (g + 1) * HD]]
            w_ref[:, g * 256 + LANES : (g + 1) * 256] = jnp.concatenate(pair, 1)
        cos_own[...], sin_own[...] = turned(tables, pl.ds(0, span), rank_ref[0])

    joint = jnp.dot(x_ref[0], w_ref[...], preferred_element_type=F32)
    low = lax.broadcasted_iota(jnp.int32, (span, LANES), 1) < HD
    cosine, sine = cos_own[...], sin_own[...]
    for g in range(groups):
        query = joint[:, g * 256 : g * 256 + LANES]
        other = joint[:, g * 256 + LANES : (g + 1) * 256]
        query = (query * cosine + swap_halves(query) * sine).astype(BF)
        other = jnp.where(low, other * cosine + swap_halves(other) * sine, other).astype(BF)
        for j in range(shares):
            out_ref[g * shares + j, pl.ds(0, rows), :] = query[j * rows : (j + 1) * rows]
            out_ref[g * shares + j, pl.ds(rows, span), :] = other


def project_qkv(normed_all, w_query, w_key, w_value, tables, rank, rows):
    seqs, span, width = normed_all.shape
    q_cols, k_cols = w_query.shape[1], w_key.shape[1]
    cols = q_cols + 2 * k_cols
    units = cols // 256 * (span // rows)
    fixed = lambda *shape: pl.BlockSpec(shape, lambda s, r: (0,) * len(shape))
    return pl.pallas_call(
        functools.partial(qkv_kernel, rows=rows),
        out_shape=(
            jax.ShapeDtypeStruct((seqs * units, rows + span, LANES), BF),
            jax.ShapeDtypeStruct((width, cols), BF),
        ),
        grid_spec=pltpu.PrefetchScalarGridSpec(
            num_scalar_prefetch=1,
            grid=(seqs,),
            in_specs=[
                pl.BlockSpec((1, span, width), lambda s, r: (s, 0, 0)),
                fixed(width, q_cols),
                fixed(width, k_cols),
                fixed(width, k_cols),
                *[fixed(*table.shape) for table in tables],
            ],
            out_specs=[pl.BlockSpec((units, rows + span, LANES), lambda s, r: (s, 0, 0)), fixed(width, cols)],
            scratch_shapes=[pltpu.VMEM((span, LANES), F32), pltpu.VMEM((span, LANES), F32)],
        ),
        cost_estimate=cost(6),
        name="project_qkv",
    )(rank, normed_all, w_query, w_key, w_value, *tables)


def grad_attn_kernel(g_ref, w_ref, out_ref, *, seqs, heads, groups):
    sub = g_ref.shape[0] // seqs
    grad = dot_nt(g_ref[...], w_ref[...]).astype(BF)
    for h in range(heads):
        for g in range(groups):
            at = (h * groups + g) * LANES
            for s in range(seqs):
                out_ref[(s * groups + g) * heads + h] = grad[s * sub : (s + 1) * sub, at : at + LANES]


def grad_attn_units(grad, w_full, seqs, heads, groups):
    tokens, width = grad.shape
    return pl.pallas_call(
        functools.partial(grad_attn_kernel, seqs=seqs, heads=heads, groups=groups),
        out_shape=jax.ShapeDtypeStruct((seqs * groups * heads, tokens // seqs, LANES), BF),
        in_specs=[pl.BlockSpec(memory_space=pltpu.VMEM)] * 2,
        out_specs=pl.BlockSpec(memory_space=pltpu.VMEM),
        cost_estimate=cost(3),
        name="grad_attn_units",
    )(grad, w_full)


def minor_of(axis):
    return 2 if axis == "head" or lax.axis_size(axis) < 16 else 4


def place_of(axis):
    minor = minor_of(axis)
    index = lax.axis_index(axis)
    return index // minor, index % minor


def hop(value, axis, da, db):
    n, minor = lax.axis_size(axis), minor_of(axis)
    major = n // minor
    pairs = [
        (a * minor + b, (a + da) % major * minor + (b + db) % minor)
        for a in range(major)
        for b in range(minor)
    ]
    return lax.ppermute(value, axis, pairs)


def after(value, *others):
    return lax.optimization_barrier((value,) + others)[0]


def gather_slots(value, axis):
    slots = [spread(value, axis)]
    for _ in range(1, lax.axis_size(axis) // minor_of(axis)):
        slots.append(spread(hop(slots[-1][0], axis, 1, 0), axis))
    return slots


def join(*values):
    return lax.optimization_barrier(values)


def spread(value, axis):
    row = [value]
    for _ in range(1, minor_of(axis)):
        row.append(hop(row[-1], axis, 0, 1))
    return row


def slot_owner(axis, a, b):
    minor = minor_of(axis)
    major = lax.axis_size(axis) // minor
    my_a, my_b = place_of(axis)
    return (my_a - a) % major * minor + (my_b - b) % minor


def add(x, y):
    return x.astype(F32) + y.astype(F32)


def ring_moved(parts, axis, da, db):
    total = parts[1 % len(parts)]
    for part in parts[2:]:
        total = add(hop(total, axis, da, db), part).astype(BF)
    return hop(total, axis, da, db)


def ring_reduce(parts, axis, da, db):
    return add(ring_moved(parts, axis, da, db), parts[0])


def pick(value, index):
    return lax.dynamic_index_in_dim(value, index, 0, keepdims=False)


def small_sum(value, axis):
    minor = minor_of(axis)
    major = lax.axis_size(axis) // minor
    value = value + sum(hop(value, axis, 0, d) for d in range(1, minor))
    return value + sum(hop(value, axis, d, 0) for d in range(1, major))


def expert_kernel(owner_ref, *refs, halves, steps, tall):
    slots, (gate_ref, up_ref, down_ref) = refs[: len(refs) - 3], refs[len(refs) - 3 :]
    e, y, k = pl.program_id(0), pl.program_id(1), pl.program_id(2)
    row = y * steps + k
    for i, slot in enumerate(slots):

        @pl.when(owner_ref[i] == e * halves + y)
        def _():
            block = slot[...].astype(F32)
            half = block.shape[1] // 2

            @pl.when(row < tall)
            def _():
                gate_ref[0] = block[:, :half]
                up_ref[0] = block[:, half:]

            @pl.when(row >= tall)
            def _():
                down_ref[0] = block


def expert_outputs(slots, width, ff):
    my_a, my_b = place_of("head")
    halves, experts = len(slots), len(slots[0])
    flat = [block for row in slots for block in row]
    owner = [
        (my_b - b) % experts * halves + (my_a - a) % halves
        for a in range(halves)
        for b in range(experts)
    ]
    owner = jnp.stack(owner).astype(jnp.int32)
    block = math.gcd(flat[0].shape[0], 256)
    steps, tall = flat[0].shape[0] // block, width // block

    def spec(i):
        def place(e, y, k, owner):
            turn = owner[i] - (e * halves + y)
            return (jnp.where(turn == 0, k, jnp.where(turn > 0, 0, steps - 1)), 0)

        return pl.BlockSpec((block, width), place)

    return pl.pallas_call(
        functools.partial(expert_kernel, halves=halves, steps=steps, tall=tall),
        out_shape=(
            jax.ShapeDtypeStruct((experts, width, ff), F32),
            jax.ShapeDtypeStruct((experts, width, ff), F32),
            jax.ShapeDtypeStruct((experts, ff, width), F32),
        ),
        grid_spec=pltpu.PrefetchScalarGridSpec(
            num_scalar_prefetch=1,
            grid=(experts, halves, steps),
            in_specs=[spec(i) for i in range(len(flat))],
            out_specs=[
                pl.BlockSpec((1, block, ff), lambda e, y, k, o: (e, jnp.minimum(y * steps + k, tall - 1), 0)),
                pl.BlockSpec((1, block, ff), lambda e, y, k, o: (e, jnp.minimum(y * steps + k, tall - 1), 0)),
                pl.BlockSpec((1, block, width), lambda e, y, k, o: (e, jnp.maximum(y * steps + k - tall, 0), 0)),
            ],
        ),
        cost_estimate=cost(12),
        name="expert_outputs",
    )(owner, *flat)


def in_order(slots, axis, by_minor=False):
    major, minor = len(slots), len(slots[0])
    whole = jnp.zeros((major * minor,) + slots[0][0].shape, slots[0][0].dtype)
    for a, row in enumerate(slots):
        for b, block in enumerate(row):
            owner = slot_owner(axis, a, b)
            if by_minor:
                owner = owner % minor * major + owner // minor
            whole = lax.dynamic_update_index_in_dim(whole, block, owner, 0)
    return whole


def norm_backward(values, inv_root, gain_vec, grad_normed):
    weighted = grad_normed * gain_vec
    gain_part = jnp.sum(grad_normed * values * inv_root, (0, 1))
    grad_values = inv_root * weighted - values * (inv_root * inv_root * inv_root) * jnp.mean(
        values * weighted, -1, keepdims=True
    )
    return (grad_values, gain_part)


def moe_kernel(*refs, parts):
    x_refs, c_refs = refs[:parts], refs[parts : 2 * parts]
    w_ref, gate_ref, up_ref, down_ref = refs[2 * parts : 2 * parts + 4]
    xs_ref, cs_ref, h_ref, dg_ref, du_ref, out_acc, dx_acc = refs[-7:]
    out_refs, dx_refs = refs[-7 - 2 * parts : -7 - parts], refs[-7 - parts : -7]
    j = pl.program_id(0)
    rows = x_refs[0].shape[0]

    @pl.when(j == 0)
    def _():
        for p in range(parts):
            xs_ref[pl.ds(p * rows, rows), :] = x_refs[p][...]
            cs_ref[pl.ds(p * rows, rows), :] = c_refs[p][...]

    gate, up, down = gate_ref[0], up_ref[0], down_ref[0]
    x, c = xs_ref[...], cs_ref[...]
    weight = jnp.broadcast_to(w_ref[0], (LANES, x.shape[0])).T
    weight = jnp.concatenate([weight] * (gate.shape[1] // LANES), 1)
    gate_lin, up_lin = dot(x, gate), dot(x, up)
    sig = 1.0 / (1.0 + jnp.exp(-gate_lin))
    silu = gate_lin * sig
    h_ref[...] = (weight * silu * up_lin).astype(BF)
    grad_hidden = weight * dot_nt(c, down)
    du_ref[...] = (grad_hidden * silu).astype(BF)
    dg_ref[...] = (grad_hidden * up_lin * (sig + silu * (1.0 - sig))).astype(BF)
    out = dot(h_ref[...], down)
    dx = dot_nt(dg_ref[...], gate) + dot_nt(du_ref[...], up)

    @pl.when(j == 0)
    def _():
        out_acc[...] = out
        dx_acc[...] = dx

    @pl.when(j > 0)
    def _():
        for p in range(parts):
            at = pl.ds(p * rows, rows)
            out_refs[p][...] = (out_acc[at, :] + out[p * rows : (p + 1) * rows]).astype(BF)
            dx_refs[p][...] = (dx_acc[at, :] + dx[p * rows : (p + 1) * rows]).astype(BF)


def moe_block(k, count, xs_in, cs_in, weight, gate, up, down, kept):
    parts = len(xs_in)
    rows, width = xs_in[0].shape
    m = parts * rows
    experts, _, ff = gate.shape
    alone = pl.BlockSpec((rows, width), lambda j: (0, 0))
    wide = pl.BlockSpec((m, width), lambda j: (k, 0))
    narrow = pl.BlockSpec((m, ff), lambda j: (k, j))
    tall = pl.BlockSpec((1, width, ff), lambda j: (j, 0, 0))
    row = jax.ShapeDtypeStruct((rows, width), BF)
    xs = jax.ShapeDtypeStruct((count * m, width), BF)
    hs = jax.ShapeDtypeStruct((count * m, experts * ff), BF)
    outs = pl.pallas_call(
        functools.partial(moe_kernel, parts=parts),
        out_shape=(row,) * (2 * parts) + (xs, xs, hs, hs, hs),
        grid=(experts,),
        in_specs=[alone] * (2 * parts)
        + [
            pl.BlockSpec((1, 1, m), lambda j: (j, 0, 0)),
            tall,
            tall,
            pl.BlockSpec((1, ff, width), lambda j: (j, 0, 0)),
        ]
        + [pl.BlockSpec(memory_space=pl.ANY)] * len(kept),
        out_specs=[alone] * (2 * parts) + [wide, wide, narrow, narrow, narrow],
        scratch_shapes=[pltpu.VMEM((m, width), F32), pltpu.VMEM((m, width), F32)],
        input_output_aliases={2 * parts + 4 + i: 2 * parts + i for i in range(len(kept))},
        cost_estimate=cost(13),
        name="moe_block",
    )(*xs_in, *cs_in, weight, gate, up, down, *kept)
    return outs[:parts], outs[parts : 2 * parts], outs[2 * parts :]


def expert_grad_kernel(expert_ref, x_ref, dg_ref, du_ref, h_ref, c_ref, out_ref, *, tall, ff):
    i = pl.program_id(0)

    @pl.when(i < tall)
    def _():
        out_ref[:, :ff] = dot_tn(x_ref[...], dg_ref[...]).astype(BF)
        out_ref[:, ff:] = dot_tn(x_ref[...], du_ref[...]).astype(BF)

    @pl.when(i >= tall)
    def _():
        out_ref[...] = dot_tn(h_ref[...], c_ref[...]).astype(BF)


def expert_grad(e, xs, cs, hs, dgs, dus, ff):
    m, width = xs.shape
    block = 256
    tall, steps = width // block, (width + ff) // block
    return pl.pallas_call(
        functools.partial(expert_grad_kernel, tall=tall, ff=ff),
        out_shape=jax.ShapeDtypeStruct((width + ff, width), BF),
        grid_spec=pltpu.PrefetchScalarGridSpec(
            num_scalar_prefetch=1,
            grid=(steps,),
            in_specs=[
                pl.BlockSpec((m, block), lambda i, s: (0, jnp.minimum(i, tall - 1))),
                pl.BlockSpec((m, ff), lambda i, s: (0, s[0])),
                pl.BlockSpec((m, ff), lambda i, s: (0, s[0])),
                pl.BlockSpec((m, block), lambda i, s: (0, s[0] * (ff // block) + jnp.maximum(i - tall, 0))),
                pl.BlockSpec((m, width), lambda i, s: (0, 0)),
            ],
            out_specs=pl.BlockSpec((block, width), lambda i, s: (i, 0)),
        ),
        cost_estimate=cost(13),
        name="expert_grad",
    )(e.astype(jnp.int32).reshape(1), xs, dgs, dus, hs, cs)


def qkv_grad_kernel(owner_ref, x_ref, g_ref, w_ref, *refs, rows, sub):
    part_refs, (grad_ref, acc_ref) = refs[:-2], refs[-2:]
    s = pl.program_id(0)
    span = x_ref.shape[1]
    shares = span // rows
    joint = []
    for g in range(g_ref.shape[0] // shares):
        units = [g_ref[g * shares + j] for j in range(shares)]
        joint.append(jnp.concatenate([unit[:rows] for unit in units], 0))
        if shares == 1:
            joint.append(units[0][rows:])
        else:
            joint.append(sum(unit[rows:].astype(F32) for unit in units).astype(BF))
    joint = jnp.concatenate(joint, 1)
    acc_ref[...] = jnp.where(s == 0, 0.0, acc_ref[...]) + dot_tn(x_ref[0], joint)
    back = dot_nt(joint, w_ref[...]).astype(BF)

    def give(part_ref, place):
        part_ref[0] = back[place * sub : (place + 1) * sub]

    for place in range(span // sub):
        for slot, part_ref in enumerate(part_refs):
            pl.when(owner_ref[place] == slot)(functools.partial(give, part_ref, place))

    @pl.when(s == pl.num_programs(0) - 1)
    def _():
        grad_ref[...] = acc_ref[...].astype(BF)


def qkv_grad(slot_at, normed_all, grad_pay, w_joint, rows, sub):
    seqs, span, width = normed_all.shape
    n, r, _ = grad_pay.shape
    cols = w_joint.shape[1]
    heads = span // sub
    return pl.pallas_call(
        functools.partial(qkv_grad_kernel, rows=rows, sub=sub),
        out_shape=(
            *[jax.ShapeDtypeStruct((seqs, sub, width), BF)] * heads,
            jax.ShapeDtypeStruct((width, cols), BF),
        ),
        grid_spec=pltpu.PrefetchScalarGridSpec(
            num_scalar_prefetch=1,
            grid=(seqs,),
            in_specs=[
                pl.BlockSpec((1, span, width), lambda s, o: (s, 0, 0)),
                pl.BlockSpec((n // seqs, r, LANES), lambda s, o: (s, 0, 0)),
                pl.BlockSpec((width, cols), lambda s, o: (0, 0)),
            ],
            out_specs=[
                *[pl.BlockSpec((1, sub, width), lambda s, o: (s, 0, 0))] * heads,
                pl.BlockSpec((width, cols), lambda s, o: (0, 0)),
            ],
            scratch_shapes=[pltpu.VMEM((width, cols), F32)],
        ),
        cost_estimate=cost(7),
        name="qkv_grad",
    )(slot_at, normed_all, grad_pay, w_joint)


def weight_kernel(owner_ref, *refs, tall, low):
    slots, (q_ref, k_ref, v_ref, o_ref) = refs[:-4], refs[-4:]
    cols = slots[0].shape[1]
    pieces = o_ref.shape[1] // cols
    short = low // pieces
    for i, slot in enumerate(slots):
        block = slot[...].astype(F32)
        at = pl.ds(pl.multiple_of(owner_ref[i] * tall, tall), tall)
        keys, values = [], []
        for g in range(cols // 256):
            q_ref[at, g * LANES : (g + 1) * LANES] = block[:tall, g * 256 : g * 256 + LANES]
            keys.append(block[:tall, g * 256 + LANES : g * 256 + LANES + HD])
            values.append(block[:tall, g * 256 + LANES + HD : (g + 1) * 256])
        k_ref[at, :] = jnp.concatenate(keys, 1)
        v_ref[at, :] = jnp.concatenate(values, 1)
        at = pl.ds(pl.multiple_of(owner_ref[i] * short, short), short)
        for p in range(pieces):
            o_ref[at, p * cols : (p + 1) * cols] = block[tall + p * short : tall + (p + 1) * short]


def weight_outputs(slots, owner, width, q_cols, k_cols, low):
    tall = width // len(slots)
    return pl.pallas_call(
        functools.partial(weight_kernel, tall=tall, low=low),
        out_shape=(
            jax.ShapeDtypeStruct((width, q_cols), F32),
            jax.ShapeDtypeStruct((width, k_cols), F32),
            jax.ShapeDtypeStruct((width, k_cols), F32),
            jax.ShapeDtypeStruct((q_cols, width), F32),
        ),
        in_specs=[pl.BlockSpec(memory_space=pltpu.SMEM)] + [pl.BlockSpec(memory_space=pltpu.VMEM)] * len(slots),
        out_specs=[pl.BlockSpec(memory_space=pltpu.VMEM)] * 4,
        cost_estimate=cost(3),
        name="weight_outputs",
    )(owner, *slots)


def per_device(
    hidden_in,
    norm_gain1,
    w_query,
    w_key,
    w_value,
    w_out,
    norm_gain2,
    expert_gate,
    expert_up,
    expert_down,
    routes,
    gate_weights,
    cotangent,
):
    seqs, sub, width = hidden_in.shape
    tokens = seqs * sub
    heads, ranks = lax.axis_size("head"), lax.axis_size("seq")
    kv_local = w_key.shape[1] // HD
    q_cols, k_cols = w_query.shape[1], w_key.shape[1]
    span = sub * heads
    total_len = span * ranks
    shares = ranks // (seqs * kv_local)
    rows = span // shares
    experts_local = expert_gate.shape[0]
    expert_total = experts_local * ranks
    capacity = tokens * TOP * 5 // (4 * expert_total)
    seq_rank = lax.axis_index("seq")
    head_rank = lax.axis_index("head")
    share = (seq_rank % shares).astype(jnp.int32).reshape(1)

    x_float = hidden_in.astype(F32)
    inv_one = lax.rsqrt(jnp.mean(x_float * x_float, -1, keepdims=True) + norm_eps)
    normed_one = (x_float * inv_one * norm_gain1).astype(BF)
    normed_all = in_order(gather_slots(normed_one, "head"), "head")
    normed_all = normed_all.transpose(1, 0, 2, 3).reshape(seqs, span, width)

    route_tok = routes.reshape(tokens, TOP)
    gate_tok = gate_weights.reshape(tokens, TOP)
    chosen = route_tok[:, :, None] == jnp.arange(expert_total, dtype=jnp.int32)
    named = jnp.any(chosen, 1)
    gate_of = jnp.sum(jnp.where(chosen, gate_tok[:, :, None], 0.0), 1)
    order = jnp.arange(tokens, dtype=jnp.int32)
    before = (order[:, None] > order[None, :]).astype(BF)
    rank_of = dot(before, named.astype(BF))
    weight_of = jnp.where(named & (rank_of < capacity), gate_of, 0.0)
    minor = minor_of("seq")
    major = ranks // minor
    weight_send = weight_of.reshape(tokens, ranks, experts_local).transpose(1, 2, 0)
    weight_all = lax.all_to_all(weight_send, "seq", 0, 0, tiled=True)
    weights = [
        jnp.concatenate([pick(weight_all, slot_owner("seq", a, b)) for b in range(minor)], 1)[:, None, :]
        for a in range(major)
    ]

    tables = [jnp.asarray(table) for table in angle_tables(span, 1) + angle_tables(ranks, span)]
    cot_value = cotangent.reshape(tokens, width)
    cot_line = [cot_value]
    for a in range(1, major - 1):
        cot_line.append(hop(cot_line[-1], "seq", 1, 0))
    cot_rows = [spread(cot_line[a], "seq") for a in range(major - 2)]
    normed_all = after(normed_all, cot_line[1], weight_all)
    pay, w_joint = project_qkv(normed_all, w_query, w_key, w_value, tables, seq_rank.astype(jnp.int32).reshape(1), rows)

    pay = after(pay, cot_line[-1], *[block for row in cot_rows for block in row])
    pay = lax.all_to_all(pay, "seq", 0, 0, tiled=True)
    w_full = in_order(gather_slots(after(w_out, normed_all), "head"), "head").reshape(heads * q_cols, width)
    cot_line.append(hop(after(cot_line[-1], pay), "seq", 1, 0))
    cot_rows.append(spread(after(cot_line[-2], pay), "seq"))
    attn, attn_t, lse = attn_fwd(after(pay, *weights), share, span)
    attn = after(attn, cot_line[-1], *cot_rows[-1])
    cot_rows.append(spread(cot_line[-1], "seq"))

    def to_tokens(value):
        if shares == 1:
            value = value.reshape(ranks * heads, sub, LANES)
            value = lax.all_to_all(value, ("seq", "head"), 0, 0, tiled=True)
            value = value.reshape(seqs, kv_local, heads, sub, LANES)
            return value.transpose(0, 3, 2, 1, 4)
        value = lax.all_to_all(value, "seq", 0, 0, tiled=True)
        value = value.reshape(seqs, kv_local, heads, sub, LANES).transpose(2, 0, 1, 3, 4)
        value = lax.all_to_all(value, "head", 0, 0, tiled=True)
        return value.transpose(1, 3, 0, 2, 4)

    def to_units(value):
        value = value.transpose(2, 0, 3, 1, 4)
        value = lax.all_to_all(value, "head", 0, 0, tiled=True)
        value = value.transpose(1, 2, 0, 3, 4).reshape(ranks, rows, LANES)
        return lax.all_to_all(value, "seq", 0, 0, tiled=True)

    attn_local = after(to_tokens(attn), w_full, *cot_rows[-1]).reshape(tokens, heads * q_cols)
    resid = x_float + dot(attn_local, w_full).reshape(seqs, sub, width)
    inv_two = lax.rsqrt(jnp.mean(resid * resid, -1, keepdims=True) + norm_eps)
    normed_two = (resid * inv_two * norm_gain2).astype(BF).reshape(tokens, width)

    def block(a, row, kept):
        return moe_block(
            a, major, row, cot_rows[a], weights[a], expert_gate, expert_up, expert_down, kept
        )

    row, value = join(spread(normed_two, "seq"), hop(normed_two, "seq", 1, 0))
    outs, kept, out_slots, grads = (), (), [], []
    for a in range(major - 1):
        if a + 2 < major:
            moved = hop(value, "seq", 1, 0)
        else:
            moved = ring_reduce(grads[1], "seq", 0, 1).astype(BF)
        if a + 2 < major:
            coming = spread(value, "seq")
        else:
            coming = [value] + [hop(other, "seq", 1, 0) for other in row[1:]]
        outs, grad, kept = block(a, row, kept)
        row, value, outs, grad = join(coming, moved, outs, grad)
        out_slots.append(outs)
        grads.append(grad)
    total, grad_rows = value, {}
    ff = expert_gate.shape[2]
    my_y, my_core = place_of("head")
    experts = [1 - my_core, my_core]
    expert_sum = []
    for a in range(2, major + 1):
        moved = hop(total, "seq", 1, 0)
        slot = a % major
        came = ring_reduce(grads[slot], "seq", 0, 1).astype(BF)
        if a == 2:
            outs, grad, kept = block(major - 1, row, kept)
            moved, came, outs, grad = join(moved, came, outs, grad)
            out_slots.append(outs)
            grads.append(grad)
            total = add(moved, came).astype(BF)
            continue
        if len(expert_sum) < 2:
            xs, cs, hs, dgs, dus = kept
            part = expert_grad(experts[len(expert_sum)], after(xs, total), cs, hs, dgs, dus, ff)
            if not expert_sum:
                moved, came, part = join(moved, came, part)
            expert_sum.append(part)
        total = add(moved, came)
        if a < major:
            total = total.astype(BF)
    grad_normed_two = total.reshape(seqs, sub, width)
    grad_out = cotangent.astype(F32)
    grad_norm_two, gain_two_part = norm_backward(resid, inv_two, norm_gain2, grad_normed_two)
    grad_resid = grad_out + grad_norm_two
    halves = heads // 2
    expert_sum = [value.reshape(halves, -1, width) for value in expert_sum]
    other = hop(expert_sum[0], "head", 0, 1)
    grad_resid_b = after(grad_resid.astype(BF), expert_sum[1])
    if shares == 1:
        grad_attn_sent = grad_attn_units(grad_resid_b.reshape(tokens, width), w_full, seqs, heads, kv_local)
        grad_attn = lax.all_to_all(grad_attn_sent, ("seq", "head"), 0, 0, tiled=True).reshape(ranks, rows, LANES)
    else:
        grad_attn = dot_nt(grad_resid_b.reshape(tokens, width), w_full).astype(BF)
        grad_attn_sent = grad_attn.reshape(seqs, sub, heads, kv_local, LANES)
        grad_attn = to_units(grad_attn_sent)
    out_near = ring_moved([after(block, grad_normed_two) for block in out_slots[1]], "seq", 0, 1)
    out_near = add(out_near, out_slots[1][0]).astype(BF)
    mine = add(after(expert_sum[1], grad_attn_sent), other).astype(BF)
    tall = mine.shape[1]
    cut = tall // 3

    def cut_of(index, start, size):
        return lax.dynamic_slice(mine, (index, start, 0), (1, size, width))[0]

    places = [(my_y + d) % halves for d in range(1, halves)]
    lower = [cut_of(place, cut, tall - cut) for place in places]
    upper = [cut_of(place, 0, cut) for place in places]
    grad_attn, out_near, out_slots, lower, upper = join(grad_attn, out_near, out_slots, lower, upper)
    lower = [hop(value, "head", d, 0) for d, value in enumerate(lower, 1)]

    out_moved = hop(out_near, "seq", 1, 0)
    out_rows = [ring_moved(out_slots[a], "seq", 0, 1) for a in range(2, major)]
    grad_pay = attn_bwd(pay, grad_attn, attn_t, lse, tables, share, span)
    grad_pay, out_moved, out_rows, lower, upper, mine, out_slots = join(
        grad_pay, out_moved, out_rows, lower, upper, mine, out_slots
    )
    upper = [hop(value, "head", d, 0) for d, value in enumerate(upper, 1)]

    my_a, my_b = place_of("seq")
    cols = w_joint.shape[1]
    got_pay = lax.all_to_all(grad_pay, "seq", 0, 0, tiled=True)
    out_last = ring_moved(out_slots[0], "seq", 0, 1)
    out_w_part = dot_tn(attn_local, after(grad_resid_b, grad_pay).reshape(tokens, width)).astype(BF)
    out_w_part = out_w_part.reshape(heads, q_cols, width)
    out_w = [
        ring_reduce([pick(out_w_part, slot_owner("head", a, b)) for b in range(2)], "head", 0, 1).astype(BF)
        for a in range(halves)
    ]
    out_w = ring_reduce(out_w, "head", 1, 0).astype(BF)
    part = pick(mine, my_y)
    for over, under in zip(upper, lower):
        part = add(part, jnp.concatenate([over, under], 0))
    part = after(part.astype(BF), out_w)
    out_w = out_w.reshape(minor, major, q_cols // ranks, width // cols, cols)
    out_w = out_w.transpose(0, 1, 3, 2, 4).reshape(minor, major, -1, cols)
    expert_rows = [hop(part, "head", d, 0) for d in range(1, halves)]
    out_total = (add(out_rows[0], out_slots[2][0]) + out_moved.astype(F32)).astype(BF)
    got_pay, part, out_last, out_w, out_total = join(got_pay, part, out_last, out_w, out_total)

    slot_at = [
        (my_y - place // 2) % halves * 2 + (my_core - place % 2) % 2 for place in range(heads)
    ]
    slot_at = jnp.stack(slot_at).astype(jnp.int32)
    *grad_part, grad_w_joint = qkv_grad(slot_at, normed_all, got_pay, w_joint, rows, sub)

    values = [grad_w_joint.reshape(minor, major, width // ranks, cols), out_w]
    came = [[hop(pick(value, (my_b + d) % minor), "seq", 0, d) for d in range(1, minor)] for value in values]
    out_moved = hop(out_total, "seq", 1, 0)
    part_rows = [
        ring_reduce([grad_part[a * 2 + b] for b in range(2)], "head", 0, 1).astype(BF) for a in range(halves)
    ]
    came, out_moved, part_rows, expert_rows = join(came, out_moved, part_rows, expert_rows)

    def summed(value, moved):
        for other in moved:
            value = add(value, other)
        return value.astype(BF)

    low = values[1].shape[2]
    total = jnp.concatenate([summed(pick(value, my_b), moved) for value, moved in zip(values, came)], 1)
    came = [hop(pick(total, (my_a + d) % major), "seq", d, 0) for d in range(1, major)]
    part_moved = ring_moved(part_rows, "head", 1, 0)
    expert_rows = [part] + expert_rows
    expert_slots = [[row, hop(row, "head", 0, 1)] for row in expert_rows]
    expert_totals = expert_outputs(expert_slots, width, ff)
    came, part_moved, expert_totals, total = join(came, part_moved, expert_totals, total)
    gate_total, up_total, down_total = expert_totals

    total = summed(pick(total, my_a), came)
    first = [hop(total, "seq", 0, d) for d in range(1, minor)]
    sums = [hop(total, "seq", d, 0) for d in range(1, major)]
    part_moved = after(part_moved, total)
    grad_normed_one = add(part_moved, part_rows[0])
    grad_norm_one, gain_one_part = norm_backward(x_float, inv_one, norm_gain1, grad_normed_one)
    gains = after(jnp.stack([gain_one_part, gain_two_part]), *first)
    gains = gains + sum(hop(gains, "seq", d, 0) for d in range(1, major))
    input_grad = (grad_resid + grad_norm_one).astype(BF)
    first, sums, out_total, gains, input_grad = join(
        first,
        sums,
        (add(out_rows[1], out_slots[3][0]) + out_moved.astype(F32)).astype(BF),
        gains,
        input_grad,
    )

    rest = [[hop(value, "seq", 0, d) for value in sums] for d in range(1, minor)]
    out_moved = hop(out_total, "seq", 1, 0)
    gains = small_sum(gains, "head")
    gains = gains + sum(hop(gains, "seq", 0, d) for d in range(1, minor))
    weight_slots = [total] + first
    weight_owner = [(my_b - d) % minor * major + my_a for d in range(minor)]
    for d in range(1, major):
        weight_slots += [sums[d - 1]] + [row[d - 1] for row in rest]
        weight_owner += [(my_b - b) % minor * major + (my_a - d) % major for b in range(minor)]
    weight_owner = jnp.stack(weight_owner).astype(jnp.int32)
    query_total, key_total, value_total, w_out_total = weight_outputs(
        weight_slots, weight_owner, width, q_cols, k_cols, low
    )
    out_total = add(out_last, out_slots[0][0]) + out_moved.astype(F32)
    layer_out = (resid + out_total.reshape(seqs, sub, width)).astype(BF)

    return (
        layer_out,
        input_grad,
        gains[0],
        query_total,
        key_total,
        value_total,
        w_out_total,
        gains[1],
        gate_total,
        up_total,
        down_total,
    )


def solution(mesh):
    return jax.shard_map(
        per_device,
        mesh=mesh,
        in_specs=(
            P(None, ("seq", "head"), None),
            P(),
            P(None, "head"),
            P(None, "head"),
            P(None, "head"),
            P("head", None),
            P(),
            P("seq", None, None),
            P("seq", None, None),
            P("seq", None, None),
            P(None, ("seq", "head"), None),
            P(None, ("seq", "head"), None),
            P(None, ("seq", "head"), None),
        ),
        out_specs=(
            P(None, ("seq", "head"), None),
            P(None, ("seq", "head"), None),
            P(),
            P(None, "head"),
            P(None, "head"),
            P(None, "head"),
            P("head", None),
            P(),
            P("seq", None, None),
            P("seq", None, None),
            P("seq", None, None),
        ),
        check_vma=False,
    )
```

```python
import functools
import math

import jax
import jax.numpy as jnp
import numpy as np
from jax import lax
from jax.experimental import pallas as pl
from jax.experimental.pallas import tpu as pltpu
from jax.sharding import PartitionSpec as P

HD = 64
TOP = 8
LANES = 128

norm_eps = 1e-06
rope_base = 10000.0
masked_value = -1e30
BF = jnp.bfloat16
F32 = jnp.float32


def cost(us):
    return pl.CostEstimate(flops=0, bytes_accessed=us * 3000000, transcendentals=0)


def attn_fwd_kernel(share_ref, pay_ref, out_ref, ot_ref, lse_ref, kv_ref, kvt_ref, *, span, rows, block):
    b = pl.program_id(0)
    count = pay_ref.shape[0]

    @pl.when(b == 0)
    def _():
        def fill(i, _):
            start = pl.multiple_of(i * span, span)
            tile = pay_ref[i, pl.ds(rows, span), :]
            kv_ref[pl.ds(start, span), :] = tile
            kvt_ref[:, pl.ds(start, span)] = tile.T
            return 0
        lax.fori_loop(0, count, fill, 0)

    q_start = b * span + share_ref[0] * rows
    qt = pay_ref[b, pl.ds(0, rows), :].T * jnp.bfloat16(0.125)
    qt = jnp.concatenate([qt[:HD], qt[HD:]], 1)
    qt = jnp.concatenate([qt, jnp.zeros_like(qt)], 0)
    last = (q_start + rows - 1) // block

    def step(kb, carry, masked):
        run_max, run_sum, acc = carry
        start = pl.multiple_of(kb * block, block)
        scores = jnp.dot(kv_ref[pl.ds(start, block), :], qt, preferred_element_type=jnp.float32)
        if masked:
            keys = start + lax.broadcasted_iota(jnp.int32, scores.shape, 0)
            queries = q_start + lax.broadcasted_iota(jnp.int32, scores.shape, 1) % rows
            scores = jnp.where(keys <= queries, scores, masked_value)
        new_max = jnp.maximum(run_max, jnp.max(scores, 0, keepdims=True))
        factor = jnp.exp(run_max - new_max)
        probs = jnp.exp(scores - new_max)
        run_sum = run_sum * factor + jnp.sum(probs, 0, keepdims=True)
        acc = acc * factor + jnp.dot(
            kvt_ref[pl.ds(HD, HD), pl.ds(start, block)], probs.astype(jnp.bfloat16), preferred_element_type=jnp.float32)
        return new_max, run_sum, acc

    carry = (jnp.full((1, 2 * rows), masked_value, jnp.float32), jnp.zeros((1, 2 * rows), jnp.float32), jnp.zeros((HD, 2 * rows), jnp.float32))
    carry = lax.fori_loop(0, last, functools.partial(step, masked=False), carry)
    run_max, run_sum, acc = step(last, carry, True)
    ot = acc / run_sum
    ot_ref[0] = ot
    lse_ref[0] = jnp.broadcast_to(run_max + jnp.log(run_sum), lse_ref.shape[1:])
    out_ref[0] = jnp.concatenate([ot[:, :rows], ot[:, rows:]], 0).T.astype(jnp.bfloat16)

def attn_fwd(pay, share, span, block=512):
    n, r, _ = pay.shape
    rows = r - span
    total = n * span
    block = min(block, total)
    return pl.pallas_call(
        functools.partial(attn_fwd_kernel, span=span, rows=rows, block=block),
        out_shape=(jax.ShapeDtypeStruct((n, rows, 128), jnp.bfloat16), jax.ShapeDtypeStruct((n, HD, 2 * rows), jnp.float32), jax.ShapeDtypeStruct((n, 8, 2 * rows), jnp.float32)),
        grid_spec=pltpu.PrefetchScalarGridSpec(
            num_scalar_prefetch=1, grid=(n,),
            in_specs=[pl.BlockSpec((n, r, 128), lambda b, s: (0, 0, 0))],
            out_specs=[pl.BlockSpec((1, rows, 128), lambda b, s: (b, 0, 0)), pl.BlockSpec((1, HD, 2 * rows), lambda b, s: (b, 0, 0)), pl.BlockSpec((1, 8, 2 * rows), lambda b, s: (b, 0, 0))],
            scratch_shapes=[pltpu.VMEM((total, 128), jnp.bfloat16), pltpu.VMEM((128, total), jnp.bfloat16)],
        ),
        cost_estimate=cost(16),
        name="attn_fwd",
    )(share, pay)

def swap_halves(v):
    lane = lax.broadcasted_iota(jnp.int32, v.shape, v.ndim - 1)
    return jnp.where(lane % HD < HD // 2, pltpu.roll(v, 128 - HD // 2, v.ndim - 1), pltpu.roll(v, HD // 2, v.ndim - 1))

def attn_bwd_kernel(share_ref, pay_ref, go_ref, ot_ref, lse_ref, *refs, span, rows, block):
    tables, (out_ref, kv_ref, kvt_ref, dk_ref, dv_ref) = refs[:4], refs[4:]
    b = pl.program_id(0)
    count = pay_ref.shape[0]

    @pl.when(b == 0)
    def _():
        def fill(i, _):
            start = pl.multiple_of(i * span, span)
            tile = pay_ref[i, pl.ds(rows, span), :]
            kv_ref[pl.ds(start, span), :] = tile
            kvt_ref[:, pl.ds(start, span)] = tile.T
            return 0
        lax.fori_loop(0, count, fill, 0)
        dk_ref[...] = jnp.zeros_like(dk_ref)
        dv_ref[...] = jnp.zeros_like(dv_ref)

    q_start = b * span + share_ref[0] * rows
    low = lax.broadcasted_iota(jnp.int32, (rows, 128), 1) < HD
    q01 = pay_ref[b, pl.ds(0, rows), :] * jnp.bfloat16(0.125)
    go01 = go_ref[0]
    zero = jnp.zeros_like(q01)
    q_rows = jnp.concatenate([jnp.where(low, q01, zero), jnp.where(low, zero, q01)], 0)
    go_rows = jnp.concatenate([jnp.where(low, go01, zero), jnp.where(low, zero, go01)], 0)
    qt = q01.T
    qt = jnp.concatenate([qt[:HD], qt[HD:]], 1)
    qt = jnp.concatenate([qt, jnp.zeros_like(qt)], 0)
    gt = go01.T
    gt = jnp.concatenate([gt[:HD], gt[HD:]], 1)
    delta = jnp.sum(gt.astype(jnp.float32) * ot_ref[0], 0, keepdims=True)
    gt = jnp.concatenate([jnp.zeros_like(gt), gt], 0)
    lse = lse_ref[0, 0:1, :]
    last = (q_start + rows - 1) // block

    def step(kb, dq, masked):
        start = pl.multiple_of(kb * block, block)
        kv = kv_ref[pl.ds(start, block), :]
        scores = jnp.dot(kv, qt, preferred_element_type=jnp.float32)
        probs = jnp.exp(scores - lse)
        if masked:
            keys = start + lax.broadcasted_iota(jnp.int32, scores.shape, 0)
            queries = q_start + lax.broadcasted_iota(jnp.int32, scores.shape, 1) % rows
            probs = jnp.where(keys <= queries, probs, 0.0)
        dprobs = jnp.dot(kv, gt, preferred_element_type=jnp.float32)
        dscores = (probs * (dprobs - delta)).astype(jnp.bfloat16)
        dv_ref[pl.ds(start, block), :] += jnp.dot(probs.astype(jnp.bfloat16), go_rows, preferred_element_type=jnp.float32)
        dk_ref[pl.ds(start, block), :] += jnp.dot(dscores, q_rows, preferred_element_type=jnp.float32)
        return dq + jnp.dot(kvt_ref[pl.ds(0, HD), pl.ds(start, block)], dscores, preferred_element_type=jnp.float32)

    dq = lax.fori_loop(0, last, functools.partial(step, masked=False), jnp.zeros((HD, 2 * rows), jnp.float32))
    dq = step(last, dq, True)
    dq = jnp.concatenate([dq[:, :rows], dq[:, rows:]], 0).T * 0.125
    cosine, sine = turned(tables, pl.ds(pl.multiple_of(share_ref[0] * rows, rows), rows), b)
    dq = dq * cosine - swap_halves(dq) * sine
    out_ref[b, pl.ds(0, rows), :] = dq.astype(jnp.bfloat16)

    @pl.when(b == count - 1)
    def _():
        def drain(i, _):
            start = pl.multiple_of(i * span, span)
            dk = dk_ref[pl.ds(start, span), :]
            dk = dk + pltpu.roll(dk, HD, 1)
            cosine, sine = turned(tables, pl.ds(0, span), i)
            dk = dk * cosine - swap_halves(dk) * sine
            dv = dv_ref[pl.ds(start, span), :]
            dv = dv + pltpu.roll(dv, HD, 1)
            lane = lax.broadcasted_iota(jnp.int32, dk.shape, 1)
            out_ref[i, pl.ds(rows, span), :] = jnp.where(lane < HD, dk, dv).astype(jnp.bfloat16)
            return 0
        lax.fori_loop(0, count, drain, 0)

def attn_bwd(pay, go, ot, lse, tables, share, span, block=512):
    n, r, _ = pay.shape
    rows = r - span
    total = n * span
    block = min(block, total)
    whole = lambda *shape: pl.BlockSpec(shape, lambda b, s: (0,) * len(shape))
    return pl.pallas_call(
        functools.partial(attn_bwd_kernel, span=span, rows=rows, block=block),
        out_shape=jax.ShapeDtypeStruct((n, r, 128), jnp.bfloat16),
        grid_spec=pltpu.PrefetchScalarGridSpec(
            num_scalar_prefetch=1, grid=(n,),
            in_specs=[whole(n, r, 128), pl.BlockSpec((1, rows, 128), lambda b, s: (b, 0, 0)), pl.BlockSpec((1, HD, 2 * rows), lambda b, s: (b, 0, 0)), pl.BlockSpec((1, 8, 2 * rows), lambda b, s: (b, 0, 0)), *[whole(*table.shape) for table in tables]],
            out_specs=whole(n, r, 128),
            scratch_shapes=[pltpu.VMEM((total, 128), jnp.bfloat16), pltpu.VMEM((128, total), jnp.bfloat16), pltpu.VMEM((total, 128), jnp.float32), pltpu.VMEM((total, 128), jnp.float32)],
        ),
        cost_estimate=cost(24),
        name="attn_bwd",
    )(share, pay, go, ot, lse, *tables)

def angle_tables(count, step):
    half = HD // 2
    angles = step * np.arange(count)[:, None] * rope_base ** (-2.0 * np.arange(half) / HD)
    cosine, sine = np.cos(angles), np.sin(angles)
    tables = np.concatenate([cosine] * 4, 1), np.concatenate([-sine, sine] * 2, 1)
    return [table.astype(np.float32) for table in tables]


def turned(tables, at, far):
    cos_ref, sin_ref, cos_far_ref, sin_far_ref = tables
    cosine, sine = cos_ref[at, :], sin_ref[at, :]
    cos_far, sin_far = cos_far_ref[pl.ds(far, 1), :], sin_far_ref[pl.ds(far, 1), :]
    return cosine * cos_far - sine * sin_far, sine * cos_far + cosine * sin_far


def dot(left, right):
    return jnp.dot(left, right, preferred_element_type=F32)


def dot_nt(left, right):
    return lax.dot_general(left, right, (((1,), (1,)), ((), ())), preferred_element_type=F32)


def dot_tn(left, right):
    return lax.dot_general(left, right, (((0,), (0,)), ((), ())), preferred_element_type=F32)


def qkv_kernel(rank_ref, x_ref, wq_ref, wk_ref, wv_ref, *refs, rows):
    tables, (out_ref, w_ref, cos_own, sin_own) = refs[:4], refs[4:]
    span = x_ref.shape[1]
    shares = span // rows
    groups = wk_ref.shape[1] // HD

    @pl.when(pl.program_id(0) == 0)
    def _():
        for g in range(groups):
            w_ref[:, g * 256 : g * 256 + LANES] = wq_ref[:, g * LANES : (g + 1) * LANES]
            pair = [wk_ref[:, g * HD : (g + 1) * HD], wv_ref[:, g * HD : (g + 1) * HD]]
            w_ref[:, g * 256 + LANES : (g + 1) * 256] = jnp.concatenate(pair, 1)
        cos_own[...], sin_own[...] = turned(tables, pl.ds(0, span), rank_ref[0])

    joint = jnp.dot(x_ref[0], w_ref[...], preferred_element_type=F32)
    low = lax.broadcasted_iota(jnp.int32, (span, LANES), 1) < HD
    cosine, sine = cos_own[...], sin_own[...]
    for g in range(groups):
        query = joint[:, g * 256 : g * 256 + LANES]
        other = joint[:, g * 256 + LANES : (g + 1) * 256]
        query = (query * cosine + swap_halves(query) * sine).astype(BF)
        other = jnp.where(low, other * cosine + swap_halves(other) * sine, other).astype(BF)
        for j in range(shares):
            out_ref[g * shares + j, pl.ds(0, rows), :] = query[j * rows : (j + 1) * rows]
            out_ref[g * shares + j, pl.ds(rows, span), :] = other


def project_qkv(normed_all, w_query, w_key, w_value, tables, rank, rows):
    seqs, span, width = normed_all.shape
    q_cols, k_cols = w_query.shape[1], w_key.shape[1]
    cols = q_cols + 2 * k_cols
    units = cols // 256 * (span // rows)
    fixed = lambda *shape: pl.BlockSpec(shape, lambda s, r: (0,) * len(shape))
    return pl.pallas_call(
        functools.partial(qkv_kernel, rows=rows),
        out_shape=(
            jax.ShapeDtypeStruct((seqs * units, rows + span, LANES), BF),
            jax.ShapeDtypeStruct((width, cols), BF),
        ),
        grid_spec=pltpu.PrefetchScalarGridSpec(
            num_scalar_prefetch=1,
            grid=(seqs,),
            in_specs=[
                pl.BlockSpec((1, span, width), lambda s, r: (s, 0, 0)),
                fixed(width, q_cols),
                fixed(width, k_cols),
                fixed(width, k_cols),
                *[fixed(*table.shape) for table in tables],
            ],
            out_specs=[pl.BlockSpec((units, rows + span, LANES), lambda s, r: (s, 0, 0)), fixed(width, cols)],
            scratch_shapes=[pltpu.VMEM((span, LANES), F32), pltpu.VMEM((span, LANES), F32)],
        ),
        cost_estimate=cost(6),
        name="project_qkv",
    )(rank, normed_all, w_query, w_key, w_value, *tables)


def grad_attn_kernel(g_ref, w_ref, out_ref, *, seqs, heads, groups):
    sub = g_ref.shape[0] // seqs
    grad = dot_nt(g_ref[...], w_ref[...]).astype(BF)
    for h in range(heads):
        for g in range(groups):
            at = (h * groups + g) * LANES
            for s in range(seqs):
                out_ref[(s * groups + g) * heads + h] = grad[s * sub : (s + 1) * sub, at : at + LANES]


def grad_attn_units(grad, w_full, seqs, heads, groups):
    tokens, width = grad.shape
    return pl.pallas_call(
        functools.partial(grad_attn_kernel, seqs=seqs, heads=heads, groups=groups),
        out_shape=jax.ShapeDtypeStruct((seqs * groups * heads, tokens // seqs, LANES), BF),
        in_specs=[pl.BlockSpec(memory_space=pltpu.VMEM)] * 2,
        out_specs=pl.BlockSpec(memory_space=pltpu.VMEM),
        cost_estimate=cost(3),
        name="grad_attn_units",
    )(grad, w_full)


def minor_of(axis):
    return 2 if axis == "head" or lax.axis_size(axis) < 16 else 4


def place_of(axis):
    minor = minor_of(axis)
    index = lax.axis_index(axis)
    return index // minor, index % minor


def hop(value, axis, da, db):
    n, minor = lax.axis_size(axis), minor_of(axis)
    major = n // minor
    pairs = [
        (a * minor + b, (a + da) % major * minor + (b + db) % minor)
        for a in range(major)
        for b in range(minor)
    ]
    return lax.ppermute(value, axis, pairs)


def after(value, *others):
    return lax.optimization_barrier((value,) + others)[0]


def gather_slots(value, axis):
    slots = [spread(value, axis)]
    for _ in range(1, lax.axis_size(axis) // minor_of(axis)):
        slots.append(spread(hop(slots[-1][0], axis, 1, 0), axis))
    return slots


def join(*values):
    return lax.optimization_barrier(values)


def spread(value, axis):
    row = [value]
    for _ in range(1, minor_of(axis)):
        row.append(hop(row[-1], axis, 0, 1))
    return row


def slot_owner(axis, a, b):
    minor = minor_of(axis)
    major = lax.axis_size(axis) // minor
    my_a, my_b = place_of(axis)
    return (my_a - a) % major * minor + (my_b - b) % minor


def add(x, y):
    return x.astype(F32) + y.astype(F32)


def ring_moved(parts, axis, da, db):
    total = parts[1 % len(parts)]
    for part in parts[2:]:
        total = add(hop(total, axis, da, db), part).astype(BF)
    return hop(total, axis, da, db)


def ring_reduce(parts, axis, da, db):
    return add(ring_moved(parts, axis, da, db), parts[0])


def pick(value, index):
    return lax.dynamic_index_in_dim(value, index, 0, keepdims=False)


def small_sum(value, axis):
    minor = minor_of(axis)
    major = lax.axis_size(axis) // minor
    value = value + sum(hop(value, axis, 0, d) for d in range(1, minor))
    return value + sum(hop(value, axis, d, 0) for d in range(1, major))


def expert_kernel(owner_ref, *refs, halves, steps, tall):
    slots, (gate_ref, up_ref, down_ref) = refs[: len(refs) - 3], refs[len(refs) - 3 :]
    e, y, k = pl.program_id(0), pl.program_id(1), pl.program_id(2)
    row = y * steps + k
    for i, slot in enumerate(slots):

        @pl.when(owner_ref[i] == e * halves + y)
        def _():
            block = slot[...].astype(F32)
            half = block.shape[1] // 2

            @pl.when(row < tall)
            def _():
                gate_ref[0] = block[:, :half]
                up_ref[0] = block[:, half:]

            @pl.when(row >= tall)
            def _():
                down_ref[0] = block


def expert_outputs(slots, width, ff):
    my_a, my_b = place_of("head")
    halves, experts = len(slots), len(slots[0])
    flat = [block for row in slots for block in row]
    owner = [
        (my_b - b) % experts * halves + (my_a - a) % halves
        for a in range(halves)
        for b in range(experts)
    ]
    owner = jnp.stack(owner).astype(jnp.int32)
    block = math.gcd(flat[0].shape[0], 256)
    steps, tall = flat[0].shape[0] // block, width // block

    def spec(i):
        def place(e, y, k, owner):
            turn = owner[i] - (e * halves + y)
            return (jnp.where(turn == 0, k, jnp.where(turn > 0, 0, steps - 1)), 0)

        return pl.BlockSpec((block, width), place)

    return pl.pallas_call(
        functools.partial(expert_kernel, halves=halves, steps=steps, tall=tall),
        out_shape=(
            jax.ShapeDtypeStruct((experts, width, ff), F32),
            jax.ShapeDtypeStruct((experts, width, ff), F32),
            jax.ShapeDtypeStruct((experts, ff, width), F32),
        ),
        grid_spec=pltpu.PrefetchScalarGridSpec(
            num_scalar_prefetch=1,
            grid=(experts, halves, steps),
            in_specs=[spec(i) for i in range(len(flat))],
            out_specs=[
                pl.BlockSpec((1, block, ff), lambda e, y, k, o: (e, jnp.minimum(y * steps + k, tall - 1), 0)),
                pl.BlockSpec((1, block, ff), lambda e, y, k, o: (e, jnp.minimum(y * steps + k, tall - 1), 0)),
                pl.BlockSpec((1, block, width), lambda e, y, k, o: (e, jnp.maximum(y * steps + k - tall, 0), 0)),
            ],
        ),
        cost_estimate=cost(12),
        name="expert_outputs",
    )(owner, *flat)


def in_order(slots, axis, by_minor=False):
    major, minor = len(slots), len(slots[0])
    whole = jnp.zeros((major * minor,) + slots[0][0].shape, slots[0][0].dtype)
    for a, row in enumerate(slots):
        for b, block in enumerate(row):
            owner = slot_owner(axis, a, b)
            if by_minor:
                owner = owner % minor * major + owner // minor
            whole = lax.dynamic_update_index_in_dim(whole, block, owner, 0)
    return whole


def norm_backward(values, inv_root, gain_vec, grad_normed):
    weighted = grad_normed * gain_vec
    gain_part = jnp.sum(grad_normed * values * inv_root, (0, 1))
    grad_values = inv_root * weighted - values * (inv_root * inv_root * inv_root) * jnp.mean(
        values * weighted, -1, keepdims=True
    )
    return (grad_values, gain_part)


def moe_kernel(*refs, parts):
    x_refs, c_refs = refs[:parts], refs[parts : 2 * parts]
    w_ref, gate_ref, up_ref, down_ref = refs[2 * parts : 2 * parts + 4]
    xs_ref, cs_ref, h_ref, dg_ref, du_ref, out_acc, dx_acc = refs[-7:]
    out_refs, dx_refs = refs[-7 - 2 * parts : -7 - parts], refs[-7 - parts : -7]
    j = pl.program_id(0)
    rows = x_refs[0].shape[0]

    @pl.when(j == 0)
    def _():
        for p in range(parts):
            xs_ref[pl.ds(p * rows, rows), :] = x_refs[p][...]
            cs_ref[pl.ds(p * rows, rows), :] = c_refs[p][...]

    gate, up, down = gate_ref[0], up_ref[0], down_ref[0]
    x, c = xs_ref[...], cs_ref[...]
    weight = jnp.broadcast_to(w_ref[0], (LANES, x.shape[0])).T
    weight = jnp.concatenate([weight] * (gate.shape[1] // LANES), 1)
    gate_lin, up_lin = dot(x, gate), dot(x, up)
    sig = 1.0 / (1.0 + jnp.exp(-gate_lin))
    silu = gate_lin * sig
    h_ref[...] = (weight * silu * up_lin).astype(BF)
    grad_hidden = weight * dot_nt(c, down)
    du_ref[...] = (grad_hidden * silu).astype(BF)
    dg_ref[...] = (grad_hidden * up_lin * (sig + silu * (1.0 - sig))).astype(BF)
    out = dot(h_ref[...], down)
    dx = dot_nt(dg_ref[...], gate) + dot_nt(du_ref[...], up)

    @pl.when(j == 0)
    def _():
        out_acc[...] = out
        dx_acc[...] = dx

    @pl.when(j > 0)
    def _():
        for p in range(parts):
            at = pl.ds(p * rows, rows)
            out_refs[p][...] = (out_acc[at, :] + out[p * rows : (p + 1) * rows]).astype(BF)
            dx_refs[p][...] = (dx_acc[at, :] + dx[p * rows : (p + 1) * rows]).astype(BF)


def moe_block(k, count, xs_in, cs_in, weight, gate, up, down, kept):
    parts = len(xs_in)
    rows, width = xs_in[0].shape
    m = parts * rows
    experts, _, ff = gate.shape
    alone = pl.BlockSpec((rows, width), lambda j: (0, 0))
    wide = pl.BlockSpec((m, width), lambda j: (k, 0))
    narrow = pl.BlockSpec((m, ff), lambda j: (k, j))
    tall = pl.BlockSpec((1, width, ff), lambda j: (j, 0, 0))
    row = jax.ShapeDtypeStruct((rows, width), BF)
    xs = jax.ShapeDtypeStruct((count * m, width), BF)
    hs = jax.ShapeDtypeStruct((count * m, experts * ff), BF)
    outs = pl.pallas_call(
        functools.partial(moe_kernel, parts=parts),
        out_shape=(row,) * (2 * parts) + (xs, xs, hs, hs, hs),
        grid=(experts,),
        in_specs=[alone] * (2 * parts)
        + [
            pl.BlockSpec((1, 1, m), lambda j: (j, 0, 0)),
            tall,
            tall,
            pl.BlockSpec((1, ff, width), lambda j: (j, 0, 0)),
        ]
        + [pl.BlockSpec(memory_space=pl.ANY)] * len(kept),
        out_specs=[alone] * (2 * parts) + [wide, wide, narrow, narrow, narrow],
        scratch_shapes=[pltpu.VMEM((m, width), F32), pltpu.VMEM((m, width), F32)],
        input_output_aliases={2 * parts + 4 + i: 2 * parts + i for i in range(len(kept))},
        cost_estimate=cost(13),
        name="moe_block",
    )(*xs_in, *cs_in, weight, gate, up, down, *kept)
    return outs[:parts], outs[parts : 2 * parts], outs[2 * parts :]


def expert_grad_kernel(expert_ref, x_ref, dg_ref, du_ref, h_ref, c_ref, out_ref, *, tall, ff):
    i = pl.program_id(0)

    @pl.when(i < tall)
    def _():
        out_ref[:, :ff] = dot_tn(x_ref[...], dg_ref[...]).astype(BF)
        out_ref[:, ff:] = dot_tn(x_ref[...], du_ref[...]).astype(BF)

    @pl.when(i >= tall)
    def _():
        out_ref[...] = dot_tn(h_ref[...], c_ref[...]).astype(BF)


def expert_grad(e, xs, cs, hs, dgs, dus, ff):
    m, width = xs.shape
    block = 256
    tall, steps = width // block, (width + ff) // block
    return pl.pallas_call(
        functools.partial(expert_grad_kernel, tall=tall, ff=ff),
        out_shape=jax.ShapeDtypeStruct((width + ff, width), BF),
        grid_spec=pltpu.PrefetchScalarGridSpec(
            num_scalar_prefetch=1,
            grid=(steps,),
            in_specs=[
                pl.BlockSpec((m, block), lambda i, s: (0, jnp.minimum(i, tall - 1))),
                pl.BlockSpec((m, ff), lambda i, s: (0, s[0])),
                pl.BlockSpec((m, ff), lambda i, s: (0, s[0])),
                pl.BlockSpec((m, block), lambda i, s: (0, s[0] * (ff // block) + jnp.maximum(i - tall, 0))),
                pl.BlockSpec((m, width), lambda i, s: (0, 0)),
            ],
            out_specs=pl.BlockSpec((block, width), lambda i, s: (i, 0)),
        ),
        cost_estimate=cost(13),
        name="expert_grad",
    )(e.astype(jnp.int32).reshape(1), xs, dgs, dus, hs, cs)


def qkv_grad_kernel(owner_ref, x_ref, g_ref, w_ref, *refs, rows, sub):
    part_refs, (grad_ref, acc_ref) = refs[:-2], refs[-2:]
    s = pl.program_id(0)
    span = x_ref.shape[1]
    shares = span // rows
    joint = []
    for g in range(g_ref.shape[0] // shares):
        units = [g_ref[g * shares + j] for j in range(shares)]
        joint.append(jnp.concatenate([unit[:rows] for unit in units], 0))
        if shares == 1:
            joint.append(units[0][rows:])
        else:
            joint.append(sum(unit[rows:].astype(F32) for unit in units).astype(BF))
    joint = jnp.concatenate(joint, 1)
    acc_ref[...] = jnp.where(s == 0, 0.0, acc_ref[...]) + dot_tn(x_ref[0], joint)
    back = dot_nt(joint, w_ref[...]).astype(BF)

    def give(part_ref, place):
        part_ref[0] = back[place * sub : (place + 1) * sub]

    for place in range(span // sub):
        for slot, part_ref in enumerate(part_refs):
            pl.when(owner_ref[place] == slot)(functools.partial(give, part_ref, place))

    @pl.when(s == pl.num_programs(0) - 1)
    def _():
        grad_ref[...] = acc_ref[...].astype(BF)


def qkv_grad(slot_at, normed_all, grad_pay, w_joint, rows, sub):
    seqs, span, width = normed_all.shape
    n, r, _ = grad_pay.shape
    cols = w_joint.shape[1]
    heads = span // sub
    return pl.pallas_call(
        functools.partial(qkv_grad_kernel, rows=rows, sub=sub),
        out_shape=(
            *[jax.ShapeDtypeStruct((seqs, sub, width), BF)] * heads,
            jax.ShapeDtypeStruct((width, cols), BF),
        ),
        grid_spec=pltpu.PrefetchScalarGridSpec(
            num_scalar_prefetch=1,
            grid=(seqs,),
            in_specs=[
                pl.BlockSpec((1, span, width), lambda s, o: (s, 0, 0)),
                pl.BlockSpec((n // seqs, r, LANES), lambda s, o: (s, 0, 0)),
                pl.BlockSpec((width, cols), lambda s, o: (0, 0)),
            ],
            out_specs=[
                *[pl.BlockSpec((1, sub, width), lambda s, o: (s, 0, 0))] * heads,
                pl.BlockSpec((width, cols), lambda s, o: (0, 0)),
            ],
            scratch_shapes=[pltpu.VMEM((width, cols), F32)],
        ),
        cost_estimate=cost(7),
        name="qkv_grad",
    )(slot_at, normed_all, grad_pay, w_joint)


def weight_kernel(owner_ref, *refs, tall, low):
    slots, (q_ref, k_ref, v_ref, o_ref) = refs[:-4], refs[-4:]
    cols = slots[0].shape[1]
    pieces = o_ref.shape[1] // cols
    short = low // pieces
    for i, slot in enumerate(slots):
        block = slot[...].astype(F32)
        at = pl.ds(pl.multiple_of(owner_ref[i] * tall, tall), tall)
        keys, values = [], []
        for g in range(cols // 256):
            q_ref[at, g * LANES : (g + 1) * LANES] = block[:tall, g * 256 : g * 256 + LANES]
            keys.append(block[:tall, g * 256 + LANES : g * 256 + LANES + HD])
            values.append(block[:tall, g * 256 + LANES + HD : (g + 1) * 256])
        k_ref[at, :] = jnp.concatenate(keys, 1)
        v_ref[at, :] = jnp.concatenate(values, 1)
        at = pl.ds(pl.multiple_of(owner_ref[i] * short, short), short)
        for p in range(pieces):
            o_ref[at, p * cols : (p + 1) * cols] = block[tall + p * short : tall + (p + 1) * short]


def weight_outputs(slots, owner, width, q_cols, k_cols, low):
    tall = width // len(slots)
    return pl.pallas_call(
        functools.partial(weight_kernel, tall=tall, low=low),
        out_shape=(
            jax.ShapeDtypeStruct((width, q_cols), F32),
            jax.ShapeDtypeStruct((width, k_cols), F32),
            jax.ShapeDtypeStruct((width, k_cols), F32),
            jax.ShapeDtypeStruct((q_cols, width), F32),
        ),
        in_specs=[pl.BlockSpec(memory_space=pltpu.SMEM)] + [pl.BlockSpec(memory_space=pltpu.VMEM)] * len(slots),
        out_specs=[pl.BlockSpec(memory_space=pltpu.VMEM)] * 4,
        cost_estimate=cost(3),
        name="weight_outputs",
    )(owner, *slots)


def per_device(
    hidden_in,
    norm_gain1,
    w_query,
    w_key,
    w_value,
    w_out,
    norm_gain2,
    expert_gate,
    expert_up,
    expert_down,
    routes,
    gate_weights,
    cotangent,
):
    seqs, sub, width = hidden_in.shape
    tokens = seqs * sub
    heads, ranks = lax.axis_size("head"), lax.axis_size("seq")
    kv_local = w_key.shape[1] // HD
    q_cols, k_cols = w_query.shape[1], w_key.shape[1]
    span = sub * heads
    total_len = span * ranks
    shares = ranks // (seqs * kv_local)
    rows = span // shares
    experts_local = expert_gate.shape[0]
    expert_total = experts_local * ranks
    capacity = tokens * TOP * 5 // (4 * expert_total)
    seq_rank = lax.axis_index("seq")
    head_rank = lax.axis_index("head")
    share = (seq_rank % shares).astype(jnp.int32).reshape(1)

    x_float = hidden_in.astype(F32)
    inv_one = lax.rsqrt(jnp.mean(x_float * x_float, -1, keepdims=True) + norm_eps)
    normed_one = (x_float * inv_one * norm_gain1).astype(BF)
    normed_all = in_order(gather_slots(normed_one, "head"), "head")
    normed_all = normed_all.transpose(1, 0, 2, 3).reshape(seqs, span, width)

    route_tok = routes.reshape(tokens, TOP)
    gate_tok = gate_weights.reshape(tokens, TOP)
    chosen = route_tok[:, :, None] == jnp.arange(expert_total, dtype=jnp.int32)
    named = jnp.any(chosen, 1)
    gate_of = jnp.sum(jnp.where(chosen, gate_tok[:, :, None], 0.0), 1)
    order = jnp.arange(tokens, dtype=jnp.int32)
    before = (order[:, None] > order[None, :]).astype(BF)
    rank_of = dot(before, named.astype(BF))
    weight_of = jnp.where(named & (rank_of < capacity), gate_of, 0.0)
    minor = minor_of("seq")
    major = ranks // minor
    weight_send = weight_of.reshape(tokens, ranks, experts_local).transpose(1, 2, 0)
    weight_all = lax.all_to_all(weight_send, "seq", 0, 0, tiled=True)
    tables = [jnp.asarray(table) for table in angle_tables(span, 1) + angle_tables(ranks, span)]
    cot_value = cotangent.reshape(tokens, width)
    cot_line = [cot_value]
    for a in range(1, major - 1):
        cot_line.append(hop(cot_line[-1], "seq", 1, 0))
    cot_rows = [spread(cot_line[a], "seq") for a in range(major - 2)]
    normed_all = after(normed_all, cot_line[1], weight_all)
    pay, w_joint = project_qkv(normed_all, w_query, w_key, w_value, tables, seq_rank.astype(jnp.int32).reshape(1), rows)

    pay = after(pay, cot_line[-1], *[block for row in cot_rows for block in row])
    pay = lax.all_to_all(pay, "seq", 0, 0, tiled=True)
    w_full = in_order(gather_slots(after(w_out, normed_all), "head"), "head").reshape(heads * q_cols, width)
    cot_line.append(hop(after(cot_line[-1], pay), "seq", 1, 0))
    cot_rows.append(spread(after(cot_line[-2], pay), "seq"))
    attn, attn_t, lse = attn_fwd(pay, share, span)
    attn = after(attn, cot_line[-1], *cot_rows[-1])
    cot_rows.append(spread(cot_line[-1], "seq"))

    def to_tokens(value):
        if shares == 1:
            value = value.reshape(ranks * heads, sub, LANES)
            value = lax.all_to_all(value, ("seq", "head"), 0, 0, tiled=True)
            value = value.reshape(seqs, kv_local, heads, sub, LANES)
            return value.transpose(0, 3, 2, 1, 4)
        value = lax.all_to_all(value, "seq", 0, 0, tiled=True)
        value = value.reshape(seqs, kv_local, heads, sub, LANES).transpose(2, 0, 1, 3, 4)
        value = lax.all_to_all(value, "head", 0, 0, tiled=True)
        return value.transpose(1, 3, 0, 2, 4)

    def to_units(value):
        value = value.transpose(2, 0, 3, 1, 4)
        value = lax.all_to_all(value, "head", 0, 0, tiled=True)
        value = value.transpose(1, 2, 0, 3, 4).reshape(ranks, rows, LANES)
        return lax.all_to_all(value, "seq", 0, 0, tiled=True)

    attn_local = after(to_tokens(attn), w_full).reshape(tokens, heads * q_cols)
    resid = x_float + dot(attn_local, w_full).reshape(seqs, sub, width)
    inv_two = lax.rsqrt(jnp.mean(resid * resid, -1, keepdims=True) + norm_eps)
    normed_two = (resid * inv_two * norm_gain2).astype(BF).reshape(tokens, width)
    normed_two = after(normed_two, *cot_rows[-1])

    def block(a, row, kept):
        return moe_block(
            a, major, row, cot_rows[a], weights[a], expert_gate, expert_up, expert_down, kept
        )

    weight_all = after(weight_all, normed_two)
    weights = [
        jnp.concatenate([pick(weight_all, slot_owner("seq", a, b)) for b in range(minor)], 1)[:, None, :]
        for a in range(major)
    ]
    row, value, weights = join(spread(normed_two, "seq"), hop(normed_two, "seq", 1, 0), weights)
    outs, kept, out_slots, grads = (), (), [], []
    for a in range(major - 1):
        if a + 2 < major:
            moved = hop(value, "seq", 1, 0)
        else:
            moved = ring_reduce(grads[1], "seq", 0, 1).astype(BF)
        if a + 2 < major:
            coming = spread(value, "seq")
        else:
            coming = [value] + [hop(other, "seq", 1, 0) for other in row[1:]]
        outs, grad, kept = block(a, row, kept)
        row, value, outs, grad = join(coming, moved, outs, grad)
        out_slots.append(outs)
        grads.append(grad)
    total, grad_rows = value, {}
    ff = expert_gate.shape[2]
    my_y, my_core = place_of("head")
    experts = [1 - my_core, my_core]
    expert_sum = []
    for a in range(2, major + 1):
        moved = hop(total, "seq", 1, 0)
        slot = a % major
        came = ring_reduce(grads[slot], "seq", 0, 1).astype(BF)
        if a == 2:
            outs, grad, kept = block(major - 1, row, kept)
            moved, came, outs, grad = join(moved, came, outs, grad)
            out_slots.append(outs)
            grads.append(grad)
            total = add(moved, came).astype(BF)
            continue
        if len(expert_sum) < 2:
            xs, cs, hs, dgs, dus = kept
            part = expert_grad(experts[len(expert_sum)], after(xs, total), cs, hs, dgs, dus, ff)
            if not expert_sum:
                moved, came, part = join(moved, came, part)
            expert_sum.append(part)
        total = add(moved, came)
        if a < major:
            total = total.astype(BF)
    grad_normed_two = total.reshape(seqs, sub, width)
    grad_out = cotangent.astype(F32)
    grad_norm_two, gain_two_part = norm_backward(resid, inv_two, norm_gain2, grad_normed_two)
    grad_resid = grad_out + grad_norm_two
    halves = heads // 2
    expert_sum = [value.reshape(halves, -1, width) for value in expert_sum]
    other = hop(expert_sum[0], "head", 0, 1)
    grad_resid_b = after(grad_resid.astype(BF), expert_sum[1])
    if shares == 1:
        grad_attn_sent = grad_attn_units(grad_resid_b.reshape(tokens, width), w_full, seqs, heads, kv_local)
        grad_attn = lax.all_to_all(grad_attn_sent, ("seq", "head"), 0, 0, tiled=True).reshape(ranks, rows, LANES)
    else:
        grad_attn = dot_nt(grad_resid_b.reshape(tokens, width), w_full).astype(BF)
        grad_attn_sent = grad_attn.reshape(seqs, sub, heads, kv_local, LANES)
        grad_attn = to_units(grad_attn_sent)
    out_near = ring_moved([after(block, grad_normed_two) for block in out_slots[1]], "seq", 0, 1)
    out_near = add(out_near, out_slots[1][0]).astype(BF)
    mine = add(after(expert_sum[1], grad_attn_sent), other).astype(BF)
    tall = mine.shape[1]
    cut = tall // 4

    def cut_of(index, start, size):
        return lax.dynamic_slice(mine, (index, start, 0), (1, size, width))[0]

    places = [(my_y + d) % halves for d in range(1, halves)]
    lower = [cut_of(place, cut, tall - cut) for place in places]
    upper = [cut_of(place, 0, cut) for place in places]
    grad_attn, out_near, out_slots, lower, upper = join(grad_attn, out_near, out_slots, lower, upper)
    lower = [hop(value, "head", d, 0) for d, value in enumerate(lower, 1)]

    out_moved = hop(out_near, "seq", 1, 0)
    out_rows = [ring_moved(out_slots[a], "seq", 0, 1) for a in range(2, major)]
    grad_pay = attn_bwd(pay, grad_attn, attn_t, lse, tables, share, span)
    grad_pay, out_moved, out_rows, lower, upper, mine, out_slots = join(
        grad_pay, out_moved, out_rows, lower, upper, mine, out_slots
    )
    upper = [hop(value, "head", d, 0) for d, value in enumerate(upper, 1)]

    my_a, my_b = place_of("seq")
    cols = w_joint.shape[1]
    got_pay = lax.all_to_all(grad_pay, "seq", 0, 0, tiled=True)
    out_last = ring_moved(out_slots[0], "seq", 0, 1)
    out_w_part = dot_tn(attn_local, after(grad_resid_b, grad_pay).reshape(tokens, width)).astype(BF)
    out_w_part = out_w_part.reshape(heads, q_cols, width)
    out_w = [
        ring_reduce([pick(out_w_part, slot_owner("head", a, b)) for b in range(2)], "head", 0, 1).astype(BF)
        for a in range(halves)
    ]
    out_w_moved = ring_moved(out_w, "head", 1, 0)
    part = pick(mine, my_y)
    for over, under in zip(upper, lower):
        part = add(part, jnp.concatenate([over, under], 0))
    part = after(part.astype(BF), out_w_moved)
    expert_rows = [hop(part, "head", d, 0) for d in range(1, halves)]
    out_total = (add(out_rows[0], out_slots[2][0]) + out_moved.astype(F32)).astype(BF)
    got_pay, part, out_last, out_w_moved, out_total = join(got_pay, part, out_last, out_w_moved, out_total)

    slot_at = [
        (my_y - place // 2) % halves * 2 + (my_core - place % 2) % 2 for place in range(heads)
    ]
    slot_at = jnp.stack(slot_at).astype(jnp.int32)
    *grad_part, grad_w_joint = qkv_grad(slot_at, normed_all, got_pay, w_joint, rows, sub)

    part_rows = [
        ring_reduce([grad_part[a * 2 + b] for b in range(2)], "head", 0, 1).astype(BF) for a in range(halves)
    ]
    out_w = add(after(out_w_moved, part_rows[0]), out_w[0]).astype(BF)
    out_w = out_w.reshape(minor, major, q_cols // ranks, width // cols, cols)
    out_w = out_w.transpose(0, 1, 3, 2, 4).reshape(minor, major, -1, cols)
    values = [grad_w_joint.reshape(minor, major, width // ranks, cols), out_w]
    came = [[hop(pick(value, (my_b + d) % minor), "seq", 0, d) for d in range(1, minor)] for value in values]
    out_moved = hop(out_total, "seq", 1, 0)
    came, out_moved, part_rows, expert_rows = join(came, out_moved, part_rows, expert_rows)

    def summed(value, moved):
        for other in moved:
            value = add(value, other)
        return value.astype(BF)

    low = values[1].shape[2]
    total = jnp.concatenate([summed(pick(value, my_b), moved) for value, moved in zip(values, came)], 1)
    came = [hop(pick(total, (my_a + d) % major), "seq", d, 0) for d in range(1, major)]
    part_moved = ring_moved(part_rows, "head", 1, 0)
    expert_rows = [part] + expert_rows
    expert_slots = [[row, hop(row, "head", 0, 1)] for row in expert_rows]
    expert_totals = expert_outputs(expert_slots, width, ff)
    came, part_moved, expert_totals, total = join(came, part_moved, expert_totals, total)
    gate_total, up_total, down_total = expert_totals

    total = summed(pick(total, my_a), came)
    first = [hop(total, "seq", 0, d) for d in range(1, minor)]
    sums = [hop(total, "seq", d, 0) for d in range(1, major)]
    part_moved = after(part_moved, total)
    grad_normed_one = add(part_moved, part_rows[0])
    grad_norm_one, gain_one_part = norm_backward(x_float, inv_one, norm_gain1, grad_normed_one)
    gains = after(jnp.stack([gain_one_part, gain_two_part]), *first, sums[0])
    gains = gains + sum(hop(gains, "seq", d, 0) for d in range(1, major))
    input_grad = (grad_resid + grad_norm_one).astype(BF)
    first, sums, out_total, gains, input_grad = join(
        first,
        sums,
        (add(out_rows[1], out_slots[3][0]) + out_moved.astype(F32)).astype(BF),
        gains,
        input_grad,
    )

    rest = [[hop(value, "seq", 0, d) for value in sums] for d in range(1, minor)]
    out_moved = hop(out_total, "seq", 1, 0)
    gains = small_sum(after(gains, rest[0][0]), "head")
    gains = gains + sum(hop(gains, "seq", 0, d) for d in range(1, minor))
    weight_slots = [total] + first
    weight_owner = [(my_b - d) % minor * major + my_a for d in range(minor)]
    for d in range(1, major):
        weight_slots += [sums[d - 1]] + [row[d - 1] for row in rest]
        weight_owner += [(my_b - b) % minor * major + (my_a - d) % major for b in range(minor)]
    weight_owner = jnp.stack(weight_owner).astype(jnp.int32)
    query_total, key_total, value_total, w_out_total = weight_outputs(
        weight_slots, weight_owner, width, q_cols, k_cols, low
    )
    out_total = add(out_last, out_slots[0][0]) + out_moved.astype(F32)
    layer_out = (resid + out_total.reshape(seqs, sub, width)).astype(BF)

    return (
        layer_out,
        input_grad,
        gains[0],
        query_total,
        key_total,
        value_total,
        w_out_total,
        gains[1],
        gate_total,
        up_total,
        down_total,
    )


def solution(mesh):
    return jax.shard_map(
        per_device,
        mesh=mesh,
        in_specs=(
            P(None, ("seq", "head"), None),
            P(),
            P(None, "head"),
            P(None, "head"),
            P(None, "head"),
            P("head", None),
            P(),
            P("seq", None, None),
            P("seq", None, None),
            P("seq", None, None),
            P(None, ("seq", "head"), None),
            P(None, ("seq", "head"), None),
            P(None, ("seq", "head"), None),
        ),
        out_specs=(
            P(None, ("seq", "head"), None),
            P(None, ("seq", "head"), None),
            P(),
            P(None, "head"),
            P(None, "head"),
            P(None, "head"),
            P("head", None),
            P(),
            P("seq", None, None),
            P("seq", None, None),
            P("seq", None, None),
        ),
        check_vma=False,
    )
```

```python
import functools
import math

import jax
import jax.numpy as jnp
import numpy as np
from jax import lax
from jax.experimental import pallas as pl
from jax.experimental.pallas import tpu as pltpu
from jax.sharding import PartitionSpec as P

HD = 64
TOP = 8
LANES = 128

norm_eps = 1e-06
rope_base = 10000.0
masked_value = -1e30
BF = jnp.bfloat16
F32 = jnp.float32


def cost(us):
    return pl.CostEstimate(flops=0, bytes_accessed=us * 3000000, transcendentals=0)


def attn_fwd_kernel(share_ref, pay_ref, out_ref, ot_ref, lse_ref, kv_ref, kvt_ref, *, span, rows, block):
    b = pl.program_id(0)
    count = pay_ref.shape[0]

    @pl.when(b == 0)
    def _():
        def fill(i, _):
            start = pl.multiple_of(i * span, span)
            tile = pay_ref[i, pl.ds(rows, span), :]
            kv_ref[pl.ds(start, span), :] = tile
            kvt_ref[:, pl.ds(start, span)] = tile.T
            return 0
        lax.fori_loop(0, count, fill, 0)

    q_start = b * span + share_ref[0] * rows
    qt = pay_ref[b, pl.ds(0, rows), :].T * jnp.bfloat16(0.125)
    qt = jnp.concatenate([qt[:HD], qt[HD:]], 1)
    qt = jnp.concatenate([qt, jnp.zeros_like(qt)], 0)
    last = (q_start + rows - 1) // block

    def step(kb, carry, masked):
        run_max, run_sum, acc = carry
        start = pl.multiple_of(kb * block, block)
        scores = jnp.dot(kv_ref[pl.ds(start, block), :], qt, preferred_element_type=jnp.float32)
        if masked:
            keys = start + lax.broadcasted_iota(jnp.int32, scores.shape, 0)
            queries = q_start + lax.broadcasted_iota(jnp.int32, scores.shape, 1) % rows
            scores = jnp.where(keys <= queries, scores, masked_value)
        new_max = jnp.maximum(run_max, jnp.max(scores, 0, keepdims=True))
        factor = jnp.exp(run_max - new_max)
        probs = jnp.exp(scores - new_max)
        run_sum = run_sum * factor + jnp.sum(probs, 0, keepdims=True)
        acc = acc * factor + jnp.dot(
            kvt_ref[pl.ds(HD, HD), pl.ds(start, block)], probs.astype(jnp.bfloat16), preferred_element_type=jnp.float32)
        return new_max, run_sum, acc

    carry = (jnp.full((1, 2 * rows), masked_value, jnp.float32), jnp.zeros((1, 2 * rows), jnp.float32), jnp.zeros((HD, 2 * rows), jnp.float32))
    carry = lax.fori_loop(0, last, functools.partial(step, masked=False), carry)
    run_max, run_sum, acc = step(last, carry, True)
    ot = acc / run_sum
    ot_ref[0] = ot
    lse_ref[0] = jnp.broadcast_to(run_max + jnp.log(run_sum), lse_ref.shape[1:])
    out_ref[0] = jnp.concatenate([ot[:, :rows], ot[:, rows:]], 0).T.astype(jnp.bfloat16)

def attn_fwd(pay, share, span, block=512):
    n, r, _ = pay.shape
    rows = r - span
    total = n * span
    block = min(block, total)
    return pl.pallas_call(
        functools.partial(attn_fwd_kernel, span=span, rows=rows, block=block),
        out_shape=(jax.ShapeDtypeStruct((n, rows, 128), jnp.bfloat16), jax.ShapeDtypeStruct((n, HD, 2 * rows), jnp.float32), jax.ShapeDtypeStruct((n, 8, 2 * rows), jnp.float32)),
        grid_spec=pltpu.PrefetchScalarGridSpec(
            num_scalar_prefetch=1, grid=(n,),
            in_specs=[pl.BlockSpec((n, r, 128), lambda b, s: (0, 0, 0))],
            out_specs=[pl.BlockSpec((1, rows, 128), lambda b, s: (b, 0, 0)), pl.BlockSpec((1, HD, 2 * rows), lambda b, s: (b, 0, 0)), pl.BlockSpec((1, 8, 2 * rows), lambda b, s: (b, 0, 0))],
            scratch_shapes=[pltpu.VMEM((total, 128), jnp.bfloat16), pltpu.VMEM((128, total), jnp.bfloat16)],
        ),
        cost_estimate=cost(16),
        name="attn_fwd",
    )(share, pay)

def swap_halves(v):
    lane = lax.broadcasted_iota(jnp.int32, v.shape, v.ndim - 1)
    return jnp.where(lane % HD < HD // 2, pltpu.roll(v, 128 - HD // 2, v.ndim - 1), pltpu.roll(v, HD // 2, v.ndim - 1))

def attn_bwd_kernel(share_ref, pay_ref, go_ref, ot_ref, lse_ref, *refs, span, rows, block):
    tables, (out_ref, kv_ref, kvt_ref, dk_ref, dv_ref) = refs[:4], refs[4:]
    b = pl.program_id(0)
    count = pay_ref.shape[0]

    @pl.when(b == 0)
    def _():
        def fill(i, _):
            start = pl.multiple_of(i * span, span)
            tile = pay_ref[i, pl.ds(rows, span), :]
            kv_ref[pl.ds(start, span), :] = tile
            kvt_ref[:, pl.ds(start, span)] = tile.T
            return 0
        lax.fori_loop(0, count, fill, 0)
        dk_ref[...] = jnp.zeros_like(dk_ref)
        dv_ref[...] = jnp.zeros_like(dv_ref)

    q_start = b * span + share_ref[0] * rows
    low = lax.broadcasted_iota(jnp.int32, (rows, 128), 1) < HD
    q01 = pay_ref[b, pl.ds(0, rows), :] * jnp.bfloat16(0.125)
    go01 = go_ref[0]
    zero = jnp.zeros_like(q01)
    q_rows = jnp.concatenate([jnp.where(low, q01, zero), jnp.where(low, zero, q01)], 0)
    go_rows = jnp.concatenate([jnp.where(low, go01, zero), jnp.where(low, zero, go01)], 0)
    qt = q01.T
    qt = jnp.concatenate([qt[:HD], qt[HD:]], 1)
    qt = jnp.concatenate([qt, jnp.zeros_like(qt)], 0)
    gt = go01.T
    gt = jnp.concatenate([gt[:HD], gt[HD:]], 1)
    delta = jnp.sum(gt.astype(jnp.float32) * ot_ref[0], 0, keepdims=True)
    gt = jnp.concatenate([jnp.zeros_like(gt), gt], 0)
    lse = lse_ref[0, 0:1, :]
    last = (q_start + rows - 1) // block

    def step(kb, dq, masked):
        start = pl.multiple_of(kb * block, block)
        kv = kv_ref[pl.ds(start, block), :]
        scores = jnp.dot(kv, qt, preferred_element_type=jnp.float32)
        probs = jnp.exp(scores - lse)
        if masked:
            keys = start + lax.broadcasted_iota(jnp.int32, scores.shape, 0)
            queries = q_start + lax.broadcasted_iota(jnp.int32, scores.shape, 1) % rows
            probs = jnp.where(keys <= queries, probs, 0.0)
        dprobs = jnp.dot(kv, gt, preferred_element_type=jnp.float32)
        dscores = (probs * (dprobs - delta)).astype(jnp.bfloat16)
        dv_ref[pl.ds(start, block), :] += jnp.dot(probs.astype(jnp.bfloat16), go_rows, preferred_element_type=jnp.float32)
        dk_ref[pl.ds(start, block), :] += jnp.dot(dscores, q_rows, preferred_element_type=jnp.float32)
        return dq + jnp.dot(kvt_ref[pl.ds(0, HD), pl.ds(start, block)], dscores, preferred_element_type=jnp.float32)

    dq = lax.fori_loop(0, last, functools.partial(step, masked=False), jnp.zeros((HD, 2 * rows), jnp.float32))
    dq = step(last, dq, True)
    dq = jnp.concatenate([dq[:, :rows], dq[:, rows:]], 0).T * 0.125
    cosine, sine = turned(tables, pl.ds(pl.multiple_of(share_ref[0] * rows, rows), rows), b)
    dq = dq * cosine - swap_halves(dq) * sine
    out_ref[b, pl.ds(0, rows), :] = dq.astype(jnp.bfloat16)

    @pl.when(b == count - 1)
    def _():
        def drain(i, _):
            start = pl.multiple_of(i * span, span)
            dk = dk_ref[pl.ds(start, span), :]
            dk = dk + pltpu.roll(dk, HD, 1)
            cosine, sine = turned(tables, pl.ds(0, span), i)
            dk = dk * cosine - swap_halves(dk) * sine
            dv = dv_ref[pl.ds(start, span), :]
            dv = dv + pltpu.roll(dv, HD, 1)
            lane = lax.broadcasted_iota(jnp.int32, dk.shape, 1)
            out_ref[i, pl.ds(rows, span), :] = jnp.where(lane < HD, dk, dv).astype(jnp.bfloat16)
            return 0
        lax.fori_loop(0, count, drain, 0)

def attn_bwd(pay, go, ot, lse, tables, share, span, block=512):
    n, r, _ = pay.shape
    rows = r - span
    total = n * span
    block = min(block, total)
    whole = lambda *shape: pl.BlockSpec(shape, lambda b, s: (0,) * len(shape))
    return pl.pallas_call(
        functools.partial(attn_bwd_kernel, span=span, rows=rows, block=block),
        out_shape=jax.ShapeDtypeStruct((n, r, 128), jnp.bfloat16),
        grid_spec=pltpu.PrefetchScalarGridSpec(
            num_scalar_prefetch=1, grid=(n,),
            in_specs=[whole(n, r, 128), pl.BlockSpec((1, rows, 128), lambda b, s: (b, 0, 0)), pl.BlockSpec((1, HD, 2 * rows), lambda b, s: (b, 0, 0)), pl.BlockSpec((1, 8, 2 * rows), lambda b, s: (b, 0, 0)), *[whole(*table.shape) for table in tables]],
            out_specs=whole(n, r, 128),
            scratch_shapes=[pltpu.VMEM((total, 128), jnp.bfloat16), pltpu.VMEM((128, total), jnp.bfloat16), pltpu.VMEM((total, 128), jnp.float32), pltpu.VMEM((total, 128), jnp.float32)],
        ),
        cost_estimate=cost(24),
        name="attn_bwd",
    )(share, pay, go, ot, lse, *tables)

def angle_tables(count, step):
    half = HD // 2
    angles = step * np.arange(count)[:, None] * rope_base ** (-2.0 * np.arange(half) / HD)
    cosine, sine = np.cos(angles), np.sin(angles)
    tables = np.concatenate([cosine] * 4, 1), np.concatenate([-sine, sine] * 2, 1)
    return [table.astype(np.float32) for table in tables]


def turned(tables, at, far):
    cos_ref, sin_ref, cos_far_ref, sin_far_ref = tables
    cosine, sine = cos_ref[at, :], sin_ref[at, :]
    cos_far, sin_far = cos_far_ref[pl.ds(far, 1), :], sin_far_ref[pl.ds(far, 1), :]
    return cosine * cos_far - sine * sin_far, sine * cos_far + cosine * sin_far


def dot(left, right):
    return jnp.dot(left, right, preferred_element_type=F32)


def dot_nt(left, right):
    return lax.dot_general(left, right, (((1,), (1,)), ((), ())), preferred_element_type=F32)


def dot_tn(left, right):
    return lax.dot_general(left, right, (((0,), (0,)), ((), ())), preferred_element_type=F32)


def qkv_kernel(rank_ref, x_ref, wq_ref, wk_ref, wv_ref, *refs, rows):
    tables, (out_ref, w_ref, cos_own, sin_own) = refs[:4], refs[4:]
    span = x_ref.shape[1]
    shares = span // rows
    groups = wk_ref.shape[1] // HD

    @pl.when(pl.program_id(0) == 0)
    def _():
        for g in range(groups):
            w_ref[:, g * 256 : g * 256 + LANES] = wq_ref[:, g * LANES : (g + 1) * LANES]
            pair = [wk_ref[:, g * HD : (g + 1) * HD], wv_ref[:, g * HD : (g + 1) * HD]]
            w_ref[:, g * 256 + LANES : (g + 1) * 256] = jnp.concatenate(pair, 1)
        cos_own[...], sin_own[...] = turned(tables, pl.ds(0, span), rank_ref[0])

    joint = jnp.dot(x_ref[0], w_ref[...], preferred_element_type=F32)
    low = lax.broadcasted_iota(jnp.int32, (span, LANES), 1) < HD
    cosine, sine = cos_own[...], sin_own[...]
    for g in range(groups):
        query = joint[:, g * 256 : g * 256 + LANES]
        other = joint[:, g * 256 + LANES : (g + 1) * 256]
        query = (query * cosine + swap_halves(query) * sine).astype(BF)
        other = jnp.where(low, other * cosine + swap_halves(other) * sine, other).astype(BF)
        for j in range(shares):
            out_ref[g * shares + j, pl.ds(0, rows), :] = query[j * rows : (j + 1) * rows]
            out_ref[g * shares + j, pl.ds(rows, span), :] = other


def project_qkv(normed_all, w_query, w_key, w_value, tables, rank, rows):
    seqs, span, width = normed_all.shape
    q_cols, k_cols = w_query.shape[1], w_key.shape[1]
    cols = q_cols + 2 * k_cols
    units = cols // 256 * (span // rows)
    fixed = lambda *shape: pl.BlockSpec(shape, lambda s, r: (0,) * len(shape))
    return pl.pallas_call(
        functools.partial(qkv_kernel, rows=rows),
        out_shape=(
            jax.ShapeDtypeStruct((seqs * units, rows + span, LANES), BF),
            jax.ShapeDtypeStruct((width, cols), BF),
        ),
        grid_spec=pltpu.PrefetchScalarGridSpec(
            num_scalar_prefetch=1,
            grid=(seqs,),
            in_specs=[
                pl.BlockSpec((1, span, width), lambda s, r: (s, 0, 0)),
                fixed(width, q_cols),
                fixed(width, k_cols),
                fixed(width, k_cols),
                *[fixed(*table.shape) for table in tables],
            ],
            out_specs=[pl.BlockSpec((units, rows + span, LANES), lambda s, r: (s, 0, 0)), fixed(width, cols)],
            scratch_shapes=[pltpu.VMEM((span, LANES), F32), pltpu.VMEM((span, LANES), F32)],
        ),
        cost_estimate=cost(6),
        name="project_qkv",
    )(rank, normed_all, w_query, w_key, w_value, *tables)


def grad_attn_kernel(g_ref, w_ref, out_ref, *, seqs, heads, groups):
    sub = g_ref.shape[0] // seqs
    grad = dot_nt(g_ref[...], w_ref[...]).astype(BF)
    for h in range(heads):
        for g in range(groups):
            at = (h * groups + g) * LANES
            for s in range(seqs):
                out_ref[(s * groups + g) * heads + h] = grad[s * sub : (s + 1) * sub, at : at + LANES]


def grad_attn_units(grad, w_full, seqs, heads, groups):
    tokens, width = grad.shape
    return pl.pallas_call(
        functools.partial(grad_attn_kernel, seqs=seqs, heads=heads, groups=groups),
        out_shape=jax.ShapeDtypeStruct((seqs * groups * heads, tokens // seqs, LANES), BF),
        in_specs=[pl.BlockSpec(memory_space=pltpu.VMEM)] * 2,
        out_specs=pl.BlockSpec(memory_space=pltpu.VMEM),
        cost_estimate=cost(3),
        name="grad_attn_units",
    )(grad, w_full)


def minor_of(axis):
    return 2 if axis == "head" or lax.axis_size(axis) < 16 else 4


def place_of(axis):
    minor = minor_of(axis)
    index = lax.axis_index(axis)
    return index // minor, index % minor


def hop(value, axis, da, db):
    n, minor = lax.axis_size(axis), minor_of(axis)
    major = n // minor
    pairs = [
        (a * minor + b, (a + da) % major * minor + (b + db) % minor)
        for a in range(major)
        for b in range(minor)
    ]
    return lax.ppermute(value, axis, pairs)


def after(value, *others):
    return lax.optimization_barrier((value,) + others)[0]


def gather_slots(value, axis):
    slots = [spread(value, axis)]
    for _ in range(1, lax.axis_size(axis) // minor_of(axis)):
        slots.append(spread(hop(slots[-1][0], axis, 1, 0), axis))
    return slots


def join(*values):
    return lax.optimization_barrier(values)


def spread(value, axis):
    row = [value]
    for _ in range(1, minor_of(axis)):
        row.append(hop(row[-1], axis, 0, 1))
    return row


def slot_owner(axis, a, b):
    minor = minor_of(axis)
    major = lax.axis_size(axis) // minor
    my_a, my_b = place_of(axis)
    return (my_a - a) % major * minor + (my_b - b) % minor


def add(x, y):
    return x.astype(F32) + y.astype(F32)


def ring_moved(parts, axis, da, db):
    total = parts[1 % len(parts)]
    for part in parts[2:]:
        total = add(hop(total, axis, da, db), part).astype(BF)
    return hop(total, axis, da, db)


def ring_reduce(parts, axis, da, db):
    return add(ring_moved(parts, axis, da, db), parts[0])


def pick(value, index):
    return lax.dynamic_index_in_dim(value, index, 0, keepdims=False)


def small_sum(value, axis):
    minor = minor_of(axis)
    major = lax.axis_size(axis) // minor
    value = value + sum(hop(value, axis, 0, d) for d in range(1, minor))
    return value + sum(hop(value, axis, d, 0) for d in range(1, major))


def expert_kernel(owner_ref, *refs, halves, steps, tall):
    slots, (gate_ref, up_ref, down_ref) = refs[: len(refs) - 3], refs[len(refs) - 3 :]
    e, y, k = pl.program_id(0), pl.program_id(1), pl.program_id(2)
    row = y * steps + k
    for i, slot in enumerate(slots):

        @pl.when(owner_ref[i] == e * halves + y)
        def _():
            block = slot[...].astype(F32)
            half = block.shape[1] // 2

            @pl.when(row < tall)
            def _():
                gate_ref[0] = block[:, :half]
                up_ref[0] = block[:, half:]

            @pl.when(row >= tall)
            def _():
                down_ref[0] = block


def expert_outputs(slots, width, ff):
    my_a, my_b = place_of("head")
    halves, experts = len(slots), len(slots[0])
    flat = [block for row in slots for block in row]
    owner = [
        (my_b - b) % experts * halves + (my_a - a) % halves
        for a in range(halves)
        for b in range(experts)
    ]
    owner = jnp.stack(owner).astype(jnp.int32)
    block = math.gcd(flat[0].shape[0], 256)
    steps, tall = flat[0].shape[0] // block, width // block

    def spec(i):
        def place(e, y, k, owner):
            turn = owner[i] - (e * halves + y)
            return (jnp.where(turn == 0, k, jnp.where(turn > 0, 0, steps - 1)), 0)

        return pl.BlockSpec((block, width), place)

    return pl.pallas_call(
        functools.partial(expert_kernel, halves=halves, steps=steps, tall=tall),
        out_shape=(
            jax.ShapeDtypeStruct((experts, width, ff), F32),
            jax.ShapeDtypeStruct((experts, width, ff), F32),
            jax.ShapeDtypeStruct((experts, ff, width), F32),
        ),
        grid_spec=pltpu.PrefetchScalarGridSpec(
            num_scalar_prefetch=1,
            grid=(experts, halves, steps),
            in_specs=[spec(i) for i in range(len(flat))],
            out_specs=[
                pl.BlockSpec((1, block, ff), lambda e, y, k, o: (e, jnp.minimum(y * steps + k, tall - 1), 0)),
                pl.BlockSpec((1, block, ff), lambda e, y, k, o: (e, jnp.minimum(y * steps + k, tall - 1), 0)),
                pl.BlockSpec((1, block, width), lambda e, y, k, o: (e, jnp.maximum(y * steps + k - tall, 0), 0)),
            ],
        ),
        cost_estimate=cost(12),
        name="expert_outputs",
    )(owner, *flat)


def in_order(slots, axis, by_minor=False):
    major, minor = len(slots), len(slots[0])
    whole = jnp.zeros((major * minor,) + slots[0][0].shape, slots[0][0].dtype)
    for a, row in enumerate(slots):
        for b, block in enumerate(row):
            owner = slot_owner(axis, a, b)
            if by_minor:
                owner = owner % minor * major + owner // minor
            whole = lax.dynamic_update_index_in_dim(whole, block, owner, 0)
    return whole


def norm_backward(values, inv_root, gain_vec, grad_normed):
    weighted = grad_normed * gain_vec
    gain_part = jnp.sum(grad_normed * values * inv_root, (0, 1))
    grad_values = inv_root * weighted - values * (inv_root * inv_root * inv_root) * jnp.mean(
        values * weighted, -1, keepdims=True
    )
    return (grad_values, gain_part)


def moe_kernel(*refs, parts):
    x_refs, c_refs = refs[:parts], refs[parts : 2 * parts]
    w_ref, gate_ref, up_ref, down_ref = refs[2 * parts : 2 * parts + 4]
    xs_ref, cs_ref, h_ref, dg_ref, du_ref, out_acc, dx_acc = refs[-7:]
    out_refs, dx_refs = refs[-7 - 2 * parts : -7 - parts], refs[-7 - parts : -7]
    j = pl.program_id(0)
    rows = x_refs[0].shape[0]

    @pl.when(j == 0)
    def _():
        for p in range(parts):
            xs_ref[pl.ds(p * rows, rows), :] = x_refs[p][...]
            cs_ref[pl.ds(p * rows, rows), :] = c_refs[p][...]

    gate, up, down = gate_ref[0], up_ref[0], down_ref[0]
    x, c = xs_ref[...], cs_ref[...]
    weight = jnp.broadcast_to(w_ref[0], (LANES, x.shape[0])).T
    weight = jnp.concatenate([weight] * (gate.shape[1] // LANES), 1)
    gate_lin, up_lin = dot(x, gate), dot(x, up)
    sig = 1.0 / (1.0 + jnp.exp(-gate_lin))
    silu = gate_lin * sig
    h_ref[...] = (weight * silu * up_lin).astype(BF)
    grad_hidden = weight * dot_nt(c, down)
    du_ref[...] = (grad_hidden * silu).astype(BF)
    dg_ref[...] = (grad_hidden * up_lin * (sig + silu * (1.0 - sig))).astype(BF)
    out = dot(h_ref[...], down)
    dx = dot_nt(dg_ref[...], gate) + dot_nt(du_ref[...], up)

    @pl.when(j == 0)
    def _():
        out_acc[...] = out
        dx_acc[...] = dx

    @pl.when(j > 0)
    def _():
        for p in range(parts):
            at = pl.ds(p * rows, rows)
            out_refs[p][...] = (out_acc[at, :] + out[p * rows : (p + 1) * rows]).astype(BF)
            dx_refs[p][...] = (dx_acc[at, :] + dx[p * rows : (p + 1) * rows]).astype(BF)


def moe_block(k, count, xs_in, cs_in, weight, gate, up, down, kept):
    parts = len(xs_in)
    rows, width = xs_in[0].shape
    m = parts * rows
    experts, _, ff = gate.shape
    alone = pl.BlockSpec((rows, width), lambda j: (0, 0))
    wide = pl.BlockSpec((m, width), lambda j: (k, 0))
    narrow = pl.BlockSpec((m, ff), lambda j: (k, j))
    tall = pl.BlockSpec((1, width, ff), lambda j: (j, 0, 0))
    row = jax.ShapeDtypeStruct((rows, width), BF)
    xs = jax.ShapeDtypeStruct((count * m, width), BF)
    hs = jax.ShapeDtypeStruct((count * m, experts * ff), BF)
    outs = pl.pallas_call(
        functools.partial(moe_kernel, parts=parts),
        out_shape=(row,) * (2 * parts) + (xs, xs, hs, hs, hs),
        grid=(experts,),
        in_specs=[alone] * (2 * parts)
        + [
            pl.BlockSpec((1, 1, m), lambda j: (j, 0, 0)),
            tall,
            tall,
            pl.BlockSpec((1, ff, width), lambda j: (j, 0, 0)),
        ]
        + [pl.BlockSpec(memory_space=pl.ANY)] * len(kept),
        out_specs=[alone] * (2 * parts) + [wide, wide, narrow, narrow, narrow],
        scratch_shapes=[pltpu.VMEM((m, width), F32), pltpu.VMEM((m, width), F32)],
        input_output_aliases={2 * parts + 4 + i: 2 * parts + i for i in range(len(kept))},
        cost_estimate=cost(13),
        name="moe_block",
    )(*xs_in, *cs_in, weight, gate, up, down, *kept)
    return outs[:parts], outs[parts : 2 * parts], outs[2 * parts :]


def expert_grad_kernel(expert_ref, x_ref, dg_ref, du_ref, h_ref, c_ref, out_ref, *, tall, ff):
    i = pl.program_id(0)

    @pl.when(i < tall)
    def _():
        out_ref[:, :ff] = dot_tn(x_ref[...], dg_ref[...]).astype(BF)
        out_ref[:, ff:] = dot_tn(x_ref[...], du_ref[...]).astype(BF)

    @pl.when(i >= tall)
    def _():
        out_ref[...] = dot_tn(h_ref[...], c_ref[...]).astype(BF)


def expert_grad(e, xs, cs, hs, dgs, dus, ff):
    m, width = xs.shape
    block = 256
    tall, steps = width // block, (width + ff) // block
    return pl.pallas_call(
        functools.partial(expert_grad_kernel, tall=tall, ff=ff),
        out_shape=jax.ShapeDtypeStruct((width + ff, width), BF),
        grid_spec=pltpu.PrefetchScalarGridSpec(
            num_scalar_prefetch=1,
            grid=(steps,),
            in_specs=[
                pl.BlockSpec((m, block), lambda i, s: (0, jnp.minimum(i, tall - 1))),
                pl.BlockSpec((m, ff), lambda i, s: (0, s[0])),
                pl.BlockSpec((m, ff), lambda i, s: (0, s[0])),
                pl.BlockSpec((m, block), lambda i, s: (0, s[0] * (ff // block) + jnp.maximum(i - tall, 0))),
                pl.BlockSpec((m, width), lambda i, s: (0, 0)),
            ],
            out_specs=pl.BlockSpec((block, width), lambda i, s: (i, 0)),
        ),
        cost_estimate=cost(13),
        name="expert_grad",
    )(e.astype(jnp.int32).reshape(1), xs, dgs, dus, hs, cs)


def qkv_grad_kernel(owner_ref, x_ref, g_ref, w_ref, *refs, rows, sub):
    part_refs, (grad_ref, acc_ref) = refs[:-2], refs[-2:]
    s = pl.program_id(0)
    span = x_ref.shape[1]
    shares = span // rows
    joint = []
    for g in range(g_ref.shape[0] // shares):
        units = [g_ref[g * shares + j] for j in range(shares)]
        joint.append(jnp.concatenate([unit[:rows] for unit in units], 0))
        if shares == 1:
            joint.append(units[0][rows:])
        else:
            joint.append(sum(unit[rows:].astype(F32) for unit in units).astype(BF))
    joint = jnp.concatenate(joint, 1)
    acc_ref[...] = jnp.where(s == 0, 0.0, acc_ref[...]) + dot_tn(x_ref[0], joint)
    back = dot_nt(joint, w_ref[...]).astype(BF)

    def give(part_ref, place):
        part_ref[0] = back[place * sub : (place + 1) * sub]

    for place in range(span // sub):
        for slot, part_ref in enumerate(part_refs):
            pl.when(owner_ref[place] == slot)(functools.partial(give, part_ref, place))

    @pl.when(s == pl.num_programs(0) - 1)
    def _():
        grad_ref[...] = acc_ref[...].astype(BF)


def qkv_grad(slot_at, normed_all, grad_pay, w_joint, rows, sub):
    seqs, span, width = normed_all.shape
    n, r, _ = grad_pay.shape
    cols = w_joint.shape[1]
    heads = span // sub
    return pl.pallas_call(
        functools.partial(qkv_grad_kernel, rows=rows, sub=sub),
        out_shape=(
            *[jax.ShapeDtypeStruct((seqs, sub, width), BF)] * heads,
            jax.ShapeDtypeStruct((width, cols), BF),
        ),
        grid_spec=pltpu.PrefetchScalarGridSpec(
            num_scalar_prefetch=1,
            grid=(seqs,),
            in_specs=[
                pl.BlockSpec((1, span, width), lambda s, o: (s, 0, 0)),
                pl.BlockSpec((n // seqs, r, LANES), lambda s, o: (s, 0, 0)),
                pl.BlockSpec((width, cols), lambda s, o: (0, 0)),
            ],
            out_specs=[
                *[pl.BlockSpec((1, sub, width), lambda s, o: (s, 0, 0))] * heads,
                pl.BlockSpec((width, cols), lambda s, o: (0, 0)),
            ],
            scratch_shapes=[pltpu.VMEM((width, cols), F32)],
        ),
        cost_estimate=cost(7),
        name="qkv_grad",
    )(slot_at, normed_all, grad_pay, w_joint)


def weight_kernel(owner_ref, *refs, tall, low):
    slots, (q_ref, k_ref, v_ref, o_ref) = refs[:-4], refs[-4:]
    cols = slots[0].shape[1]
    pieces = o_ref.shape[1] // cols
    short = low // pieces
    for i, slot in enumerate(slots):
        block = slot[...].astype(F32)
        at = pl.ds(pl.multiple_of(owner_ref[i] * tall, tall), tall)
        keys, values = [], []
        for g in range(cols // 256):
            q_ref[at, g * LANES : (g + 1) * LANES] = block[:tall, g * 256 : g * 256 + LANES]
            keys.append(block[:tall, g * 256 + LANES : g * 256 + LANES + HD])
            values.append(block[:tall, g * 256 + LANES + HD : (g + 1) * 256])
        k_ref[at, :] = jnp.concatenate(keys, 1)
        v_ref[at, :] = jnp.concatenate(values, 1)
        at = pl.ds(pl.multiple_of(owner_ref[i] * short, short), short)
        for p in range(pieces):
            o_ref[at, p * cols : (p + 1) * cols] = block[tall + p * short : tall + (p + 1) * short]


def weight_outputs(slots, owner, width, q_cols, k_cols, low):
    tall = width // len(slots)
    return pl.pallas_call(
        functools.partial(weight_kernel, tall=tall, low=low),
        out_shape=(
            jax.ShapeDtypeStruct((width, q_cols), F32),
            jax.ShapeDtypeStruct((width, k_cols), F32),
            jax.ShapeDtypeStruct((width, k_cols), F32),
            jax.ShapeDtypeStruct((q_cols, width), F32),
        ),
        in_specs=[pl.BlockSpec(memory_space=pltpu.SMEM)] + [pl.BlockSpec(memory_space=pltpu.VMEM)] * len(slots),
        out_specs=[pl.BlockSpec(memory_space=pltpu.VMEM)] * 4,
        cost_estimate=cost(3),
        name="weight_outputs",
    )(owner, *slots)


def per_device(
    hidden_in,
    norm_gain1,
    w_query,
    w_key,
    w_value,
    w_out,
    norm_gain2,
    expert_gate,
    expert_up,
    expert_down,
    routes,
    gate_weights,
    cotangent,
):
    seqs, sub, width = hidden_in.shape
    tokens = seqs * sub
    heads, ranks = lax.axis_size("head"), lax.axis_size("seq")
    kv_local = w_key.shape[1] // HD
    q_cols, k_cols = w_query.shape[1], w_key.shape[1]
    span = sub * heads
    total_len = span * ranks
    shares = ranks // (seqs * kv_local)
    rows = span // shares
    experts_local = expert_gate.shape[0]
    expert_total = experts_local * ranks
    capacity = tokens * TOP * 5 // (4 * expert_total)
    seq_rank = lax.axis_index("seq")
    head_rank = lax.axis_index("head")
    share = (seq_rank % shares).astype(jnp.int32).reshape(1)

    x_float = hidden_in.astype(F32)
    inv_one = lax.rsqrt(jnp.mean(x_float * x_float, -1, keepdims=True) + norm_eps)
    normed_one = (x_float * inv_one * norm_gain1).astype(BF)
    normed_all = in_order(gather_slots(normed_one, "head"), "head")
    normed_all = normed_all.transpose(1, 0, 2, 3).reshape(seqs, span, width)

    route_tok = routes.reshape(tokens, TOP)
    gate_tok = gate_weights.reshape(tokens, TOP)
    chosen = route_tok[:, :, None] == jnp.arange(expert_total, dtype=jnp.int32)
    named = jnp.any(chosen, 1)
    gate_of = jnp.sum(jnp.where(chosen, gate_tok[:, :, None], 0.0), 1)
    order = jnp.arange(tokens, dtype=jnp.int32)
    before = (order[:, None] > order[None, :]).astype(BF)
    rank_of = dot(before, named.astype(BF))
    weight_of = jnp.where(named & (rank_of < capacity), gate_of, 0.0)
    minor = minor_of("seq")
    major = ranks // minor
    weight_send = weight_of.reshape(tokens, ranks, experts_local).transpose(1, 2, 0)
    weight_all = lax.all_to_all(weight_send, "seq", 0, 0, tiled=True)
    tables = [jnp.asarray(table) for table in angle_tables(span, 1) + angle_tables(ranks, span)]
    cot_value = cotangent.reshape(tokens, width)
    cot_line = [cot_value]
    for a in range(1, major - 1):
        cot_line.append(hop(cot_line[-1], "seq", 1, 0))
    cot_rows = [spread(cot_line[a], "seq") for a in range(major - 2)]
    normed_all = after(normed_all, cot_line[1], weight_all)
    pay, w_joint = project_qkv(normed_all, w_query, w_key, w_value, tables, seq_rank.astype(jnp.int32).reshape(1), rows)

    pay = after(pay, cot_line[-1], *[block for row in cot_rows for block in row])
    pay = lax.all_to_all(pay, "seq", 0, 0, tiled=True)
    w_full = in_order(gather_slots(after(w_out, normed_all), "head"), "head").reshape(heads * q_cols, width)
    cot_line.append(hop(after(cot_line[-1], pay), "seq", 1, 0))
    cot_rows.append(spread(after(cot_line[-2], pay), "seq"))
    attn, attn_t, lse = attn_fwd(pay, share, span)
    attn = after(attn, cot_line[-1], *cot_rows[-1])
    cot_rows.append(spread(cot_line[-1], "seq"))

    def to_tokens(value):
        if shares == 1:
            value = value.reshape(ranks * heads, sub, LANES)
            value = lax.all_to_all(value, ("seq", "head"), 0, 0, tiled=True)
            value = value.reshape(seqs, kv_local, heads, sub, LANES)
            return value.transpose(0, 3, 2, 1, 4)
        value = lax.all_to_all(value, "seq", 0, 0, tiled=True)
        value = value.reshape(seqs, kv_local, heads, sub, LANES).transpose(2, 0, 1, 3, 4)
        value = lax.all_to_all(value, "head", 0, 0, tiled=True)
        return value.transpose(1, 3, 0, 2, 4)

    def to_units(value):
        value = value.transpose(2, 0, 3, 1, 4)
        value = lax.all_to_all(value, "head", 0, 0, tiled=True)
        value = value.transpose(1, 2, 0, 3, 4).reshape(ranks, rows, LANES)
        return lax.all_to_all(value, "seq", 0, 0, tiled=True)

    attn_local = after(to_tokens(attn), w_full).reshape(tokens, heads * q_cols)
    resid = x_float + dot(attn_local, w_full).reshape(seqs, sub, width)
    inv_two = lax.rsqrt(jnp.mean(resid * resid, -1, keepdims=True) + norm_eps)
    normed_two = (resid * inv_two * norm_gain2).astype(BF).reshape(tokens, width)
    normed_two = after(normed_two, *cot_rows[-1])

    def block(a, row, kept):
        return moe_block(
            a, major, row, cot_rows[a], weights[a], expert_gate, expert_up, expert_down, kept
        )

    weight_all = after(weight_all, normed_two)
    weights = [
        jnp.concatenate([pick(weight_all, slot_owner("seq", a, b)) for b in range(minor)], 1)[:, None, :]
        for a in range(major)
    ]
    row, value, weights = join(spread(normed_two, "seq"), hop(normed_two, "seq", 1, 0), weights)
    outs, kept, out_slots, grads = (), (), [], []
    for a in range(major - 1):
        if a + 2 < major:
            moved = hop(value, "seq", 1, 0)
        else:
            moved = ring_reduce(grads[1], "seq", 0, 1).astype(BF)
        if a + 2 < major:
            coming = spread(value, "seq")
        else:
            coming = [value] + [hop(other, "seq", 1, 0) for other in row[1:]]
        outs, grad, kept = block(a, row, kept)
        row, value, outs, grad = join(coming, moved, outs, grad)
        out_slots.append(outs)
        grads.append(grad)
    total, grad_rows = value, {}
    ff = expert_gate.shape[2]
    my_y, my_core = place_of("head")
    experts = [1 - my_core, my_core]
    expert_sum = []
    for a in range(2, major + 1):
        moved = hop(total, "seq", 1, 0)
        slot = a % major
        came = ring_reduce(grads[slot], "seq", 0, 1).astype(BF)
        if a == 2:
            outs, grad, kept = block(major - 1, row, kept)
            moved, came, outs, grad = join(moved, came, outs, grad)
            out_slots.append(outs)
            grads.append(grad)
            total = add(moved, came).astype(BF)
            continue
        if len(expert_sum) < 2:
            xs, cs, hs, dgs, dus = kept
            part = expert_grad(experts[len(expert_sum)], after(xs, total), cs, hs, dgs, dus, ff)
            if not expert_sum:
                moved, came, part = join(moved, came, part)
            expert_sum.append(part)
        total = add(moved, came)
        if a < major:
            total = total.astype(BF)
    grad_normed_two = total.reshape(seqs, sub, width)
    grad_out = cotangent.astype(F32)
    grad_norm_two, gain_two_part = norm_backward(resid, inv_two, norm_gain2, grad_normed_two)
    grad_resid = grad_out + grad_norm_two
    halves = heads // 2
    expert_sum = [value.reshape(halves, -1, width) for value in expert_sum]
    other = hop(expert_sum[0], "head", 0, 1)
    grad_resid_b = after(grad_resid.astype(BF), expert_sum[1])
    if shares == 1:
        grad_attn_sent = grad_attn_units(grad_resid_b.reshape(tokens, width), w_full, seqs, heads, kv_local)
        grad_attn = lax.all_to_all(grad_attn_sent, ("seq", "head"), 0, 0, tiled=True).reshape(ranks, rows, LANES)
    else:
        grad_attn = dot_nt(grad_resid_b.reshape(tokens, width), w_full).astype(BF)
        grad_attn_sent = grad_attn.reshape(seqs, sub, heads, kv_local, LANES)
        grad_attn = to_units(grad_attn_sent)
    out_near = ring_moved([after(block, grad_normed_two) for block in out_slots[1]], "seq", 0, 1)
    out_near = add(out_near, out_slots[1][0]).astype(BF)
    mine = add(after(expert_sum[1], grad_attn_sent), other).astype(BF)
    tall = mine.shape[1]
    cut = tall // 4

    def cut_of(index, start, size):
        return lax.dynamic_slice(mine, (index, start, 0), (1, size, width))[0]

    places = [(my_y + d) % halves for d in range(1, halves)]
    lower = [cut_of(place, cut, tall - cut) for place in places]
    upper = [cut_of(place, 0, cut) for place in places]
    grad_attn, out_near, out_slots, lower, upper = join(grad_attn, out_near, out_slots, lower, upper)
    lower = [hop(value, "head", d, 0) for d, value in enumerate(lower, 1)]

    out_moved = hop(out_near, "seq", 1, 0)
    out_rows = [ring_moved(out_slots[a], "seq", 0, 1) for a in range(2, major)]
    grad_pay = attn_bwd(pay, grad_attn, attn_t, lse, tables, share, span)
    grad_pay, out_moved, out_rows, lower, upper, mine, out_slots = join(
        grad_pay, out_moved, out_rows, lower, upper, mine, out_slots
    )
    upper = [hop(value, "head", d, 0) for d, value in enumerate(upper, 1)]

    my_a, my_b = place_of("seq")
    cols = w_joint.shape[1]
    got_pay = lax.all_to_all(grad_pay, "seq", 0, 0, tiled=True)
    out_last = ring_moved(out_slots[0], "seq", 0, 1)
    out_w_part = dot_tn(attn_local, after(grad_resid_b, grad_pay).reshape(tokens, width)).astype(BF)
    out_w_part = out_w_part.reshape(heads, q_cols, width)
    out_w = [
        ring_reduce([pick(out_w_part, slot_owner("head", a, b)) for b in range(2)], "head", 0, 1).astype(BF)
        for a in range(halves)
    ]
    out_w_moved = ring_moved(out_w, "head", 1, 0)
    part = pick(mine, my_y)
    for over, under in zip(upper, lower):
        part = add(part, jnp.concatenate([over, under], 0))
    part = after(part.astype(BF), out_w_moved)
    expert_rows = [hop(part, "head", d, 0) for d in range(1, halves)]
    out_total = (add(out_rows[0], out_slots[2][0]) + out_moved.astype(F32)).astype(BF)
    got_pay, part, out_last, out_w_moved, out_total = join(got_pay, part, out_last, out_w_moved, out_total)

    slot_at = [
        (my_y - place // 2) % halves * 2 + (my_core - place % 2) % 2 for place in range(heads)
    ]
    slot_at = jnp.stack(slot_at).astype(jnp.int32)
    *grad_part, grad_w_joint = qkv_grad(slot_at, normed_all, got_pay, w_joint, rows, sub)

    part_rows = [
        ring_reduce([grad_part[a * 2 + b] for b in range(2)], "head", 0, 1).astype(BF) for a in range(halves)
    ]
    out_w = add(after(out_w_moved, part_rows[0]), out_w[0]).astype(BF)
    out_w = out_w.reshape(minor, major, q_cols // ranks, width // cols, cols)
    out_w = out_w.transpose(0, 1, 3, 2, 4).reshape(minor, major, -1, cols)
    values = [grad_w_joint.reshape(minor, major, width // ranks, cols), out_w]
    came = [[hop(pick(value, (my_b + d) % minor), "seq", 0, d) for d in range(1, minor)] for value in values]
    out_moved = hop(out_total, "seq", 1, 0)
    came, out_moved, part_rows, expert_rows = join(came, out_moved, part_rows, expert_rows)

    def summed(value, moved):
        for other in moved:
            value = add(value, other)
        return value.astype(BF)

    low = values[1].shape[2]
    total = jnp.concatenate([summed(pick(value, my_b), moved) for value, moved in zip(values, came)], 1)
    came = [hop(pick(total, (my_a + d) % major), "seq", d, 0) for d in range(1, major)]
    part_moved = ring_moved(part_rows, "head", 1, 0)
    expert_rows = [part] + expert_rows
    expert_slots = [[row, hop(row, "head", 0, 1)] for row in expert_rows]
    expert_totals = expert_outputs(expert_slots, width, ff)
    came, part_moved, expert_totals, total = join(came, part_moved, expert_totals, total)
    gate_total, up_total, down_total = expert_totals

    total = summed(pick(total, my_a), came)
    first = [hop(total, "seq", 0, d) for d in range(1, minor)]
    sums = [hop(total, "seq", d, 0) for d in range(1, major)]
    part_moved = after(part_moved, total)
    grad_normed_one = add(part_moved, part_rows[0])
    grad_norm_one, gain_one_part = norm_backward(x_float, inv_one, norm_gain1, grad_normed_one)
    gains = after(jnp.stack([gain_one_part, gain_two_part]), *first, sums[0])
    gains = gains + sum(hop(gains, "seq", d, 0) for d in range(1, major))
    input_grad = (grad_resid + grad_norm_one).astype(BF)
    first, sums, out_total, input_grad = join(
        first,
        sums,
        (add(out_rows[1], out_slots[3][0]) + out_moved.astype(F32)).astype(BF),
        input_grad,
    )

    rest = [[hop(value, "seq", 0, d) for value in sums] for d in range(1, minor)]
    out_moved = hop(after(out_total, gains), "seq", 1, 0)
    gains = small_sum(after(gains, rest[0][0]), "head")
    gains = gains + sum(hop(gains, "seq", 0, d) for d in range(1, minor))
    weight_slots = [total] + first
    weight_owner = [(my_b - d) % minor * major + my_a for d in range(minor)]
    for d in range(1, major):
        weight_slots += [sums[d - 1]] + [row[d - 1] for row in rest]
        weight_owner += [(my_b - b) % minor * major + (my_a - d) % major for b in range(minor)]
    weight_owner = jnp.stack(weight_owner).astype(jnp.int32)
    query_total, key_total, value_total, w_out_total = weight_outputs(
        weight_slots, weight_owner, width, q_cols, k_cols, low
    )
    out_total = add(out_last, out_slots[0][0]) + out_moved.astype(F32)
    layer_out = (resid + out_total.reshape(seqs, sub, width)).astype(BF)

    return (
        layer_out,
        input_grad,
        gains[0],
        query_total,
        key_total,
        value_total,
        w_out_total,
        gains[1],
        gate_total,
        up_total,
        down_total,
    )


def solution(mesh):
    return jax.shard_map(
        per_device,
        mesh=mesh,
        in_specs=(
            P(None, ("seq", "head"), None),
            P(),
            P(None, "head"),
            P(None, "head"),
            P(None, "head"),
            P("head", None),
            P(),
            P("seq", None, None),
            P("seq", None, None),
            P("seq", None, None),
            P(None, ("seq", "head"), None),
            P(None, ("seq", "head"), None),
            P(None, ("seq", "head"), None),
        ),
        out_specs=(
            P(None, ("seq", "head"), None),
            P(None, ("seq", "head"), None),
            P(),
            P(None, "head"),
            P(None, "head"),
            P(None, "head"),
            P("head", None),
            P(),
            P("seq", None, None),
            P("seq", None, None),
            P("seq", None, None),
        ),
        check_vma=False,
    )
```
